512 devices in a mesh: gz: 8 (over y), row: 4 (over x), col: 16 (over z, core).
Axes of the slice: x: 4, y: 8, z: 8, core: 2. Of those that a mesh axis runs over, the one named last changes fastest.
Arguments:
- anc_lower: bfloat16 [17, 1024, 1024], P(None, 'col', 'row'), may hold values from -0.125 to 0.125
- anc_upper: bfloat16 [17, 1024, 1024], P(None, 'col', 'row'), may hold values from -0.125 to 0.125
- sub_lower: bfloat16 [112, 1024, 1024], P('gz', 'col', 'row'), may hold values from -0.125 to 0.125
- sub_upper: bfloat16 [112, 1024, 1024], P('gz', 'col', 'row'), may hold values from -0.125 to 0.125
- anc_rhs: bfloat16 [7, 1024, 64], P(None, 'col'), may hold values from -6 to 6
- sub_rhs: bfloat16 [24, 1024, 64], P('gz', 'col'), may hold values from -6 to 6
- layer_subtree: int32 [8], replicated, may hold values from 0 to 7, each once
- sub_pattern: int32 [88, 2], P('gz'), may hold values 0 or 1
Outputs:
- anc_solution: float32 [7, 1024, 64], P(None, ('row', 'col'))
- sub_solution: float32 [24, 1024, 64], P('gz', ('row', 'col'))
The draws below stay inside these ranges and needn't reach their ends.
Inputs may be any that keep to these rules, and one draw needn't show every extreme that they name: `layer_subtree`: each subtree is held by exactly one layer.
All inputs are finite; a program needn't handle non-finite values. No bound on the sum of `sub_pattern` on one device may be relied on, other than what follows from the above.
Results may differ from the reference program's by a relative error of at most 0.018.
Values may be sent and summed in bfloat16 or wider, within the bound.
No kernel may reach another device: no remote copies, remote signals or barrier semaphores. Data moves between devices by JAX's collectives and lax.ppermute only.
A program may use at most 64 MiB of HBM per device.

```python
import jax
import jax.numpy as jnp
import numpy as np

S = 1024
R = 64
SUB_LEVELS = 2
SUB_NODES = 3
ANC_NODES = 7
SUB_PAIRS = 11
ANC_PAIRS = 10
N_GZ = 8


def place_ends(result, stream_key, low, high):
    longest = result.shape.index(max(result.shape))
    spots = []
    for shift in (0, 1):
        where = [jax.random.randint(jax.random.fold_in(stream_key, axis), (), 0, length) for axis, length in enumerate(result.shape)]
        where[longest] = (where[longest] + shift) % result.shape[longest]
        spots.append(tuple(where))
    return result.at[spots[0]].set(low).at[spots[1]].set(high)


def level_of(key, shape, pieces, low, top_value):
    def one(dim, parts):
        steps = jax.random.uniform(jax.random.fold_in(jax.random.fold_in(key, 6), dim), (parts,), jnp.float32, low / len(pieces), top_value / len(pieces))
        return jnp.repeat(jnp.exp(steps), shape[dim] // parts).reshape((-1,) + (1,) * (len(shape) - dim - 1))

    loudness = one(*pieces[0])
    for cut in pieces[1:]:
        loudness = loudness * one(*cut)
    return loudness


def noise(key, dims, spread, reach, pieces=(), kind=jnp.bfloat16):
    result = spread * jax.random.normal(key, dims, jnp.float32)
    if pieces:
        result = result * level_of(key, dims, pieces, -0.22, 0.18)
    return jnp.clip(result, -reach, reach).astype(kind)


def setup_inputs(seed: int = 0) -> dict:
    key_of = jax.random.split(jax.random.key(seed), 9)
    return {
        "anc_lower": noise(key_of[0], (ANC_NODES + ANC_PAIRS, S, S), (2 * S) ** -0.5, 0.125, ((1, 16), (2, 4))),
        "anc_upper": noise(key_of[1], (ANC_NODES + ANC_PAIRS, S, S), (2 * S) ** -0.5, 0.125, ((1, 16), (2, 4))),
        "sub_lower": noise(key_of[2], (N_GZ * (SUB_NODES + SUB_PAIRS), S, S), (2 * S) ** -0.5, 0.125, ((0, 8), (1, 16), (2, 4))),
        "sub_upper": noise(key_of[3], (N_GZ * (SUB_NODES + SUB_PAIRS), S, S), (2 * S) ** -0.5, 0.125, ((0, 8), (1, 16), (2, 4))),
        "anc_rhs": noise(key_of[4], (ANC_NODES, S, R), 1.0, 6.0, ((1, 16),)),
        "sub_rhs": noise(key_of[5], (N_GZ * SUB_NODES, S, R), 1.0, 6.0, ((0, 8), (1, 16))),
        "layer_subtree": jax.random.permutation(key_of[6], N_GZ).astype(jnp.int32),
        "sub_pattern": place_ends((jax.random.randint(key_of[7], (N_GZ * SUB_PAIRS, 2), 0, 4) < 3).astype(jnp.int32), jax.random.fold_in(key_of[7], 1), 0, 1),
    }


def subtree_pairs(levels):
    listed = []
    for member in range(SUB_NODES):
        height = (member + 1).bit_length() - 1
        for global_level in range(levels):
            listed.append((member, 0, global_level))
        for local_level in range(height):
            listed.append((member, 1, ((member + 1) >> (height - local_level)) - 1))
    return listed


def ancestor_pairs(levels):
    listed = []
    for member in range(2 ** levels - 1):
        height = (member + 1).bit_length() - 1
        for upper_level in range(height):
            listed.append((member, ((member + 1) >> (height - upper_level)) - 1))
    return listed


def level_span(depth_now):
    return 2 ** depth_now - 1, 2 ** (depth_now + 1) - 1


def apply_pair(matrix, vectors):
    return jnp.einsum("...ik,...kr->...ir", matrix.astype(jnp.float32), vectors.astype(jnp.float32))


def apply_inverse(matrix, vectors):
    return jnp.einsum("...ki,...kr->...ir", matrix.astype(jnp.float32), vectors.astype(jnp.float32))


def reference(anc_lower, anc_upper, sub_lower, sub_upper, anc_rhs, sub_rhs, layer_subtree, sub_pattern):
    layers = N_GZ
    levels = layers.bit_length() - 1
    anc_count = layers - 1
    sub_list = subtree_pairs(levels)
    anc_list = ancestor_pairs(levels)
    pair_count = len(sub_list)
    low_blocks = sub_lower.reshape(layers, SUB_NODES + pair_count, S, S)
    up_blocks = sub_upper.reshape(layers, SUB_NODES + pair_count, S, S)
    given_sub = sub_rhs.reshape(layers, SUB_NODES, S, R)
    pattern = sub_pattern.reshape(layers, pair_count, 2).astype(jnp.float32)
    powers = jnp.asarray(2 ** (levels - np.arange(levels)), jnp.int32)
    heap_ids = (layer_subtree[:, None] + layers) // powers[None, :] - 1
    choose = (heap_ids[:, :, None] == jnp.arange(anc_count, dtype=jnp.int32)[None, None, :]).astype(jnp.float32)

    sub_acc = [jnp.zeros((layers, S, R), jnp.float32) for member in range(SUB_NODES)]
    to_anc = jnp.zeros((anc_count, S, R), jnp.float32)
    sub_rows = [None] * SUB_NODES
    for depth_now in reversed(range(SUB_LEVELS)):
        first_id, stop_id = level_span(depth_now)
        for member in range(first_id, stop_id):
            residual = (given_sub[:, member].astype(jnp.float32) - sub_acc[member]).astype(jnp.bfloat16)
            sub_rows[member] = apply_inverse(low_blocks[:, member], residual).astype(jnp.bfloat16)
        for position, (source, pair_kind, target) in enumerate(sub_list):
            if first_id <= source < stop_id:
                update = apply_pair(low_blocks[:, SUB_NODES + position], sub_rows[source])
                update = update * pattern[:, position, 0][:, None, None]
                if pair_kind == 1:
                    sub_acc[target] = sub_acc[target] + update
                else:
                    to_anc = to_anc + jnp.einsum("ga,gir->air", choose[:, target], update)

    anc_acc = [jnp.zeros((S, R), jnp.float32) for member in range(anc_count)]
    anc_rows = [None] * anc_count
    for depth_now in reversed(range(levels)):
        first_id, stop_id = level_span(depth_now)
        for member in range(first_id, stop_id):
            residual = (anc_rhs[member].astype(jnp.float32) - to_anc[member] - anc_acc[member]).astype(jnp.bfloat16)
            anc_rows[member] = apply_inverse(anc_lower[member], residual).astype(jnp.bfloat16)
        for position, (source, target) in enumerate(anc_list):
            if first_id <= source < stop_id:
                anc_acc[target] = anc_acc[target] + apply_pair(anc_lower[anc_count + position], anc_rows[source])

    anc_z = [None] * anc_count
    anc_out = [None] * anc_count
    for depth_now in range(levels):
        first_id, stop_id = level_span(depth_now)
        for member in range(first_id, stop_id):
            running = anc_rows[member].astype(jnp.float32)
            for position, (source, target) in enumerate(anc_list):
                if source == member:
                    running = running - apply_pair(anc_upper[anc_count + position], anc_z[target])
            solved = apply_inverse(anc_upper[member], running.astype(jnp.bfloat16))
            anc_out[member] = solved
            anc_z[member] = solved.astype(jnp.bfloat16)

    selected = jnp.einsum("gea,air->geir", choose, jnp.stack(anc_z).astype(jnp.float32)).astype(jnp.bfloat16)
    sub_z = [None] * SUB_NODES
    sub_out = [None] * SUB_NODES
    for depth_now in range(SUB_LEVELS):
        first_id, stop_id = level_span(depth_now)
        for member in range(first_id, stop_id):
            running = sub_rows[member].astype(jnp.float32)
            for position, (source, pair_kind, target) in enumerate(sub_list):
                if source == member:
                    anchor = selected[:, target] if pair_kind == 0 else sub_z[target]
                    update = apply_pair(up_blocks[:, SUB_NODES + position], anchor)
                    running = running - update * pattern[:, position, 1][:, None, None]
            solved = apply_inverse(up_blocks[:, member], running.astype(jnp.bfloat16))
            sub_out[member] = solved
            sub_z[member] = solved.astype(jnp.bfloat16)
    return jnp.stack(anc_out), jnp.stack(sub_out, 1).reshape(layers * SUB_NODES, S, R)
```

```python
import jax
import jax.numpy as jnp
import numpy as np
from jax import lax
from jax.sharding import Mesh, PartitionSpec as P

SUB_LEVELS = 2
SUB_NODES = 3
F32 = jnp.float32
BF16 = jnp.bfloat16
CORES = 2


def level_span(depth):
    return 2**depth - 1, 2 ** (depth + 1) - 1


def depth_of(node):
    return (node + 1).bit_length() - 1


def above(node, level):
    return ((node + 1) >> (depth_of(node) - level)) - 1


def dot(spec, left, right):
    return jnp.einsum(spec, left, right, preferred_element_type=F32)


def swapped(array):
    return lax.ppermute(array, "core", [(0, 1), (1, 0)])


def summed(array, axis):
    copies = jnp.broadcast_to(array.astype(BF16), (lax.axis_size(axis), *array.shape))
    tiles = lax.all_to_all(copies, axis, 0, 0, tiled=True)
    return jnp.sum(tiles.astype(F32), axis=0)


def local(anc_lower, anc_upper, sub_lower, sub_upper, anc_rhs, sub_rhs, layer_subtree, sub_pattern):
    layers = lax.axis_size("gz")
    levels = layers.bit_length() - 1
    anc_count = layers - 1
    nrow, nz = lax.axis_size("row"), lax.axis_size("z")
    own, wide = sub_lower.shape[1:]
    size = wide * nrow
    pair_rows = own * CORES
    out_rows = wide // (nz * CORES)
    cols = sub_rhs.shape[2] // CORES
    per = cols // (layers * nrow)
    g, r, z, core = (lax.axis_index(name) for name in ("gz", "row", "z", "core"))

    sub_pairs = {}
    for m in range(SUB_NODES):
        for kind, count in ((0, levels), (1, depth_of(m))):
            for u in range(count):
                sub_pairs[m, kind, u] = len(sub_pairs)
    anc_pairs = {}
    for a in range(anc_count):
        for u in range(depth_of(a)):
            anc_pairs[a, u] = anc_count + len(anc_pairs)

    low_w = sub_pattern[:, 0].astype(BF16)
    up_w = sub_pattern[:, 1].astype(BF16)
    powers = jnp.asarray(2 ** (levels - np.arange(levels)), jnp.int32)
    heap_ids = (layer_subtree[:, None] + layers) // powers[None, :] - 1
    choose = heap_ids[:, :, None] == jnp.arange(anc_count, dtype=jnp.int32)
    choose = choose.astype(F32)
    choose_here = lax.dynamic_index_in_dim(choose, g, 0, keepdims=False)

    def halves(array, dim, base=0):
        first = lax.dynamic_slice_in_dim(array, base + core * own, own, dim)
        second = lax.dynamic_slice_in_dim(array, base + (1 - core) * own, own, dim)
        return jnp.concatenate([first, second], dim)

    def gathered(blocks):
        return lax.all_gather(blocks, "row", axis=2, tiled=True)

    low_two = (sub_lower, swapped(sub_lower))
    rhs_here = lax.dynamic_slice_in_dim(sub_rhs, core * cols, cols, 2)
    rhs_there = swapped(lax.dynamic_slice_in_dim(sub_rhs, (1 - core) * cols, cols, 2))
    rhs = jnp.concatenate([rhs_here, rhs_there], 1).transpose(0, 2, 1)
    mine = (g * nrow + r) * per
    anc_here = lax.dynamic_slice_in_dim(anc_rhs, core * cols + mine, per, 2)
    anc_there = swapped(lax.dynamic_slice_in_dim(anc_rhs, (1 - core) * cols + mine, per, 2))
    anc_given = jnp.concatenate([anc_here, anc_there], 1).transpose(0, 2, 1).astype(F32)
    up_two = (sub_upper, swapped(sub_upper))

    anc_low_row = gathered(anc_lower)
    anc_low = (anc_low_row, swapped(anc_low_row))
    anc_up_row = gathered(anc_upper)
    anc_up = (anc_up_row, swapped(anc_up_row))

    def transposed(two, index, v):
        return dot("rk,ki->ri", v[:, :own], two[0][index]) + dot("rk,ki->ri", v[:, own:], two[1][index])

    def applied(two, index, v):
        return jnp.concatenate([dot("rk,ik->ri", v, part[index]) for part in two], 1)

    def nodes_transposed(two, nodes, v):
        return jnp.stack([transposed(two, m, v[i]) for i, m in enumerate(nodes)])

    leaves = range(1, SUB_NODES)
    y_leaf = summed(nodes_transposed(low_two, leaves, rhs[1:]), "z").astype(BF16)
    y = {m: y_leaf[m - 1] for m in leaves}

    def low_part(m, kind, u):
        p = sub_pairs[m, kind, u]
        return applied(low_two, SUB_NODES + p, y[m] * low_w[p])

    update = sum(low_part(m, 1, 0) for m in leaves)
    residual = (rhs[0].astype(F32) - summed(update, "row")).astype(BF16)
    y[0] = summed(transposed(low_two, 0, residual), "z").astype(BF16)
    to_anc = jnp.stack([sum(low_part(m, 0, e) for m in range(SUB_NODES)) for e in range(levels)])
    to_anc = to_anc.reshape(levels, layers * nrow, per, pair_rows).transpose(1, 0, 2, 3)
    tiles = lax.all_to_all(to_anc.astype(BF16), ("gz", "row"), 0, 0, tiled=True)
    from_layers = jnp.sum(tiles.astype(F32).reshape(layers, nrow, levels, per, pair_rows), 1)
    reached = jnp.sum(choose[:, :, :, None, None] * from_layers[:, :, None], (0, 1))

    acc = [anc_given[a] - reached[a] for a in range(anc_count)]
    anc_y = {}
    for depth in reversed(range(levels)):
        nodes = range(*level_span(depth))
        given = jnp.stack([acc[a] for a in nodes]).astype(BF16)
        solved = summed(nodes_transposed(anc_low, nodes, given), "z").astype(BF16)
        for i, a in enumerate(nodes):
            anc_y[a] = solved[i]
            for u in range(depth):
                acc[above(a, u)] = acc[above(a, u)] - applied(anc_low, anc_pairs[a, u], solved[i])

    anc_z = {}
    anc_rows = {}
    for depth in range(levels):
        nodes = range(*level_span(depth))
        given = []
        for a in nodes:
            t = halves(anc_y[a], 1, z * pair_rows).astype(F32)
            for u in range(depth):
                t = t - applied(anc_up, anc_pairs[a, u], anc_z[above(a, u)])
            given.append(t.astype(BF16))
        solved = summed(nodes_transposed(anc_up, nodes, jnp.stack(given)), "z").astype(BF16)
        for i, a in enumerate(nodes):
            anc_z[a] = solved[i]
    every = jnp.stack([anc_z[a] for a in range(anc_count)])
    every = every.reshape(anc_count, per, nrow, wide).transpose(2, 0, 1, 3)
    every = jnp.broadcast_to(every, (layers, *every.shape)).reshape(-1, anc_count, per, wide)
    tiles = lax.all_to_all(every, ("gz", "row"), 0, 0, tiled=True)
    z_all = tiles.transpose(1, 0, 2, 3).reshape(anc_count, cols, wide)

    def out_slice(array, which):
        return lax.dynamic_slice_in_dim(array, (z * CORES + which) * out_rows, out_rows, 2)

    def joined(here, there):
        pair = jnp.where(core == 0, jnp.stack([here, there]), jnp.stack([there, here]))
        return jnp.concatenate([pair[0], pair[1]], -1)

    out_there = swapped(out_slice(z_all, 1 - core).transpose(0, 2, 1))
    out_here = out_slice(z_all, core).transpose(0, 2, 1)
    anc_out = joined(out_here, out_there).astype(F32)

    picked = dot("ea,ark->erk", choose_here.astype(BF16), z_all).astype(BF16)
    held = (r == z * nrow // nz).astype(F32)
    base = jnp.clip(z * pair_rows - r * wide, 0, wide - pair_rows)

    def up_part(m, kind, u, v):
        p = sub_pairs[m, kind, u]
        return applied(up_two, SUB_NODES + p, v * up_w[p])

    running = []
    for m in range(SUB_NODES):
        part = held * halves(y[m], 1, base).astype(F32)
        running.append(part - sum(up_part(m, 0, e, picked[e]) for e in range(levels)))

    def rows_first(m, v):
        return sum(
            dot("ki,rk->ir", up_two[i][m], v[:, i * own : (i + 1) * own]) for i in range(CORES)
        )

    t_root = summed(running[0], "row").astype(BF16)
    z_root = summed(transposed(up_two, 0, t_root), "z").astype(BF16)
    leaf = jnp.stack([running[m] - up_part(m, 1, 0, z_root) for m in leaves])
    t_leaf = summed(leaf, "row").astype(BF16)
    pieces = jnp.stack([rows_first(0, t_root)] + [rows_first(m, t_leaf[m - 1]) for m in leaves])
    pieces = pieces.astype(BF16).reshape(SUB_NODES, nz * CORES, out_rows, cols).transpose(1, 0, 2, 3)
    tiles = lax.all_to_all(pieces, ("z", "core"), 0, 0, tiled=True)
    owned = jnp.sum(tiles.astype(F32).reshape(nz, CORES, SUB_NODES, out_rows, cols), 0)
    sub_out = jnp.concatenate([owned[0], owned[1]], -1)
    return anc_out, sub_out


def solution(mesh):
    sizes = dict(mesh.shape)
    devices = mesh.devices.reshape(sizes["gz"], sizes["row"], sizes["col"] // CORES, CORES)
    split = Mesh(devices, ("gz", "row", "z", "core"))
    col = ("z", "core")
    in_specs = (
        P(None, col, "row"),
        P(None, col, "row"),
        P("gz", col, "row"),
        P("gz", col, "row"),
        P(None, col, None),
        P("gz", col, None),
        P(),
        P("gz", None),
    )
    out_specs = (P(None, ("row", "z", "core"), None), P("gz", ("row", "z", "core"), None))
    return jax.shard_map(local, mesh=split, in_specs=in_specs, out_specs=out_specs, check_vma=False)
```

```python
import functools

import jax
import jax.numpy as jnp
import numpy as np
from jax import lax
from jax.experimental import pallas as pl
from jax.experimental.pallas import tpu as pltpu
from jax.sharding import Mesh, PartitionSpec as P

SUB_LEVELS = 2
SUB_NODES = 3
LEAVES = (1, 2)
CORES = 2
ROWS8 = 8
F32 = jnp.float32
BF16 = jnp.bfloat16
VMEM_BYTES = 24 * 2**20


def level_span(depth):
    return 2**depth - 1, 2 ** (depth + 1) - 1


def depth_of(node):
    return (node + 1).bit_length() - 1


def above(node, level):
    return ((node + 1) >> (depth_of(node) - level)) - 1


def swapped(array):
    return lax.ppermute(array, "core", [(0, 1), (1, 0)])


def shape(dtype, *dims):
    return jax.ShapeDtypeStruct(dims, dtype)


def run(body, outs, smem, vmem, scratch=()):
    in_specs = [pl.BlockSpec(memory_space=pltpu.SMEM)] * len(smem)
    in_specs += [pl.BlockSpec(memory_space=pltpu.VMEM)] * len(vmem)
    single = not isinstance(outs, (list, tuple))
    spec = pl.BlockSpec(memory_space=pltpu.VMEM)
    return pl.pallas_call(
        body,
        out_shape=outs,
        in_specs=in_specs,
        out_specs=spec if single else [spec] * len(outs),
        scratch_shapes=list(scratch),
        compiler_params=pltpu.CompilerParams(vmem_limit_bytes=VMEM_BYTES),
    )(*smem, *vmem)


def total(tiles_ref):
    value = tiles_ref[0].astype(F32)
    for i in range(1, tiles_ref.shape[0]):
        value = value + tiles_ref[i].astype(F32)
    return value


def to_all(out_ref, value):
    value = value.astype(out_ref.dtype)
    for i in range(out_ref.shape[0]):
        out_ref[i] = value


def block(own_ref, other_ref, index):
    return jnp.concatenate([own_ref[index], other_ref[index]], 0)


def times(v, matrix):
    return lax.dot_general(v, matrix, (((1,), (0,)), ((), ())), preferred_element_type=F32)


def times_t(v, matrix):
    return lax.dot_general(v, matrix, (((1,), (1,)), ((), ())), preferred_element_type=F32)


def in_row(v, row):
    rows = lax.broadcasted_iota(jnp.int32, v.shape, 0)
    return jnp.where(rows == row, v, 0.0)


def own_first(v, core):
    return jnp.where(core == 1, pltpu.roll(v, v.shape[1] // 2, 1), v)


class Pairs:
    def __init__(self, levels, anc_count):
        self.sub = {}
        for m in range(SUB_NODES):
            for kind, count in ((0, levels), (1, depth_of(m))):
                for u in range(count):
                    self.sub[m, kind, u] = len(self.sub)
        self.anc = {}
        for a in range(anc_count):
            for u in range(depth_of(a)):
                self.anc[a, u] = anc_count + len(self.anc)


def sub_leaf_solve(rhs, own, other, out):
    for m in LEAVES:
        part = times(rhs[m], block(own, other, m)).astype(BF16)
        for i in range(out.shape[0]):
            out[i, m - 1] = part


def sub_low(y, w, pairs, own, other, m, kind, u):
    p = pairs.sub[m, kind, u]
    return w[p] * times_t(y, block(own, other, SUB_NODES + p))


def sub_leaf_update(pairs, w, tiles, own, other, y_out, out):
    y = total(tiles).astype(BF16)
    y_out[...] = y
    value = sum(sub_low(y[m - 1], w, pairs, own, other, m, 1, 0) for m in LEAVES)
    to_all(out, value)


def sub_leaf_anc(pairs, levels, w, y, own, other, out):
    for e in range(levels):
        out[e] = sum(sub_low(y[m - 1], w, pairs, own, other, m, 0, e) for m in LEAVES)


def sub_root_solve(tiles, rhs, own, other, out):
    given = (rhs[0].astype(F32) - total(tiles)).astype(BF16)
    to_all(out, times(given, block(own, other, 0)))


def sub_root_anc(pairs, levels, w, tiles, so_far, own, other, y_out, out):
    y = total(tiles).astype(BF16)
    y_out[...] = y
    out[...] = jnp.zeros_like(out)
    for e in range(levels):
        out[:, e, :] = so_far[e] + sub_low(y, w, pairs, own, other, 0, 0, e)


def solve_level(pairs, depth, v8, own, other, out, scratch):
    first, stop = level_span(depth)
    value = jnp.zeros_like(scratch)
    for i, a in enumerate(range(first, stop)):
        value = value + in_row(times(v8, block(own, other, i)), a)
    scratch[...] = value
    to_all(out, scratch[first : first + out.shape[1], :])


def anc_first(pairs, depth, tiles, choose, given, own, other, acc_out, out, scratch):
    acc = given[...]
    for e in range(choose.shape[0]):
        acc = acc - lax.dot_general(
            choose[e],
            tiles[:, e, :],
            (((1,), (0,)), ((), ())),
            precision=lax.Precision.HIGHEST,
            preferred_element_type=F32,
        )
    acc_out[...] = acc
    solve_level(pairs, depth, acc.astype(BF16), own, other, out, scratch)


def anc_forward(pairs, depth, tiles, y_in, acc_in, low, low_x, own, other, y_out, acc_out, out, scratch):
    first, stop = level_span(depth)
    y_out[...] = y_in[...]
    y_out[first:stop, :] = total(tiles)[: stop - first].astype(BF16).astype(F32)
    acc = acc_in[...]
    start = pairs.anc[first, 0]
    for d in range(first, stop):
        y = jnp.broadcast_to(y_out[d : d + 1, :], y_out.shape)
        for u in range(depth):
            v = in_row(y, above(d, u)).astype(BF16)
            acc = acc - times_t(v, block(low, low_x, pairs.anc[d, u] - start))
    acc_out[...] = acc
    solve_level(pairs, depth - 1, acc.astype(BF16), own, other, out, scratch)


def anc_turn(pairs, where, tiles, y_in, own, other, y_out, out, scratch):
    core, z = where[0], where[1]
    y_out[...] = y_in[...]
    y_out[0:1, :] = total(tiles)[:1].astype(BF16).astype(F32)
    pair_rows = own.shape[1] * CORES
    t = own_first(y_out[:, pl.ds(pl.multiple_of(z * pair_rows, pair_rows), pair_rows)], core)
    solve_level(pairs, 0, t.astype(BF16), own, other, out, scratch)


def anc_backward(pairs, depth, where, tiles, z_in, y_in, up, up_x, own, other, z_out, out, scratch):
    core, z = where[0], where[1]
    first, stop = level_span(depth - 1)
    z_out[...] = z_in[...]
    z_out[first:stop, :] = total(tiles)[: stop - first].astype(BF16).astype(F32)
    pair_rows = own.shape[1] * CORES
    acc = own_first(y_in[:, pl.ds(pl.multiple_of(z * pair_rows, pair_rows), pair_rows)], core)
    first, stop = level_span(depth)
    start = pairs.anc[first, 0]
    for a in range(first, stop):
        for u in range(depth):
            q = above(a, u)
            v = in_row(jnp.broadcast_to(z_out[q : q + 1, :], z_out.shape), a).astype(BF16)
            acc = acc - times_t(v, block(up, up_x, pairs.anc[a, u] - start))
    solve_level(pairs, depth, acc.astype(BF16), own, other, out, scratch)


def anc_spread(depth, nrow, tiles, z_in, out, scratch):
    first, stop = level_span(depth)
    scratch[...] = z_in[...]
    scratch[first:stop, :] = total(tiles)
    wide = out.shape[2]
    for i in range(out.shape[0]):
        r = i % nrow
        out[i] = scratch[:, r * wide : (r + 1) * wide].astype(BF16)


def sub_turn(pairs, levels, where, ids, w, tiles, y_root, y_leaf, own, other, kept, out, scratch):
    core, held, base = where[0], where[3], where[4]
    scratch[...] = tiles[...].astype(F32)
    picked = []
    for e in range(levels):
        value = 0.0
        for a in range(*level_span(e)):
            value = value + jnp.where(ids[e] == a, 1.0, 0.0) * scratch[:, a, :]
        picked.append(value.astype(BF16))
    pair_rows = own.shape[1] * CORES
    scale = held.astype(F32)
    for m in range(SUB_NODES):
        span = pl.ds(pl.multiple_of(base, pair_rows), pair_rows)
        y = y_root[:, span] if m == 0 else y_leaf[m - 1, :, span]
        value = scale * own_first(y.astype(F32), core)
        for e in range(levels):
            p = pairs.sub[m, 0, e]
            value = value - w[p] * times_t(picked[e], block(own, other, SUB_NODES + p))
        if m == 0:
            to_all(out, value)
        else:
            kept[m - 1] = value


def sub_root_back(tiles, own, other, kept, out):
    value = times(total(tiles).astype(BF16), block(own, other, 0))
    kept[...] = value
    to_all(out, value)


def sub_leaf_back(pairs, w, tiles, kept, own, other, out):
    z = total(tiles).astype(BF16)
    for m in LEAVES:
        p = pairs.sub[m, 1, 0]
        value = kept[m - 1] - w[p] * times_t(z, block(own, other, SUB_NODES + p))
        for i in range(out.shape[0]):
            out[i, m - 1] = value.astype(BF16)


def sub_finish(tiles, root, own, other, out):
    t = total(tiles).astype(BF16)
    parts = [root[...]] + [times(t[m - 1], block(own, other, m)) for m in LEAVES]
    fill = out.shape[2] - sum(part.shape[0] for part in parts)
    if fill:
        parts.append(jnp.zeros((fill, parts[0].shape[1]), F32))
    flipped = jnp.concatenate(parts, 0).T
    out[...] = flipped.reshape(out.shape).astype(BF16)


def local(anc_lower, anc_upper, sub_lower, sub_upper, anc_rhs, sub_rhs, layer_subtree, sub_pattern):
    layers = lax.axis_size("gz")
    levels = layers.bit_length() - 1
    anc_count = layers - 1
    nrow, nz = lax.axis_size("row"), lax.axis_size("z")
    own, wide = sub_lower.shape[1:]
    size = wide * nrow
    pair_rows = own * CORES
    out_rows = wide // (nz * CORES)
    cols = sub_rhs.shape[2] // CORES
    g, r, z, core = (lax.axis_index(name) for name in ("gz", "row", "z", "core"))
    pairs = Pairs(levels, anc_count)
    part = functools.partial
    scr8 = pltpu.VMEM((ROWS8, size), F32)

    low_w = sub_pattern[:, 0].astype(F32)
    up_w = sub_pattern[:, 1].astype(F32)
    powers = jnp.asarray(2 ** (levels - np.arange(levels)), jnp.int32)
    heap_ids = (layer_subtree[:, None] + layers) // powers[None, :] - 1
    nodes = jnp.arange(ROWS8, dtype=jnp.int32)
    choose = (heap_ids.T[:, None, :] == nodes[None, :, None]).astype(F32)
    choose = jnp.repeat(choose, nrow, axis=2)
    ids_here = lax.dynamic_index_in_dim(heap_ids, g, 0, keepdims=False)
    held = (r == z * nrow // nz).astype(jnp.int32)
    base = jnp.clip(z * pair_rows - r * wide, 0, wide - pair_rows)
    where = jnp.stack([core, z, jnp.int32(nz), held, base]).astype(jnp.int32)

    def gathered(blocks):
        return lax.all_gather(blocks, "row", axis=2, tiled=True)

    def exchange(array, axes):
        return lax.all_to_all(array, axes, 0, 0, tiled=True)

    low = (sub_lower, swapped(sub_lower))
    rhs_here = lax.dynamic_slice_in_dim(sub_rhs, core * cols, cols, 2)
    rhs_there = swapped(lax.dynamic_slice_in_dim(sub_rhs, (1 - core) * cols, cols, 2))
    rhs = jnp.concatenate([rhs_here, rhs_there], 1).transpose(0, 2, 1)
    mine = g * nrow + r
    anc_here = lax.dynamic_slice_in_dim(anc_rhs, core * cols + mine, 1, 2)
    anc_there = swapped(lax.dynamic_slice_in_dim(anc_rhs, (1 - core) * cols + mine, 1, 2))
    given8 = jnp.concatenate([anc_here, anc_there], 1)[:, :, 0].astype(F32)
    given8 = jnp.pad(given8, ((0, ROWS8 - anc_count), (0, 0)))
    up = (sub_upper, swapped(sub_upper))
    anc_low_row = gathered(anc_lower)
    anc_low = (anc_low_row, swapped(anc_low_row))
    anc_up_row = gathered(anc_upper)
    anc_up = (anc_up_row, swapped(anc_up_row))

    def diagonal(two, depth):
        first, stop = level_span(depth)
        return [array[first:stop] for array in two]

    def pair_blocks(two, depth):
        first, stop = level_span(depth)
        start = pairs.anc[first, 0]
        return [array[start : start + (stop - first) * depth] for array in two]

    def level_shape(depth):
        return shape(BF16, nz, max(2, 2**depth), size)

    tiles = run(sub_leaf_solve, shape(BF16, nz, 2, cols, wide), (), (rhs, *low))
    tiles = exchange(tiles, "z")
    y_leaf, tiles = run(
        part(sub_leaf_update, pairs),
        (shape(BF16, 2, cols, wide), shape(BF16, nrow, cols, pair_rows)),
        (low_w,),
        (tiles, *low),
    )
    tiles = exchange(tiles, "row")
    so_far = run(
        part(sub_leaf_anc, pairs, levels),
        shape(F32, levels, cols, pair_rows),
        (low_w,),
        (y_leaf, *low),
    )
    tiles = run(sub_root_solve, shape(BF16, nz, cols, wide), (), (tiles, rhs, *low))
    tiles = exchange(tiles, "z")
    y_root, tiles = run(
        part(sub_root_anc, pairs, levels),
        (shape(BF16, cols, wide), shape(F32, cols, ROWS8, pair_rows)),
        (low_w,),
        (tiles, so_far, *low),
    )
    tiles = exchange(tiles, ("gz", "row"))

    y8 = jnp.zeros((ROWS8, size), F32)
    acc, tiles = run(
        part(anc_first, pairs, levels - 1),
        (shape(F32, ROWS8, pair_rows), level_shape(levels - 1)),
        (),
        (tiles, choose, given8, *diagonal(anc_low, levels - 1)),
        (scr8,),
    )
    tiles = exchange(tiles, "z")
    for depth in range(levels - 1, 0, -1):
        y8, acc, tiles = run(
            part(anc_forward, pairs, depth),
            (shape(F32, ROWS8, size), shape(F32, ROWS8, pair_rows), level_shape(depth - 1)),
            (),
            (tiles, y8, acc, *pair_blocks(anc_low, depth), *diagonal(anc_low, depth - 1)),
            (scr8,),
        )
        tiles = exchange(tiles, "z")
    y8, tiles = run(
        part(anc_turn, pairs),
        (shape(F32, ROWS8, size), level_shape(0)),
        (where,),
        (tiles, y8, *diagonal(anc_up, 0)),
        (scr8,),
    )
    tiles = exchange(tiles, "z")
    z8 = jnp.zeros((ROWS8, size), F32)
    for depth in range(1, levels):
        z8, tiles = run(
            part(anc_backward, pairs, depth),
            (shape(F32, ROWS8, size), level_shape(depth)),
            (where,),
            (tiles, z8, y8, *pair_blocks(anc_up, depth), *diagonal(anc_up, depth)),
            (scr8,),
        )
        tiles = exchange(tiles, "z")
    tiles = run(
        part(anc_spread, levels - 1, nrow),
        shape(BF16, layers * nrow, ROWS8, wide),
        (),
        (tiles, z8),
        (scr8,),
    )
    z_all = exchange(tiles, ("gz", "row"))

    kept, tiles = run(
        part(sub_turn, pairs, levels),
        (shape(F32, 2, cols, pair_rows), shape(BF16, nrow, cols, pair_rows)),
        (where, ids_here, up_w),
        (z_all, y_root, y_leaf, *up),
        (pltpu.VMEM(z_all.shape, F32),),
    )
    tiles = exchange(tiles, "row")

    def out_slice(which):
        start = (z * CORES + which) * out_rows
        return lax.dynamic_slice_in_dim(z_all, start, out_rows, 2)[:, :anc_count].transpose(1, 2, 0)

    def joined(here, there):
        flipped = core == 1
        return jnp.concatenate([jnp.where(flipped, there, here), jnp.where(flipped, here, there)], -1)

    anc_out = joined(out_slice(core), swapped(out_slice(1 - core))).astype(F32)

    root, tiles = run(
        sub_root_back,
        (shape(F32, cols, wide), shape(BF16, nz, cols, wide)),
        (),
        (tiles, *up),
    )
    tiles = exchange(tiles, "z")
    tiles = run(
        part(sub_leaf_back, pairs),
        shape(BF16, nrow, 2, cols, pair_rows),
        (up_w,),
        (tiles, kept, *up),
    )
    tiles = exchange(tiles, "row")
    packed = -(-SUB_NODES * cols // 128) * 128
    tiles = run(
        sub_finish,
        shape(BF16, nz * CORES, out_rows, packed),
        (),
        (tiles, root, *up),
    )
    tiles = exchange(tiles, ("z", "core"))
    sums = jnp.sum(tiles.astype(F32).reshape(nz, CORES, out_rows, packed), 0)
    sums = sums[:, :, : SUB_NODES * cols].reshape(CORES, out_rows, SUB_NODES, cols)
    sub_out = sums.transpose(2, 1, 0, 3).reshape(SUB_NODES, out_rows, CORES * cols)
    return anc_out, sub_out


def solution(mesh):
    sizes = dict(mesh.shape)
    devices = mesh.devices.reshape(sizes["gz"], sizes["row"], sizes["col"] // CORES, CORES)
    split = Mesh(devices, ("gz", "row", "z", "core"))
    col = ("z", "core")
    in_specs = (
        P(None, col, "row"),
        P(None, col, "row"),
        P("gz", col, "row"),
        P("gz", col, "row"),
        P(None, col, None),
        P("gz", col, None),
        P(),
        P("gz", None),
    )
    out_specs = (P(None, ("row", "z", "core"), None), P("gz", ("row", "z", "core"), None))
    return jax.shard_map(local, mesh=split, in_specs=in_specs, out_specs=out_specs, check_vma=False)
```

```python
import functools

import jax
import jax.numpy as jnp
import numpy as np
from jax import lax
from jax.experimental import pallas as pl
from jax.experimental.pallas import tpu as pltpu
from jax.sharding import Mesh, PartitionSpec as P

SUB_LEVELS = 2
SUB_NODES = 3
LEAVES = (1, 2)
CORES = 2
ROWS8 = 8
F32 = jnp.float32
BF16 = jnp.bfloat16
VMEM_BYTES = 12 * 2**20


def level_span(depth):
    return 2**depth - 1, 2 ** (depth + 1) - 1


def depth_of(node):
    return (node + 1).bit_length() - 1


def above(node, level):
    return ((node + 1) >> (depth_of(node) - level)) - 1


def swapped(array):
    return lax.ppermute(array, "core", [(0, 1), (1, 0)])


def shape(dtype, *dims):
    return jax.ShapeDtypeStruct(dims, dtype)


def run(body, outs, smem, vmem, scratch=()):
    in_specs = [pl.BlockSpec(memory_space=pltpu.SMEM)] * len(smem)
    in_specs += [pl.BlockSpec(memory_space=pltpu.VMEM)] * len(vmem)
    single = not isinstance(outs, (list, tuple))
    spec = pl.BlockSpec(memory_space=pltpu.VMEM)
    return pl.pallas_call(
        body,
        out_shape=outs,
        in_specs=in_specs,
        out_specs=spec if single else [spec] * len(outs),
        scratch_shapes=list(scratch),
        compiler_params=pltpu.CompilerParams(vmem_limit_bytes=VMEM_BYTES),
    )(*smem, *vmem)


def total(tiles_ref):
    value = tiles_ref[0].astype(F32)
    for i in range(1, tiles_ref.shape[0]):
        value = value + tiles_ref[i].astype(F32)
    return value


def to_all(out_ref, value):
    value = value.astype(out_ref.dtype)
    for i in range(out_ref.shape[0]):
        out_ref[i] = value


def block(own_ref, other_ref, index):
    return jnp.concatenate([own_ref[index], other_ref[index]], 0)


def times(v, matrix):
    return lax.dot_general(v, matrix, (((1,), (0,)), ((), ())), preferred_element_type=F32)


def times_t(v, matrix):
    return lax.dot_general(v, matrix, (((1,), (1,)), ((), ())), preferred_element_type=F32)


def in_row(v, row):
    rows = lax.broadcasted_iota(jnp.int32, v.shape, 0)
    return jnp.where(rows == row, v, 0.0)


def own_first(v, core):
    return jnp.where(core == 1, pltpu.roll(v, v.shape[1] // 2, 1), v)


class Pairs:
    def __init__(self, levels, anc_count):
        self.sub = {}
        for m in range(SUB_NODES):
            for kind, count in ((0, levels), (1, depth_of(m))):
                for u in range(count):
                    self.sub[m, kind, u] = len(self.sub)
        self.anc = {}
        for a in range(anc_count):
            for u in range(depth_of(a)):
                self.anc[a, u] = anc_count + len(self.anc)


def sub_leaf_solve(where, here, there, own, other, rhs, out):
    core = where[0]
    cols = rhs.shape[1]
    for m in range(SUB_NODES):
        flipped = jnp.concatenate([here[m], there[m]], 0).astype(F32).T
        rhs[m] = jnp.where(core == 0, flipped[:cols], flipped[cols:]).astype(BF16)
    for m in LEAVES:
        part = times(rhs[m], block(own, other, m)).astype(BF16)
        for i in range(out.shape[0]):
            out[i, m - 1] = part


def sub_low(y, w, pairs, own, other, m, kind, u):
    p = pairs.sub[m, kind, u]
    return w[p] * times_t(y, block(own, other, SUB_NODES + p))


def sub_leaf_update(pairs, w, tiles, own, other, y_out, out):
    y = total(tiles).astype(BF16)
    y_out[...] = y
    value = sum(sub_low(y[m - 1], w, pairs, own, other, m, 1, 0) for m in LEAVES)
    to_all(out, value)


def sub_leaf_anc(pairs, levels, w, y, own, other, out):
    for e in range(levels):
        out[e] = sum(sub_low(y[m - 1], w, pairs, own, other, m, 0, e) for m in LEAVES)


def sub_root_solve(tiles, rhs, own, other, out):
    given = (rhs[0].astype(F32) - total(tiles)).astype(BF16)
    to_all(out, times(given, block(own, other, 0)))


def sub_root_anc(pairs, levels, w, tiles, so_far, own, other, y_out, out):
    y = total(tiles).astype(BF16)
    y_out[...] = y
    out[...] = jnp.zeros_like(out)
    for e in range(levels):
        out[:, e, :] = so_far[e] + sub_low(y, w, pairs, own, other, 0, 0, e)


def solve_level(pairs, depth, v8, own, other, out, scratch):
    first, stop = level_span(depth)
    value = jnp.zeros_like(scratch)
    for i, a in enumerate(range(first, stop)):
        value = value + in_row(times(v8, block(own, other, i)), a)
    scratch[...] = value
    to_all(out, scratch[first : first + out.shape[1], :])


def anc_prepare(where, here, there, out):
    lanes = lax.broadcasted_iota(jnp.int32, (ROWS8, here.shape[2]), 1)
    pick = jnp.where(lanes == where[5], 1.0, 0.0).astype(BF16)
    value = jnp.zeros_like(out)
    for a in range(here.shape[0]):
        value = value + in_row(times_t(pick, block(here, there, a)), a)
    out[...] = value


def anc_first(pairs, depth, tiles, choose, given, own, other, acc_out, out, scratch):
    acc = given[...]
    for e in range(choose.shape[0]):
        acc = acc - lax.dot_general(
            choose[e],
            tiles[:, e, :],
            (((1,), (0,)), ((), ())),
            precision=lax.Precision.HIGHEST,
            preferred_element_type=F32,
        )
    acc_out[...] = acc
    solve_level(pairs, depth, acc.astype(BF16), own, other, out, scratch)


def anc_forward(pairs, depth, tiles, y_in, acc_in, low, low_x, own, other, y_out, acc_out, out, scratch):
    first, stop = level_span(depth)
    y_out[...] = y_in[...]
    y_out[first:stop, :] = total(tiles)[: stop - first].astype(BF16).astype(F32)
    acc = acc_in[...]
    start = pairs.anc[first, 0]
    for d in range(first, stop):
        y = jnp.broadcast_to(y_out[d : d + 1, :], y_out.shape)
        for u in range(depth):
            v = in_row(y, above(d, u)).astype(BF16)
            acc = acc - times_t(v, block(low, low_x, pairs.anc[d, u] - start))
    acc_out[...] = acc
    solve_level(pairs, depth - 1, acc.astype(BF16), own, other, out, scratch)


def anc_turn(pairs, where, tiles, y_in, own, other, y_out, out, scratch):
    core, z = where[0], where[1]
    y_out[...] = y_in[...]
    y_out[0:1, :] = total(tiles)[:1].astype(BF16).astype(F32)
    pair_rows = own.shape[1] * CORES
    t = own_first(y_out[:, pl.ds(pl.multiple_of(z * pair_rows, pair_rows), pair_rows)], core)
    solve_level(pairs, 0, t.astype(BF16), own, other, out, scratch)


def anc_backward(pairs, depth, where, tiles, z_in, y_in, up, up_x, own, other, z_out, out, scratch):
    core, z = where[0], where[1]
    first, stop = level_span(depth - 1)
    z_out[...] = z_in[...]
    z_out[first:stop, :] = total(tiles)[: stop - first].astype(BF16).astype(F32)
    pair_rows = own.shape[1] * CORES
    acc = own_first(y_in[:, pl.ds(pl.multiple_of(z * pair_rows, pair_rows), pair_rows)], core)
    first, stop = level_span(depth)
    start = pairs.anc[first, 0]
    for a in range(first, stop):
        for u in range(depth):
            q = above(a, u)
            v = in_row(jnp.broadcast_to(z_out[q : q + 1, :], z_out.shape), a).astype(BF16)
            acc = acc - times_t(v, block(up, up_x, pairs.anc[a, u] - start))
    solve_level(pairs, depth, acc.astype(BF16), own, other, out, scratch)


def anc_spread(depth, nrow, tiles, z_in, out, scratch):
    first, stop = level_span(depth)
    scratch[...] = z_in[...]
    scratch[first:stop, :] = total(tiles)
    wide = out.shape[2]
    for i in range(out.shape[0]):
        r = i % nrow
        out[i] = scratch[:, r * wide : (r + 1) * wide].astype(BF16)


def sub_turn(pairs, levels, where, ids, w, tiles, y_root, y_leaf, own, other, kept, out, scratch):
    core, held, base = where[0], where[2], where[3]
    scratch[...] = tiles[...].astype(F32)
    picked = []
    for e in range(levels):
        value = 0.0
        for a in range(*level_span(e)):
            value = value + jnp.where(ids[e] == a, 1.0, 0.0) * scratch[:, a, :]
        picked.append(value.astype(BF16))
    pair_rows = own.shape[1] * CORES
    scale = held.astype(F32)
    for m in range(SUB_NODES):
        span = pl.ds(pl.multiple_of(base, pair_rows), pair_rows)
        y = y_root[:, span] if m == 0 else y_leaf[m - 1, :, span]
        value = scale * own_first(y.astype(F32), core)
        for e in range(levels):
            p = pairs.sub[m, 0, e]
            value = value - w[p] * times_t(picked[e], block(own, other, SUB_NODES + p))
        if m == 0:
            to_all(out, value)
        else:
            kept[m - 1] = value


def sub_root_back(tiles, own, other, kept, out):
    value = times(total(tiles).astype(BF16), block(own, other, 0))
    kept[...] = value
    to_all(out, value)


def sub_leaf_back(pairs, w, tiles, kept, own, other, out):
    z = total(tiles).astype(BF16)
    for m in LEAVES:
        p = pairs.sub[m, 1, 0]
        value = kept[m - 1] - w[p] * times_t(z, block(own, other, SUB_NODES + p))
        for i in range(out.shape[0]):
            out[i, m - 1] = value.astype(BF16)


def sub_finish(tiles, root, own, other, out):
    t = total(tiles).astype(BF16)
    parts = [root[...]] + [times(t[m - 1], block(own, other, m)) for m in LEAVES]
    fill = out.shape[2] - sum(part.shape[0] for part in parts)
    if fill:
        parts.append(jnp.zeros((fill, parts[0].shape[1]), F32))
    flipped = jnp.concatenate(parts, 0).T
    out[...] = flipped.reshape(out.shape).astype(BF16)


def local(anc_lower, anc_upper, sub_lower, sub_upper, anc_rhs, sub_rhs, layer_subtree, sub_pattern):
    layers = lax.axis_size("gz")
    levels = layers.bit_length() - 1
    anc_count = layers - 1
    nrow, nz = lax.axis_size("row"), lax.axis_size("z")
    own, wide = sub_lower.shape[1:]
    size = wide * nrow
    pair_rows = own * CORES
    out_rows = wide // (nz * CORES)
    cols = sub_rhs.shape[2] // CORES
    g, r, z, core = (lax.axis_index(name) for name in ("gz", "row", "z", "core"))
    pairs = Pairs(levels, anc_count)
    part = functools.partial
    scr8 = pltpu.VMEM((ROWS8, size), F32)

    low_w = sub_pattern[:, 0].astype(F32)
    up_w = sub_pattern[:, 1].astype(F32)
    powers = jnp.asarray(2 ** (levels - np.arange(levels)), jnp.int32)
    heap_ids = (layer_subtree[:, None] + layers) // powers[None, :] - 1
    nodes = jnp.arange(ROWS8, dtype=jnp.int32)
    choose = (heap_ids.T[:, None, :] == nodes[None, :, None]).astype(F32)
    choose = jnp.repeat(choose, nrow, axis=2)
    ids_here = lax.dynamic_index_in_dim(heap_ids, g, 0, keepdims=False)
    held = (r == z * nrow // nz).astype(jnp.int32)
    base = jnp.clip(z * pair_rows - r * wide, 0, wide - pair_rows)
    where = jnp.stack([core, z, held, base, jnp.int32(0), core * cols + g * nrow + r]).astype(jnp.int32)

    def gathered(blocks):
        return lax.all_gather(blocks, "row", axis=2, tiled=True)

    def exchange(array, axes):
        return lax.all_to_all(array, axes, 0, 0, tiled=True)

    low = (sub_lower, swapped(sub_lower))
    rhs_there = swapped(sub_rhs)
    anc_there = swapped(anc_rhs)
    up = (sub_upper, swapped(sub_upper))
    anc_low_row = gathered(anc_lower)
    anc_up_row = gathered(anc_upper)

    def diagonal(two, depth):
        first, stop = level_span(depth)
        return [array[first:stop] for array in two]

    def pair_blocks(two, depth):
        first, stop = level_span(depth)
        start = pairs.anc[first, 0]
        return [array[start : start + (stop - first) * depth] for array in two]

    def level_shape(depth):
        return shape(BF16, nz, max(2, 2**depth), size)

    rhs, tiles = run(
        sub_leaf_solve,
        (shape(BF16, SUB_NODES, cols, pair_rows), shape(BF16, nz, 2, cols, wide)),
        (where,),
        (sub_rhs, rhs_there, *low),
    )
    tiles = exchange(tiles, "z")
    y_leaf, tiles = run(
        part(sub_leaf_update, pairs),
        (shape(BF16, 2, cols, wide), shape(BF16, nrow, cols, pair_rows)),
        (low_w,),
        (tiles, *low),
    )
    tiles = exchange(tiles, "row")
    so_far = run(
        part(sub_leaf_anc, pairs, levels),
        shape(F32, levels, cols, pair_rows),
        (low_w,),
        (y_leaf, *low),
    )
    tiles = run(sub_root_solve, shape(BF16, nz, cols, wide), (), (tiles, rhs, *low))
    tiles = exchange(tiles, "z")
    anc_low_row, tiles = lax.optimization_barrier((anc_low_row, tiles))
    anc_low = (anc_low_row, swapped(anc_low_row))
    given8 = run(anc_prepare, shape(F32, ROWS8, pair_rows), (where,), (anc_rhs, anc_there))
    y_root, tiles = run(
        part(sub_root_anc, pairs, levels),
        (shape(BF16, cols, wide), shape(F32, cols, ROWS8, pair_rows)),
        (low_w,),
        (tiles, so_far, *low),
    )
    tiles = exchange(tiles, ("gz", "row"))

    y8 = jnp.zeros((ROWS8, size), F32)
    acc, tiles = run(
        part(anc_first, pairs, levels - 1),
        (shape(F32, ROWS8, pair_rows), level_shape(levels - 1)),
        (),
        (tiles, choose, given8, *diagonal(anc_low, levels - 1)),
        (scr8,),
    )
    tiles = exchange(tiles, "z")
    for depth in range(levels - 1, 0, -1):
        if depth == 1:
            anc_up_row, tiles = lax.optimization_barrier((anc_up_row, tiles))
            anc_up = (anc_up_row, swapped(anc_up_row))
        y8, acc, tiles = run(
            part(anc_forward, pairs, depth),
            (shape(F32, ROWS8, size), shape(F32, ROWS8, pair_rows), level_shape(depth - 1)),
            (),
            (tiles, y8, acc, *pair_blocks(anc_low, depth), *diagonal(anc_low, depth - 1)),
            (scr8,),
        )
        tiles = exchange(tiles, "z")
    y8, tiles = run(
        part(anc_turn, pairs),
        (shape(F32, ROWS8, size), level_shape(0)),
        (where,),
        (tiles, y8, *diagonal(anc_up, 0)),
        (scr8,),
    )
    tiles = exchange(tiles, "z")
    z8 = jnp.zeros((ROWS8, size), F32)
    for depth in range(1, levels):
        z8, tiles = run(
            part(anc_backward, pairs, depth),
            (shape(F32, ROWS8, size), level_shape(depth)),
            (where,),
            (tiles, z8, y8, *pair_blocks(anc_up, depth), *diagonal(anc_up, depth)),
            (scr8,),
        )
        tiles = exchange(tiles, "z")
    tiles = run(
        part(anc_spread, levels - 1, nrow),
        shape(BF16, layers * nrow, ROWS8, wide),
        (),
        (tiles, z8),
        (scr8,),
    )
    z_all = exchange(tiles, ("gz", "row"))

    kept, tiles = run(
        part(sub_turn, pairs, levels),
        (shape(F32, 2, cols, pair_rows), shape(BF16, nrow, cols, pair_rows)),
        (where, ids_here, up_w),
        (z_all, y_root, y_leaf, *up),
        (pltpu.VMEM(z_all.shape, F32),),
    )
    tiles = exchange(tiles, "row")

    def out_slice(which):
        start = (z * CORES + which) * out_rows
        return lax.dynamic_slice_in_dim(z_all, start, out_rows, 2)[:, :anc_count].transpose(1, 2, 0)

    def joined(here, there):
        flipped = core == 1
        return jnp.concatenate([jnp.where(flipped, there, here), jnp.where(flipped, here, there)], -1)

    anc_out = joined(out_slice(core), swapped(out_slice(1 - core))).astype(F32)

    root, tiles = run(
        sub_root_back,
        (shape(F32, cols, wide), shape(BF16, nz, cols, wide)),
        (),
        (tiles, *up),
    )
    tiles = exchange(tiles, "z")
    tiles = run(
        part(sub_leaf_back, pairs),
        shape(BF16, nrow, 2, cols, pair_rows),
        (up_w,),
        (tiles, kept, *up),
    )
    tiles = exchange(tiles, "row")
    packed = -(-SUB_NODES * cols // 128) * 128
    tiles = run(
        sub_finish,
        shape(BF16, nz * CORES, out_rows, packed),
        (),
        (tiles, root, *up),
    )
    tiles = exchange(tiles, ("z", "core"))
    sums = jnp.sum(tiles.astype(F32).reshape(nz, CORES, out_rows, packed), 0)
    sums = sums[:, :, : SUB_NODES * cols].reshape(CORES, out_rows, SUB_NODES, cols)
    sub_out = sums.transpose(2, 1, 0, 3).reshape(SUB_NODES, out_rows, CORES * cols)
    return anc_out, sub_out


def solution(mesh):
    sizes = dict(mesh.shape)
    devices = mesh.devices.reshape(sizes["gz"], sizes["row"], sizes["col"] // CORES, CORES)
    split = Mesh(devices, ("gz", "row", "z", "core"))
    col = ("z", "core")
    in_specs = (
        P(None, col, "row"),
        P(None, col, "row"),
        P("gz", col, "row"),
        P("gz", col, "row"),
        P(None, col, None),
        P("gz", col, None),
        P(),
        P("gz", None),
    )
    out_specs = (P(None, ("row", "z", "core"), None), P("gz", ("row", "z", "core"), None))
    return jax.shard_map(local, mesh=split, in_specs=in_specs, out_specs=out_specs, check_vma=False)
```

```python
import functools

import jax
import jax.numpy as jnp
import numpy as np
from jax import lax
from jax.experimental import pallas as pl
from jax.experimental.pallas import tpu as pltpu
from jax.sharding import Mesh, PartitionSpec as P


SUB_NODES = 3
LEAVES = (1, 2)
CORES = 2
ROWS8 = 8
F32 = jnp.float32
BF16 = jnp.bfloat16
VMEM_BYTES = 12 * 2**20


def level_span(depth):
    return 2**depth - 1, 2 ** (depth + 1) - 1


def depth_of(node):
    return (node + 1).bit_length() - 1


def above(node, level):
    return ((node + 1) >> (depth_of(node) - level)) - 1


def swapped(array):
    return lax.ppermute(array, "core", [(0, 1), (1, 0)])


def shape(dtype, *dims):
    return jax.ShapeDtypeStruct(dims, dtype)


def run(body, outs, smem, vmem, scratch=(), far=()):
    in_specs = [pl.BlockSpec(memory_space=pltpu.SMEM)] * len(smem)
    in_specs += [pl.BlockSpec(memory_space=pltpu.VMEM)] * len(vmem)
    in_specs += [pl.BlockSpec(memory_space=pltpu.HBM)] * len(far)
    far = [pltpu.with_memory_space_constraint(array, pltpu.HBM) for array in far]
    single = not isinstance(outs, (list, tuple))
    spec = pl.BlockSpec(memory_space=pltpu.VMEM)
    return pl.pallas_call(
        body,
        out_shape=outs,
        in_specs=in_specs,
        out_specs=spec if single else [spec] * len(outs),
        scratch_shapes=list(scratch),
        compiler_params=pltpu.CompilerParams(vmem_limit_bytes=VMEM_BYTES),
    )(*smem, *vmem, *far)


def total(tiles_ref):
    value = tiles_ref[0].astype(F32)
    for i in range(1, tiles_ref.shape[0]):
        value = value + tiles_ref[i].astype(F32)
    return value


def to_all(out_ref, value):
    value = value.astype(out_ref.dtype)
    for i in range(out_ref.shape[0]):
        out_ref[i] = value


def block(own_ref, other_ref, index):
    return jnp.concatenate([own_ref[index], other_ref[index]], 0)


def times(v, matrix):
    return lax.dot_general(v, matrix, (((1,), (0,)), ((), ())), preferred_element_type=F32)


def times_t(v, matrix):
    return lax.dot_general(v, matrix, (((1,), (1,)), ((), ())), preferred_element_type=F32)


def in_row(v, row):
    rows = lax.broadcasted_iota(jnp.int32, v.shape, 0)
    return jnp.where(rows == row, v, 0.0)


def own_first(v, core):
    return jnp.where(core == 1, pltpu.roll(v, v.shape[1] // 2, 1), v)


class Pairs:
    def __init__(self, levels, anc_count):
        self.sub = {}
        for m in range(SUB_NODES):
            for kind, count in ((0, levels), (1, depth_of(m))):
                for u in range(count):
                    self.sub[m, kind, u] = len(self.sub)
        self.anc = {}
        for a in range(anc_count):
            for u in range(depth_of(a)):
                self.anc[a, u] = anc_count + len(self.anc)


def sub_leaf_solve(where, here, there, own, other, rhs, out):
    core = where[0]
    cols = rhs.shape[1]
    for m in range(SUB_NODES):
        flipped = jnp.concatenate([here[m], there[m]], 0).astype(F32).T
        rhs[m] = jnp.where(core == 0, flipped[:cols], flipped[cols:]).astype(BF16)
    for m in LEAVES:
        part = times(rhs[m], block(own, other, m)).astype(BF16)
        for i in range(out.shape[0]):
            out[i, m - 1] = part


def sub_low(y, w, pairs, own, other, m, kind, u):
    p = pairs.sub[m, kind, u]
    return w[p] * times_t(y, block(own, other, SUB_NODES + p))


def sub_leaf_update(pairs, w, tiles, own, other, y_out, out):
    y = total(tiles).astype(BF16)
    y_out[...] = y
    value = sum(sub_low(y[m - 1], w, pairs, own, other, m, 1, 0) for m in LEAVES)
    to_all(out, value)


def sub_leaf_anc(pairs, levels, w, y, own, other, out):
    for e in range(levels):
        out[e] = sum(sub_low(y[m - 1], w, pairs, own, other, m, 0, e) for m in LEAVES)


def sub_root_solve(tiles, rhs, own, other, out):
    given = (rhs[0].astype(F32) - total(tiles)).astype(BF16)
    to_all(out, times(given, block(own, other, 0)))


def sub_root_anc(pairs, levels, w, tiles, so_far, own, other, y_out, out, scratch):
    y = total(tiles).astype(BF16)
    y_out[...] = y
    scratch[...] = jnp.zeros_like(scratch)
    for e in range(levels):
        scratch[:, e, :] = so_far[e] + sub_low(y, w, pairs, own, other, 0, 0, e)
    out[...] = scratch[...].astype(BF16)


def fetch(blocks, near, near_x, sems, own, other):
    copies = []
    at = 0
    while at < len(blocks):
        count = 1
        while at + count < len(blocks) and blocks[at + count] == blocks[at] + count:
            count += 1
        for j, (source, target) in enumerate(((own, near), (other, near_x))):
            copies.append(
                pltpu.make_async_copy(
                    source.at[pl.ds(blocks[at], count)],
                    target.at[pl.ds(at, count)],
                    sems.at[at, j],
                )
            )
        at += count
    for copy in copies:
        copy.start()
    return copies


def solve_level(depth, v8, offset, near, near_x, out, scratch):
    first, stop = level_span(depth)
    value = jnp.zeros_like(scratch)
    for i, a in enumerate(range(first, stop)):
        value = value + in_row(times(v8, block(near, near_x, offset + i)), a)
    scratch[...] = value
    to_all(out, scratch[first : first + out.shape[1], :])


def anc_prepare(where, here, there, out):
    lanes = lax.broadcasted_iota(jnp.int32, (ROWS8, here.shape[2]), 1)
    pick = jnp.where(lanes == where[5], 1.0, 0.0).astype(BF16)
    value = jnp.zeros_like(out)
    for a in range(here.shape[0]):
        value = value + in_row(times_t(pick, block(here, there, a)), a)
    out[...] = value


def anc_first(
    blocks, depth, tiles, choose, given, own, other, acc_out, out, scratch, near, near_x, sems, arrived
):
    copies = fetch(blocks, near, near_x, sems, own, other)
    arrived[...] = tiles[...].astype(F32)
    acc = given[...]
    for e in range(choose.shape[0]):
        acc = acc - lax.dot_general(
            choose[e],
            arrived[:, e, :],
            (((1,), (0,)), ((), ())),
            precision=lax.Precision.HIGHEST,
            preferred_element_type=F32,
        )
    acc_out[...] = acc
    for copy in copies:
        copy.wait()
    solve_level(depth, acc.astype(BF16), 0, near, near_x, out, scratch)


def pair_sum(depth, u, values, offset, blocks, down):
    first, stop = level_span(depth)
    result = 0.0
    for i, d in enumerate(range(first, stop)):
        source, target = (d, above(d, u)) if down else (above(d, u), d)
        v = jnp.broadcast_to(values[source : source + 1, :], values.shape)
        v = in_row(v, target).astype(BF16)
        result = result + times_t(v, block(*blocks, offset + i))
    return result


def level_rows(depth, tiles, out):
    first, stop = level_span(depth)
    out[...] = jnp.zeros_like(out)
    out[first:stop, :] = total(tiles)[: stop - first].astype(BF16).astype(F32)


def anc_forward(
    blocks, depth, tiles, acc_in, own, other, y_out, acc_out, out, scratch, near, near_x, sems
):
    copies = fetch(blocks, near, near_x, sems, own, other)
    level_rows(depth, tiles, y_out)
    for copy in copies:
        copy.wait()
    acc = acc_in[...] - pair_sum(depth, depth - 1, y_out, 0, (near, near_x), True)
    acc_out[...] = acc
    solve_level(depth - 1, acc.astype(BF16), 2**depth, near, near_x, out, scratch)


def other_pairs(blocks, depth, down, values, acc_in, own, other, acc_out, near, near_x, sems):
    copies = fetch(blocks, near, near_x, sems, own, other)
    acc = acc_in[...]
    for copy in copies:
        copy.wait()
    for u in range(depth - 1):
        acc = acc - pair_sum(depth, u, values, u * 2**depth, (near, near_x), down)
    acc_out[...] = acc


def z_rows(where, values, rows):
    core, z = where[0], where[1]
    return own_first(values[:, pl.ds(pl.multiple_of(z * rows, rows), rows)], core)


def anc_turn(blocks, where, tiles, own, other, y_out, out, scratch, near, near_x, sems):
    copies = fetch(blocks, near, near_x, sems, own, other)
    level_rows(0, tiles, y_out)
    t = z_rows(where, y_out, own.shape[1] * CORES)
    for copy in copies:
        copy.wait()
    solve_level(0, t.astype(BF16), 0, near, near_x, out, scratch)


def anc_start(where, *refs):
    out = refs[-1]
    out[...] = sum(z_rows(where, values, out.shape[1]) for values in refs[:-1])


def added(*refs):
    refs[-1][...] = sum(values[...] for values in refs[:-1])


def anc_backward(
    blocks, depth, tiles, acc_in, own, other, z_out, out, scratch, near, near_x, sems
):
    copies = fetch(blocks, near, near_x, sems, own, other)
    level_rows(depth - 1, tiles, z_out)
    for copy in copies:
        copy.wait()
    acc = acc_in[...] - pair_sum(depth, depth - 1, z_out, 0, (near, near_x), False)
    solve_level(depth, acc.astype(BF16), 2**depth, near, near_x, out, scratch)


def sub_pieces(where, y_root, y_leaf, out):
    core, held, base = where[0], where[2], where[3]
    rows = out.shape[2]
    span = pl.ds(pl.multiple_of(base, rows), rows)
    scale = held.astype(F32)
    for m in range(SUB_NODES):
        y = y_root[:, span] if m == 0 else y_leaf[m - 1, :, span]
        out[m] = scale * own_first(y.astype(F32), core)


def anc_spread(depth, nrow, tiles, z_in, out, scratch):
    first, stop = level_span(depth)
    scratch[...] = z_in[...]
    scratch[first:stop, :] = total(tiles)
    wide = out.shape[2]
    for i in range(out.shape[0]):
        r = i % nrow
        out[i] = scratch[:, r * wide : (r + 1) * wide].astype(BF16)


def sub_turn(pairs, levels, ids, w, tiles, y_own, own, other, kept, out, scratch):
    scratch[...] = tiles[...].astype(F32)
    picked = []
    for e in range(levels):
        value = 0.0
        for a in range(*level_span(e)):
            value = value + jnp.where(ids[e] == a, 1.0, 0.0) * scratch[:, a, :]
        picked.append(value.astype(BF16))
    for m in range(SUB_NODES):
        value = y_own[m]
        for e in range(levels):
            p = pairs.sub[m, 0, e]
            value = value - w[p] * times_t(picked[e], block(own, other, SUB_NODES + p))
        if m == 0:
            to_all(out, value)
        else:
            kept[m - 1] = value


def sub_root_back(tiles, own, other, kept, out):
    value = times(total(tiles).astype(BF16), block(own, other, 0))
    kept[...] = value
    to_all(out, value)


def sub_leaf_back(pairs, w, tiles, kept, own, other, out):
    z = total(tiles).astype(BF16)
    for m in LEAVES:
        p = pairs.sub[m, 1, 0]
        value = kept[m - 1] - w[p] * times_t(z, block(own, other, SUB_NODES + p))
        for i in range(out.shape[0]):
            out[i, m - 1] = value.astype(BF16)


def sub_finish(tiles, root, own, other, out):
    t = total(tiles).astype(BF16)
    parts = [root[...]] + [times(t[m - 1], block(own, other, m)) for m in LEAVES]
    fill = out.shape[2] - sum(part.shape[0] for part in parts)
    if fill:
        parts.append(jnp.zeros((fill, parts[0].shape[1]), F32))
    flipped = jnp.concatenate(parts, 0).T
    out[...] = flipped.reshape(out.shape).astype(BF16)


def local(anc_lower, anc_upper, sub_lower, sub_upper, anc_rhs, sub_rhs, layer_subtree, sub_pattern):
    layers = lax.axis_size("gz")
    levels = layers.bit_length() - 1
    anc_count = layers - 1
    nrow, nz = lax.axis_size("row"), lax.axis_size("z")
    own, wide = sub_lower.shape[1:]
    size = wide * nrow
    pair_rows = own * CORES
    out_rows = wide // (nz * CORES)
    cols = sub_rhs.shape[2] // CORES
    g, r, z, core = (lax.axis_index(name) for name in ("gz", "row", "z", "core"))
    pairs = Pairs(levels, anc_count)
    part = functools.partial
    scr8 = pltpu.VMEM((ROWS8, size), F32)

    low_w = sub_pattern[:, 0].astype(F32)
    up_w = sub_pattern[:, 1].astype(F32)
    powers = jnp.asarray(2 ** (levels - np.arange(levels)), jnp.int32)
    heap_ids = (layer_subtree[:, None] + layers) // powers[None, :] - 1
    nodes = jnp.arange(ROWS8, dtype=jnp.int32)
    choose = (heap_ids.T[:, None, :] == nodes[None, :, None]).astype(F32)
    choose = jnp.repeat(choose, nrow, axis=2)
    ids_here = lax.dynamic_index_in_dim(heap_ids, g, 0, keepdims=False)
    held = (r == z * nrow // nz).astype(jnp.int32)
    base = jnp.clip(z * pair_rows - r * wide, 0, wide - pair_rows)
    where = jnp.stack([core, z, held, base, jnp.int32(0), core * cols + g * nrow + r]).astype(jnp.int32)

    def gathered(blocks):
        return lax.all_gather(blocks, "row", axis=2, tiled=True)

    def exchange(array, axes):
        return lax.all_to_all(array, axes, 0, 0, tiled=True)

    def two_cores(array):
        return array, swapped(array)

    def tied(send, *others):
        return lax.optimization_barrier((send, *others))

    low = (sub_lower, swapped(sub_lower))
    rhs_there = swapped(sub_rhs)
    anc_low_row = gathered(anc_lower)
    anc_up_row = gathered(anc_upper)

    def diagonal(depth):
        return list(range(*level_span(depth)))

    def pair_blocks(depth, u):
        return [pairs.anc[a, u] for a in range(*level_span(depth))]

    def anc_run(body, blocks, outs, smem, vmem, two, scratch, *fixed):
        near = pltpu.VMEM((len(blocks), *two[0].shape[1:]), BF16)
        sems = pltpu.SemaphoreType.DMA((len(blocks), CORES))
        scratch = (*scratch[:1], near, near, sems, *scratch[1:])
        return run(part(body, blocks, *fixed), outs, smem, vmem, scratch, two)

    def others(depth, down, values, acc, two):
        blocks = [index for u in range(depth - 1) for index in pair_blocks(depth, u)]
        return anc_run(other_pairs, blocks, acc_shape, (), (values, acc), two, (), depth, down)

    def level_shape(depth):
        return shape(BF16, nz, max(2, 2**depth), size)

    acc_shape = shape(F32, ROWS8, pair_rows)
    row_shape = shape(F32, ROWS8, size)

    rhs, tiles = run(
        sub_leaf_solve,
        (shape(BF16, SUB_NODES, cols, pair_rows), shape(BF16, nz, 2, cols, wide)),
        (where,),
        (sub_rhs, rhs_there, *low),
    )
    tiles, anc_rhs = tied(tiles, anc_rhs)
    anc_there = swapped(anc_rhs)
    given8 = run(anc_prepare, acc_shape, (where,), (anc_rhs, anc_there))
    tiles = exchange(tiles, "z")
    tiles, given8, choose, low_w, up_w = tied(tiles, given8, choose, low_w, up_w)
    y_leaf, tiles = run(
        part(sub_leaf_update, pairs),
        (shape(BF16, 2, cols, wide), shape(BF16, nrow, cols, pair_rows)),
        (low_w,),
        (tiles, *low),
    )
    tiles = exchange(tiles, "row")
    so_far = run(
        part(sub_leaf_anc, pairs, levels),
        shape(F32, levels, cols, pair_rows),
        (low_w,),
        (y_leaf, *low),
    )
    tiles, so_far = tied(tiles, so_far)
    tiles = run(sub_root_solve, shape(BF16, nz, cols, wide), (), (tiles, rhs, *low))
    tiles = exchange(tiles, "z")
    tiles, anc_low_row = tied(tiles, anc_low_row)
    anc_low = two_cores(anc_low_row)
    c_scratch = pltpu.VMEM((layers * nrow, ROWS8, pair_rows), F32)
    y_root, tiles = run(
        part(sub_root_anc, pairs, levels),
        (shape(BF16, cols, wide), shape(BF16, layers * nrow, ROWS8, pair_rows)),
        (low_w,),
        (tiles, so_far, *low),
        (c_scratch,),
    )
    tiles = exchange(tiles, ("gz", "row"))

    acc, tiles = anc_run(
        anc_first,
        diagonal(levels - 1),
        (acc_shape, level_shape(levels - 1)),
        (),
        (tiles, choose, given8),
        anc_low,
        (scr8, c_scratch),
        levels - 1,
    )
    tiles = exchange(tiles, "z")
    y_parts = []
    for depth in range(levels - 1, 0, -1):
        if depth == 1:
            tiles, anc_up_row = tied(tiles, anc_up_row)
            anc_up = two_cores(anc_up_row)
        y8, acc, tiles = anc_run(
            anc_forward,
            pair_blocks(depth, depth - 1) + diagonal(depth - 1),
            (row_shape, acc_shape, level_shape(depth - 1)),
            (),
            (tiles, acc),
            anc_low,
            (scr8,),
            depth,
        )
        y_parts.append(y8)
        tiles = exchange(tiles, "z")
        if depth > 1:
            acc = others(depth, True, y8, acc, anc_low)
            tiles, acc = tied(tiles, acc)
    y8, tiles = anc_run(
        anc_turn,
        diagonal(0),
        (row_shape, level_shape(0)),
        (where,),
        (tiles,),
        anc_up,
        (scr8,),
    )
    y_parts.append(y8)
    tiles = exchange(tiles, "z")
    start8 = run(anc_start, acc_shape, (where,), y_parts)
    tiles, start8 = tied(tiles, start8)
    z8 = None
    for depth in range(1, levels):
        acc = start8
        if depth > 1:
            acc = others(depth, False, z8, acc, anc_up)
            tiles, acc = tied(tiles, acc)
        z_now, tiles = anc_run(
            anc_backward,
            pair_blocks(depth, depth - 1) + diagonal(depth),
            (row_shape, level_shape(depth)),
            (),
            (tiles, acc),
            anc_up,
            (scr8,),
            depth,
        )
        if depth == levels - 1:
            tiles, sub_upper = tied(tiles, sub_upper)
        tiles = exchange(tiles, "z")
        z8 = z_now if z8 is None else run(added, row_shape, (), (z8, z_now))
        tiles, z8 = tied(tiles, z8)
    up = two_cores(sub_upper)
    tiles = run(
        part(anc_spread, levels - 1, nrow),
        shape(BF16, layers * nrow, ROWS8, wide),
        (),
        (tiles, z8),
        (scr8,),
    )
    z_all = exchange(tiles, ("gz", "row"))
    y_own = run(sub_pieces, shape(F32, SUB_NODES, cols, pair_rows), (where,), (y_root, y_leaf))
    z_all, y_own, ids_here, up_there = tied(z_all, y_own, ids_here, up[1])
    up = (up[0], up_there)

    kept, tiles = run(
        part(sub_turn, pairs, levels),
        (shape(F32, 2, cols, pair_rows), shape(BF16, nrow, cols, pair_rows)),
        (ids_here, up_w),
        (z_all, y_own, *up),
        (pltpu.VMEM(z_all.shape, F32),),
    )
    tiles = exchange(tiles, "row")

    def out_slice(which):
        start = (z * CORES + which) * out_rows
        return lax.dynamic_slice_in_dim(z_all, start, out_rows, 2)[:, :anc_count].transpose(1, 2, 0)

    def joined(here, there):
        flipped = core == 1
        return jnp.concatenate([jnp.where(flipped, there, here), jnp.where(flipped, here, there)], -1)

    anc_out = joined(out_slice(core), swapped(out_slice(1 - core))).astype(F32)

    root, tiles = run(
        sub_root_back,
        (shape(F32, cols, wide), shape(BF16, nz, cols, wide)),
        (),
        (tiles, *up),
    )
    tiles = exchange(tiles, "z")
    tiles = run(
        part(sub_leaf_back, pairs),
        shape(BF16, nrow, 2, cols, pair_rows),
        (up_w,),
        (tiles, kept, *up),
    )
    tiles = exchange(tiles, "row")
    packed = -(-SUB_NODES * cols // 128) * 128
    tiles = run(
        sub_finish,
        shape(BF16, nz * CORES, out_rows, packed),
        (),
        (tiles, root, *up),
    )
    tiles = exchange(tiles, ("z", "core"))
    sums = jnp.sum(tiles.astype(F32).reshape(nz, CORES, out_rows, packed), 0)
    sums = sums[:, :, : SUB_NODES * cols].reshape(CORES, out_rows, SUB_NODES, cols)
    sub_out = sums.transpose(2, 1, 0, 3).reshape(SUB_NODES, out_rows, CORES * cols)
    return anc_out, sub_out


def solution(mesh):
    sizes = dict(mesh.shape)
    devices = mesh.devices.reshape(sizes["gz"], sizes["row"], sizes["col"] // CORES, CORES)
    split = Mesh(devices, ("gz", "row", "z", "core"))
    col = ("z", "core")
    in_specs = (
        P(None, col, "row"),
        P(None, col, "row"),
        P("gz", col, "row"),
        P("gz", col, "row"),
        P(None, col, None),
        P("gz", col, None),
        P(),
        P("gz", None),
    )
    out_specs = (P(None, ("row", "z", "core"), None), P("gz", ("row", "z", "core"), None))

    return jax.shard_map(local, mesh=split, in_specs=in_specs, out_specs=out_specs, check_vma=False)
```

```python
import functools

import jax
import jax.numpy as jnp
from jax import lax
from jax.experimental import pallas as pl
from jax.experimental.pallas import tpu as pltpu
from jax.sharding import Mesh, PartitionSpec as P


SUB_NODES = 3
LEAVES = (1, 2)
CORES = 2
ROWS8 = 8
F32 = jnp.float32
BF16 = jnp.bfloat16
VMEM_BYTES = 12 * 2**20


def level_span(depth):
    return 2**depth - 1, 2 ** (depth + 1) - 1


def depth_of(node):
    return (node + 1).bit_length() - 1


def above(node, level):
    return ((node + 1) >> (depth_of(node) - level)) - 1


def swapped(array):
    return lax.ppermute(array, "core", [(0, 1), (1, 0)])


def shape(dtype, *dims):
    return jax.ShapeDtypeStruct(dims, dtype)


def run(body, outs, smem, vmem, scratch=(), far=()):
    in_specs = [pl.BlockSpec(memory_space=pltpu.SMEM)] * len(smem)
    in_specs += [pl.BlockSpec(memory_space=pltpu.VMEM)] * len(vmem)
    in_specs += [pl.BlockSpec(memory_space=pltpu.HBM)] * len(far)
    far = [pltpu.with_memory_space_constraint(array, pltpu.HBM) for array in far]
    single = not isinstance(outs, (list, tuple))
    spec = pl.BlockSpec(memory_space=pltpu.VMEM)
    return pl.pallas_call(
        body,
        out_shape=outs,
        in_specs=in_specs,
        out_specs=spec if single else [spec] * len(outs),
        scratch_shapes=list(scratch),
        compiler_params=pltpu.CompilerParams(vmem_limit_bytes=VMEM_BYTES),
    )(*smem, *vmem, *far)


def total(tiles_ref):
    value = tiles_ref[0].astype(F32)
    for i in range(1, tiles_ref.shape[0]):
        value = value + tiles_ref[i].astype(F32)
    return value


def to_all(out_ref, value):
    value = value.astype(out_ref.dtype)
    for i in range(out_ref.shape[0]):
        out_ref[i] = value


def block(own_ref, other_ref, index):
    return jnp.concatenate([own_ref[index], other_ref[index]], 0)


def times(v, matrix):
    return lax.dot_general(v, matrix, (((1,), (0,)), ((), ())), preferred_element_type=F32)


def times_t(v, matrix):
    return lax.dot_general(v, matrix, (((1,), (1,)), ((), ())), preferred_element_type=F32)


def in_row(v, row):
    rows = lax.broadcasted_iota(jnp.int32, v.shape, 0)
    return jnp.where(rows == row, v, 0.0)


def own_first(v, core):
    return jnp.where(core == 1, pltpu.roll(v, v.shape[1] // 2, 1), v)


class Pairs:
    def __init__(self, levels, anc_count):
        self.sub = {}
        for m in range(SUB_NODES):
            for kind, count in ((0, levels), (1, depth_of(m))):
                for u in range(count):
                    self.sub[m, kind, u] = len(self.sub)
        self.anc = {}
        for a in range(anc_count):
            for u in range(depth_of(a)):
                self.anc[a, u] = anc_count + len(self.anc)


def sub_leaf_solve(where, there, other, own, here, rhs, out, near, near_rhs, sems):
    first, count = LEAVES[0], len(LEAVES)
    copies = [
        pltpu.make_async_copy(own.at[pl.ds(first, count)], near, sems.at[0]),
        pltpu.make_async_copy(here, near_rhs, sems.at[1]),
    ]
    for copy in copies:
        copy.start()
    for copy in copies:
        copy.wait()
    core = where[0]
    cols = rhs.shape[1]
    for m in range(SUB_NODES):
        flipped = jnp.concatenate([near_rhs[m], there[m]], 0).astype(F32).T
        rhs[m] = jnp.where(core == 0, flipped[:cols], flipped[cols:]).astype(BF16)
    for m in LEAVES:
        both = jnp.concatenate([near[m - first], other[m]], 0)
        part = times(rhs[m], both).astype(BF16)
        for i in range(out.shape[0]):
            out[i, m - 1] = part


def sub_low(y, w, pairs, own, other, m, kind, u):
    p = pairs.sub[m, kind, u]
    return w[p, 0].astype(F32) * times_t(y, block(own, other, SUB_NODES + p))


def sub_leaf_update(pairs, w, tiles, own, other, y_out, out):
    y = total(tiles).astype(BF16)
    y_out[...] = y
    value = sum(sub_low(y[m - 1], w, pairs, own, other, m, 1, 0) for m in LEAVES)
    to_all(out, value)


def sub_leaf_anc(pairs, levels, w, y, own, other, out):
    for e in range(levels):
        out[e] = sum(sub_low(y[m - 1], w, pairs, own, other, m, 0, e) for m in LEAVES)


def sub_root_solve(tiles, rhs, own, other, out):
    given = (rhs[0].astype(F32) - total(tiles)).astype(BF16)
    to_all(out, times(given, block(own, other, 0)))


def sub_root_anc(pairs, levels, w, tiles, so_far, own, other, y_out, out, scratch):
    y = total(tiles).astype(BF16)
    y_out[...] = y
    scratch[...] = jnp.zeros_like(scratch)
    for e in range(levels):
        scratch[:, e, :] = so_far[e] + sub_low(y, w, pairs, own, other, 0, 0, e)
    out[...] = scratch[...].astype(BF16)


def fetch(blocks, near, near_x, sems, own, other):
    copies = []
    at = 0
    while at < len(blocks):
        count = 1
        while at + count < len(blocks) and blocks[at + count] == blocks[at] + count:
            count += 1
        for j, (source, target) in enumerate(((own, near), (other, near_x))):
            copies.append(
                pltpu.make_async_copy(
                    source.at[pl.ds(blocks[at], count)],
                    target.at[pl.ds(at, count)],
                    sems.at[at, j],
                )
            )
        at += count
    for copy in copies:
        copy.start()
    return copies


def load_blocks(blocks, own, other, near, near_x, sems):
    for copy in fetch(blocks, near, near_x, sems, own, other):
        copy.wait()


def solve_level(depth, v8, offset, near, near_x, out, scratch):
    first, stop = level_span(depth)
    value = jnp.zeros_like(scratch)
    for i, a in enumerate(range(first, stop)):
        value = value + in_row(times(v8, block(near, near_x, offset + i)), a)
    scratch[...] = value
    to_all(out, scratch[first : first + out.shape[1], :])


def ancestor(subtree, g, layers, levels, e):
    return lax.shift_right_logical(subtree[g] + layers, levels - e) - 1


def anc_prepare(layers, nrow, where, subtree, here, there, choose, out):
    levels = choose.shape[0]
    rows = lax.broadcasted_iota(jnp.int32, choose.shape[1:], 0)
    source = lax.broadcasted_iota(jnp.int32, choose.shape[1:], 1)
    for e in range(levels):
        value = jnp.zeros(choose.shape[1:], F32)
        for g in range(layers):
            ours = (source >= g * nrow) & (source < (g + 1) * nrow)
            hit = ours & (rows == ancestor(subtree, g, layers, levels, e))
            value = jnp.where(hit, 1.0, value)
        choose[e] = value
    lanes = lax.broadcasted_iota(jnp.int32, (ROWS8, here.shape[2]), 1)
    pick = jnp.where(lanes == where[5], 1.0, 0.0).astype(BF16)
    value = jnp.zeros_like(out)
    for a in range(here.shape[0]):
        value = value + in_row(times_t(pick, block(here, there, a)), a)
    out[...] = value


def anc_first(depth, tiles, choose, given, near, near_x, acc_out, out, scratch, arrived):
    arrived[...] = tiles[...].astype(F32)
    acc = given[...]
    for e in range(choose.shape[0]):
        acc = acc - lax.dot_general(
            choose[e],
            arrived[:, e, :],
            (((1,), (0,)), ((), ())),
            precision=lax.Precision.HIGHEST,
            preferred_element_type=F32,
        )
    acc_out[...] = acc
    solve_level(depth, acc.astype(BF16), 0, near, near_x, out, scratch)


def pair_sum(depth, u, values, offset, blocks, down):
    first, stop = level_span(depth)
    result = 0.0
    for i, d in enumerate(range(first, stop)):
        source, target = (d, above(d, u)) if down else (above(d, u), d)
        v = jnp.broadcast_to(values[source : source + 1, :], values.shape)
        v = in_row(v, target).astype(BF16)
        result = result + times_t(v, block(*blocks, offset + i))
    return result


def level_rows(depth, tiles, out):
    first, stop = level_span(depth)
    out[...] = jnp.zeros_like(out)
    out[first:stop, :] = total(tiles)[: stop - first].astype(BF16).astype(F32)


def anc_forward(depth, tiles, acc_in, near, near_x, y_out, acc_out, out, scratch):
    level_rows(depth, tiles, y_out)
    acc = acc_in[...] - pair_sum(depth, depth - 1, y_out, 0, (near, near_x), True)
    acc_out[...] = acc
    solve_level(depth - 1, acc.astype(BF16), 2**depth, near, near_x, out, scratch)


def other_pairs(blocks, depth, down, values, acc_in, own, other, acc_out, near, near_x, sems):
    copies = fetch(blocks, near, near_x, sems, own, other)
    acc = acc_in[...]
    for copy in copies:
        copy.wait()
    for u in range(depth - 1):
        acc = acc - pair_sum(depth, u, values, u * 2**depth, (near, near_x), down)
    acc_out[...] = acc


def z_rows(where, values, rows):
    core, z = where[0], where[1]
    return own_first(values[:, pl.ds(pl.multiple_of(z * rows, rows), rows)], core)


def anc_turn(where, tiles, near, near_x, y_out, out, scratch):
    level_rows(0, tiles, y_out)
    t = z_rows(where, y_out, near.shape[1] * CORES)
    solve_level(0, t.astype(BF16), 0, near, near_x, out, scratch)


def anc_start(where, *refs):
    out = refs[-1]
    out[...] = sum(z_rows(where, values, out.shape[1]) for values in refs[:-1])


def added(*refs):
    refs[-1][...] = sum(values[...] for values in refs[:-1])


def anc_backward(depth, tiles, acc_in, near, near_x, z_out, out, scratch):
    level_rows(depth - 1, tiles, z_out)
    acc = acc_in[...] - pair_sum(depth, depth - 1, z_out, 0, (near, near_x), False)
    solve_level(depth, acc.astype(BF16), 2**depth, near, near_x, out, scratch)


def sub_pieces(where, y_root, y_leaf, out):
    core, held, base = where[0], where[2], where[3]
    rows = out.shape[2]
    span = pl.ds(pl.multiple_of(base, rows), rows)
    scale = held.astype(F32)
    for m in range(SUB_NODES):
        y = y_root[:, span] if m == 0 else y_leaf[m - 1, :, span]
        out[m] = scale * own_first(y.astype(F32), core)


def anc_spread(depth, nrow, tiles, z_in, out, scratch):
    first, stop = level_span(depth)
    scratch[...] = z_in[...]
    scratch[first:stop, :] = total(tiles)
    wide = out.shape[2]
    for i in range(out.shape[0]):
        r = i % nrow
        out[i] = scratch[:, r * wide : (r + 1) * wide].astype(BF16)


def sub_turn(pairs, layers, levels, where, subtree, w, tiles, y_own, own, other, kept, out, scratch):
    scratch[...] = tiles[...].astype(F32)
    picked = []
    for e in range(levels):
        id_here = ancestor(subtree, where[4], layers, levels, e)
        value = 0.0
        for a in range(*level_span(e)):
            value = value + jnp.where(id_here == a, 1.0, 0.0) * scratch[:, a, :]
        picked.append(value.astype(BF16))
    for m in range(SUB_NODES):
        value = y_own[m]
        for e in range(levels):
            p = pairs.sub[m, 0, e]
            value = value - w[p, 1].astype(F32) * times_t(picked[e], block(own, other, SUB_NODES + p))
        if m == 0:
            to_all(out, value)
        else:
            kept[m - 1] = value


def sub_root_back(tiles, own, other, kept, out):
    value = times(total(tiles).astype(BF16), block(own, other, 0))
    kept[...] = value
    to_all(out, value)


def sub_leaf_back(pairs, w, tiles, kept, own, other, out):
    z = total(tiles).astype(BF16)
    for m in LEAVES:
        p = pairs.sub[m, 1, 0]
        value = kept[m - 1] - w[p, 1].astype(F32) * times_t(z, block(own, other, SUB_NODES + p))
        for i in range(out.shape[0]):
            out[i, m - 1] = value.astype(BF16)


def sub_finish(tiles, root, own, other, out):
    t = total(tiles).astype(BF16)
    parts = [root[...]] + [times(t[m - 1], block(own, other, m)) for m in LEAVES]
    fill = out.shape[2] - sum(part.shape[0] for part in parts)
    if fill:
        parts.append(jnp.zeros((fill, parts[0].shape[1]), F32))
    flipped = jnp.concatenate(parts, 0).T
    out[...] = flipped.reshape(out.shape).astype(BF16)


def local(anc_lower, anc_upper, sub_lower, sub_upper, anc_rhs, sub_rhs, layer_subtree, sub_pattern):
    layers = lax.axis_size("gz")
    levels = layers.bit_length() - 1
    anc_count = layers - 1
    nrow, nz = lax.axis_size("row"), lax.axis_size("z")
    own, wide = sub_lower.shape[1:]
    size = wide * nrow
    pair_rows = own * CORES
    out_rows = wide // (nz * CORES)
    cols = sub_rhs.shape[2] // CORES
    g, r, z, core = (lax.axis_index(name) for name in ("gz", "row", "z", "core"))
    pairs = Pairs(levels, anc_count)
    part = functools.partial
    scr8 = pltpu.VMEM((ROWS8, size), F32)

    held = (r == z * nrow // nz).astype(jnp.int32)
    base = jnp.clip(z * pair_rows - r * wide, 0, wide - pair_rows)
    where = jnp.stack([core, z, held, base, g, core * cols + g * nrow + r]).astype(jnp.int32)

    def gathered(blocks):
        return lax.all_gather(blocks, "row", axis=2, tiled=True)

    def exchange(array, axes):
        return lax.all_to_all(array, axes, 0, 0, tiled=True)

    def two_cores(array):
        return array, swapped(array)

    def tied(send, *others):
        return lax.optimization_barrier((send, *others))

    low = (sub_lower, swapped(sub_lower))
    rhs_there = swapped(sub_rhs)
    anc_low_row = gathered(anc_lower)
    anc_up_row = gathered(anc_upper)

    def diagonal(depth):
        return list(range(*level_span(depth)))

    def pair_blocks(depth, u):
        return [pairs.anc[a, u] for a in range(*level_span(depth))]

    def loaded(blocks, two):
        near = shape(BF16, len(blocks), own, size)
        sems = pltpu.SemaphoreType.DMA((len(blocks), CORES))
        return run(part(load_blocks, blocks), (near, near), (), (), (sems,), two)

    def others(depth, down, values, acc, two):
        blocks = [index for u in range(depth - 1) for index in pair_blocks(depth, u)]
        near = pltpu.VMEM((len(blocks), own, size), BF16)
        sems = pltpu.SemaphoreType.DMA((len(blocks), CORES))
        body = part(other_pairs, blocks, depth, down)
        return run(body, acc_shape, (), (values, acc), (near, near, sems), two)

    def level_shape(depth):
        return shape(BF16, nz, max(2, 2**depth), size)

    acc_shape = shape(F32, ROWS8, pair_rows)
    row_shape = shape(F32, ROWS8, size)

    rhs, tiles = run(
        sub_leaf_solve,
        (shape(BF16, SUB_NODES, cols, pair_rows), shape(BF16, nz, 2, cols, wide)),
        (where,),
        (rhs_there, low[1]),
        (
            pltpu.VMEM((len(LEAVES), own, wide), BF16),
            pltpu.VMEM(sub_rhs.shape, BF16),
            pltpu.SemaphoreType.DMA((2,)),
        ),
        (sub_lower, sub_rhs),
    )
    tiles, anc_rhs = tied(tiles, anc_rhs)
    anc_there = swapped(anc_rhs)
    choose, given8 = run(
        part(anc_prepare, layers, nrow),
        (shape(F32, levels, ROWS8, layers * nrow), acc_shape),
        (where, layer_subtree),
        (anc_rhs, anc_there),
    )
    tiles = exchange(tiles, "z")
    tiles, given8, choose = tied(tiles, given8, choose)
    y_leaf, tiles = run(
        part(sub_leaf_update, pairs),
        (shape(BF16, 2, cols, wide), shape(BF16, nrow, cols, pair_rows)),
        (sub_pattern,),
        (tiles, *low),
    )
    tiles = exchange(tiles, "row")
    so_far = run(
        part(sub_leaf_anc, pairs, levels),
        shape(F32, levels, cols, pair_rows),
        (sub_pattern,),
        (y_leaf, *low),
    )
    tiles, so_far = tied(tiles, so_far)
    tiles = run(sub_root_solve, shape(BF16, nz, cols, wide), (), (tiles, rhs, *low))
    tiles = exchange(tiles, "z")
    tiles, anc_low_row = tied(tiles, anc_low_row)
    anc_low = two_cores(anc_low_row)
    c_scratch = pltpu.VMEM((layers * nrow, ROWS8, pair_rows), F32)
    y_root, tiles = run(
        part(sub_root_anc, pairs, levels),
        (shape(BF16, cols, wide), shape(BF16, layers * nrow, ROWS8, pair_rows)),
        (sub_pattern,),
        (tiles, so_far, *low),
        (c_scratch,),
    )
    tiles = exchange(tiles, ("gz", "row"))
    near = loaded(diagonal(levels - 1), anc_low)
    tiles, *near = tied(tiles, *near)

    acc, tiles = run(
        part(anc_first, levels - 1),
        (acc_shape, level_shape(levels - 1)),
        (),
        (tiles, choose, given8, *near),
        (scr8, c_scratch),
    )
    tiles = exchange(tiles, "z")
    y_parts = []
    for depth in range(levels - 1, 0, -1):
        blocks = pair_blocks(depth, depth - 1) + diagonal(depth - 1)
        near = loaded(blocks, anc_low)
        tiles, *near = tied(tiles, *near)
        if depth == 1:
            tiles, anc_up_row = tied(tiles, anc_up_row)
            anc_up = two_cores(anc_up_row)
        y8, acc, tiles = run(
            part(anc_forward, depth),
            (row_shape, acc_shape, level_shape(depth - 1)),
            (),
            (tiles, acc, *near),
            (scr8,),
        )
        y_parts.append(y8)
        tiles = exchange(tiles, "z")
        if depth > 1:
            acc = others(depth, True, y8, acc, anc_low)
            tiles, acc = tied(tiles, acc)
    near = loaded(diagonal(0), anc_up)
    tiles, *near = tied(tiles, *near)
    y8, tiles = run(
        anc_turn, (row_shape, level_shape(0)), (where,), (tiles, *near), (scr8,)
    )
    y_parts.append(y8)
    tiles = exchange(tiles, "z")
    start8 = run(anc_start, acc_shape, (where,), y_parts)
    tiles, start8 = tied(tiles, start8)
    z8 = None
    for depth in range(1, levels):
        acc = start8
        blocks = pair_blocks(depth, depth - 1) + diagonal(depth)
        near = loaded(blocks, anc_up)
        tiles, *near = tied(tiles, *near)
        if depth > 1:
            acc = others(depth, False, z8, acc, anc_up)
            tiles, acc = tied(tiles, acc)
        z_now, tiles = run(
            part(anc_backward, depth),
            (row_shape, level_shape(depth)),
            (),
            (tiles, acc, *near),
            (scr8,),
        )
        if depth == levels - 1:
            tiles, sub_upper = tied(tiles, sub_upper)
        tiles = exchange(tiles, "z")
        if z8 is None:
            z8 = z_now
        else:
            z8 = run(added, row_shape, (), (z8, z_now))
            tiles, z8 = tied(tiles, z8)
    up = two_cores(sub_upper)
    tiles = run(
        part(anc_spread, levels - 1, nrow),
        shape(BF16, layers * nrow, ROWS8, wide),
        (),
        (tiles, z8),
        (scr8,),
    )
    z_all = exchange(tiles, ("gz", "row"))
    y_own = run(sub_pieces, shape(F32, SUB_NODES, cols, pair_rows), (where,), (y_root, y_leaf))
    z_all, y_own, up_there = tied(z_all, y_own, up[1])
    up = (up[0], up_there)

    kept, tiles = run(
        part(sub_turn, pairs, layers, levels),
        (shape(F32, 2, cols, pair_rows), shape(BF16, nrow, cols, pair_rows)),
        (where, layer_subtree, sub_pattern),
        (z_all, y_own, *up),
        (pltpu.VMEM(z_all.shape, F32),),
    )
    tiles = exchange(tiles, "row")

    def out_slice(which):
        start = (z * CORES + which) * out_rows
        return lax.dynamic_slice_in_dim(z_all, start, out_rows, 2)[:, :anc_count].transpose(1, 2, 0)

    def joined(here, there):
        flipped = core == 1
        return jnp.concatenate([jnp.where(flipped, there, here), jnp.where(flipped, here, there)], -1)

    anc_out = joined(out_slice(core), swapped(out_slice(1 - core))).astype(F32)

    root, tiles = run(
        sub_root_back,
        (shape(F32, cols, wide), shape(BF16, nz, cols, wide)),
        (),
        (tiles, *up),
    )
    tiles = exchange(tiles, "z")
    tiles = run(
        part(sub_leaf_back, pairs),
        shape(BF16, nrow, 2, cols, pair_rows),
        (sub_pattern,),
        (tiles, kept, *up),
    )
    tiles = exchange(tiles, "row")
    packed = -(-SUB_NODES * cols // 128) * 128
    tiles = run(
        sub_finish,
        shape(BF16, nz * CORES, out_rows, packed),
        (),
        (tiles, root, *up),
    )
    tiles = exchange(tiles, ("z", "core"))
    sums = jnp.sum(tiles.astype(F32).reshape(nz, CORES, out_rows, packed), 0)
    sums = sums[:, :, : SUB_NODES * cols].reshape(CORES, out_rows, SUB_NODES, cols)
    sub_out = sums.transpose(2, 1, 0, 3).reshape(SUB_NODES, out_rows, CORES * cols)
    return anc_out, sub_out


def solution(mesh):
    sizes = dict(mesh.shape)
    devices = mesh.devices.reshape(sizes["gz"], sizes["row"], sizes["col"] // CORES, CORES)
    split = Mesh(devices, ("gz", "row", "z", "core"))
    col = ("z", "core")
    in_specs = (
        P(None, col, "row"),
        P(None, col, "row"),
        P("gz", col, "row"),
        P("gz", col, "row"),
        P(None, col, None),
        P("gz", col, None),
        P(),
        P("gz", None),
    )
    out_specs = (P(None, ("row", "z", "core"), None), P("gz", ("row", "z", "core"), None))

    return jax.shard_map(local, mesh=split, in_specs=in_specs, out_specs=out_specs, check_vma=False)
```

```python
import functools

import jax
import jax.numpy as jnp
from jax import lax
from jax.experimental import pallas as pl
from jax.experimental.pallas import tpu as pltpu
from jax.sharding import Mesh, PartitionSpec as P


SUB_NODES = 3
LEAVES = (1, 2)
CORES = 2
ROWS8 = 8
F32 = jnp.float32
BF16 = jnp.bfloat16
VMEM_BYTES = 12 * 2**20


def level_span(depth):
    return 2**depth - 1, 2 ** (depth + 1) - 1


def depth_of(node):
    return (node + 1).bit_length() - 1


def above(node, level):
    return ((node + 1) >> (depth_of(node) - level)) - 1


def swapped(array):
    return lax.ppermute(array, "core", [(0, 1), (1, 0)])


def shape(dtype, *dims):
    return jax.ShapeDtypeStruct(dims, dtype)


def run(body, outs, smem, vmem, scratch=(), far=()):
    in_specs = [pl.BlockSpec(memory_space=pltpu.SMEM)] * len(smem)
    in_specs += [pl.BlockSpec(memory_space=pltpu.VMEM)] * len(vmem)
    in_specs += [pl.BlockSpec(memory_space=pltpu.HBM)] * len(far)
    far = [pltpu.with_memory_space_constraint(array, pltpu.HBM) for array in far]
    single = not isinstance(outs, (list, tuple))
    spec = pl.BlockSpec(memory_space=pltpu.VMEM)
    return pl.pallas_call(
        body,
        out_shape=outs,
        in_specs=in_specs,
        out_specs=spec if single else [spec] * len(outs),
        scratch_shapes=list(scratch),
        compiler_params=pltpu.CompilerParams(vmem_limit_bytes=VMEM_BYTES),
    )(*smem, *vmem, *far)


def total(tiles_ref):
    value = tiles_ref[0].astype(F32)
    for i in range(1, tiles_ref.shape[0]):
        value = value + tiles_ref[i].astype(F32)
    return value


def to_all(out_ref, value):
    value = value.astype(out_ref.dtype)
    for i in range(out_ref.shape[0]):
        out_ref[i] = value


def block(own_ref, other_ref, index):
    return jnp.concatenate([own_ref[index], other_ref[index]], 0)


def times(v, matrix):
    return lax.dot_general(v, matrix, (((1,), (0,)), ((), ())), preferred_element_type=F32)


def times_t(v, matrix):
    return lax.dot_general(v, matrix, (((1,), (1,)), ((), ())), preferred_element_type=F32)


def in_row(v, row):
    rows = lax.broadcasted_iota(jnp.int32, v.shape, 0)
    return jnp.where(rows == row, v, 0.0)


def own_first(v, core):
    return jnp.where(core == 1, pltpu.roll(v, v.shape[1] // 2, 1), v)


class Pairs:
    def __init__(self, levels, anc_count):
        self.sub = {}
        for m in range(SUB_NODES):
            for kind, count in ((0, levels), (1, depth_of(m))):
                for u in range(count):
                    self.sub[m, kind, u] = len(self.sub)
        self.anc = {}
        for a in range(anc_count):
            for u in range(depth_of(a)):
                self.anc[a, u] = anc_count + len(self.anc)


def sub_leaf_solve(where, there, other, own, here, rhs, out, near, near_rhs, sems):
    first, count = LEAVES[0], len(LEAVES)
    copies = [
        pltpu.make_async_copy(own.at[pl.ds(first, count)], near, sems.at[0]),
        pltpu.make_async_copy(here, near_rhs, sems.at[1]),
    ]
    for copy in copies:
        copy.start()
    for copy in copies:
        copy.wait()
    core = where[0]
    cols = rhs.shape[1]
    for m in range(SUB_NODES):
        flipped = jnp.concatenate([near_rhs[m], there[m]], 0).astype(F32).T
        rhs[m] = jnp.where(core == 0, flipped[:cols], flipped[cols:]).astype(BF16)
    for m in LEAVES:
        both = jnp.concatenate([near[m - first], other[m]], 0)
        part = times(rhs[m], both).astype(BF16)
        for i in range(out.shape[0]):
            out[i, m - 1] = part


def sub_low(y, w, pairs, own, other, m, kind, u):
    p = pairs.sub[m, kind, u]
    return w[p, 0].astype(F32) * times_t(y, block(own, other, SUB_NODES + p))


def sub_leaf_update(pairs, w, tiles, own, other, y_out, out):
    y = total(tiles).astype(BF16)
    y_out[...] = y
    value = sum(sub_low(y[m - 1], w, pairs, own, other, m, 1, 0) for m in LEAVES)
    to_all(out, value)


def sub_leaf_anc(pairs, levels, w, y, own, other, out):
    for e in range(levels):
        out[e] = sum(sub_low(y[m - 1], w, pairs, own, other, m, 0, e) for m in LEAVES)


def sub_root_solve(tiles, rhs, own, other, out):
    given = (rhs[0].astype(F32) - total(tiles)).astype(BF16)
    to_all(out, times(given, block(own, other, 0)))


def sub_root_anc(pairs, levels, w, tiles, so_far, own, other, y_out, out, scratch):
    y = total(tiles).astype(BF16)
    y_out[...] = y
    scratch[...] = jnp.zeros_like(scratch)
    for e in range(levels):
        scratch[:, e, :] = so_far[e] + sub_low(y, w, pairs, own, other, 0, 0, e)
    out[...] = scratch[...].astype(BF16)


def fetch(blocks, core, gathered, near, near_x, sems):
    wide = gathered.shape[3]
    copies = []
    at = 0
    while at < len(blocks):
        count = 1
        while at + count < len(blocks) and blocks[at + count] == blocks[at] + count:
            count += 1
        for r in range(gathered.shape[0] // CORES):
            for which, target in ((core, near), (1 - core, near_x)):
                copies.append(
                    pltpu.make_async_copy(
                        gathered.at[r * CORES + which, pl.ds(blocks[at], count)],
                        target.at[pl.ds(at, count), :, pl.ds(r * wide, wide)],
                        sems.at[len(copies)],
                    )
                )
        at += count
    for copy in copies:
        copy.start()
    return copies


def load_blocks(blocks, where, gathered, near, near_x, sems):
    for copy in fetch(blocks, where[0], gathered, near, near_x, sems):
        copy.wait()


def solve_level(depth, v8, offset, near, near_x, out, scratch):
    first, stop = level_span(depth)
    value = jnp.zeros_like(scratch)
    for i, a in enumerate(range(first, stop)):
        value = value + in_row(times(v8, block(near, near_x, offset + i)), a)
    scratch[...] = value
    to_all(out, scratch[first : first + out.shape[1], :])


def ancestor(subtree, g, layers, levels, e):
    return lax.shift_right_logical(subtree[g] + layers, levels - e) - 1


def anc_prepare(layers, nrow, where, subtree, here, there, choose, out):
    levels = choose.shape[0]
    rows = lax.broadcasted_iota(jnp.int32, choose.shape[1:], 0)
    source = lax.broadcasted_iota(jnp.int32, choose.shape[1:], 1)
    for e in range(levels):
        value = jnp.zeros(choose.shape[1:], F32)
        for g in range(layers):
            ours = (source >= g * nrow) & (source < (g + 1) * nrow)
            hit = ours & (rows == ancestor(subtree, g, layers, levels, e))
            value = jnp.where(hit, 1.0, value)
        choose[e] = value
    lanes = lax.broadcasted_iota(jnp.int32, (ROWS8, here.shape[2]), 1)
    pick = jnp.where(lanes == where[5], 1.0, 0.0).astype(BF16)
    value = jnp.zeros_like(out)
    for a in range(here.shape[0]):
        value = value + in_row(times_t(pick, block(here, there, a)), a)
    out[...] = value


def anc_first(depth, tiles, choose, given, near, near_x, acc_out, out, scratch, arrived):
    arrived[...] = tiles[...].astype(F32)
    acc = given[...]
    for e in range(choose.shape[0]):
        acc = acc - lax.dot_general(
            choose[e],
            arrived[:, e, :],
            (((1,), (0,)), ((), ())),
            precision=lax.Precision.HIGHEST,
            preferred_element_type=F32,
        )
    acc_out[...] = acc
    solve_level(depth, acc.astype(BF16), 0, near, near_x, out, scratch)


def pair_sum(depth, u, values, offset, blocks, down):
    first, stop = level_span(depth)
    result = 0.0
    for i, d in enumerate(range(first, stop)):
        source, target = (d, above(d, u)) if down else (above(d, u), d)
        v = jnp.broadcast_to(values[source : source + 1, :], values.shape)
        v = in_row(v, target).astype(BF16)
        result = result + times_t(v, block(*blocks, offset + i))
    return result


def level_rows(depth, tiles, out):
    first, stop = level_span(depth)
    out[...] = jnp.zeros_like(out)
    out[first:stop, :] = total(tiles)[: stop - first].astype(BF16).astype(F32)


def anc_forward(depth, tiles, acc_in, near, near_x, y_out, acc_out, out, scratch):
    level_rows(depth, tiles, y_out)
    acc = acc_in[...] - pair_sum(depth, depth - 1, y_out, 0, (near, near_x), True)
    acc_out[...] = acc
    solve_level(depth - 1, acc.astype(BF16), 2**depth, near, near_x, out, scratch)


def other_pairs(blocks, depth, down, where, values, acc_in, gathered, acc_out, near, near_x, sems):
    copies = fetch(blocks, where[0], gathered, near, near_x, sems)
    acc = acc_in[...]
    for copy in copies:
        copy.wait()
    for u in range(depth - 1):
        acc = acc - pair_sum(depth, u, values, u * 2**depth, (near, near_x), down)
    acc_out[...] = acc


def z_rows(where, values, rows):
    core, z = where[0], where[1]
    return own_first(values[:, pl.ds(pl.multiple_of(z * rows, rows), rows)], core)


def anc_turn(where, tiles, near, near_x, y_out, out, scratch):
    level_rows(0, tiles, y_out)
    t = z_rows(where, y_out, near.shape[1] * CORES)
    solve_level(0, t.astype(BF16), 0, near, near_x, out, scratch)


def anc_start(where, *refs):
    out = refs[-1]
    out[...] = sum(z_rows(where, values, out.shape[1]) for values in refs[:-1])


def added(*refs):
    refs[-1][...] = sum(values[...] for values in refs[:-1])


def anc_backward(depth, tiles, acc_in, near, near_x, z_out, out, scratch):
    level_rows(depth - 1, tiles, z_out)
    acc = acc_in[...] - pair_sum(depth, depth - 1, z_out, 0, (near, near_x), False)
    solve_level(depth, acc.astype(BF16), 2**depth, near, near_x, out, scratch)


def sub_pieces(where, y_root, y_leaf, out):
    core, held, base = where[0], where[2], where[3]
    rows = out.shape[2]
    span = pl.ds(pl.multiple_of(base, rows), rows)
    scale = held.astype(F32)
    for m in range(SUB_NODES):
        y = y_root[:, span] if m == 0 else y_leaf[m - 1, :, span]
        out[m] = scale * own_first(y.astype(F32), core)


def anc_spread(depth, nrow, tiles, z_in, out, scratch):
    first, stop = level_span(depth)
    scratch[...] = z_in[...]
    scratch[first:stop, :] = total(tiles)
    wide = out.shape[2]
    for i in range(out.shape[0]):
        r = i % nrow
        out[i] = scratch[:, r * wide : (r + 1) * wide].astype(BF16)


def sub_turn(pairs, layers, levels, where, subtree, w, tiles, y_own, own, other, kept, out, scratch):
    scratch[...] = tiles[...].astype(F32)
    picked = []
    for e in range(levels):
        id_here = ancestor(subtree, where[4], layers, levels, e)
        value = 0.0
        for a in range(*level_span(e)):
            value = value + jnp.where(id_here == a, 1.0, 0.0) * scratch[:, a, :]
        picked.append(value.astype(BF16))
    for m in range(SUB_NODES):
        value = y_own[m]
        for e in range(levels):
            p = pairs.sub[m, 0, e]
            value = value - w[p, 1].astype(F32) * times_t(picked[e], block(own, other, SUB_NODES + p))
        if m == 0:
            to_all(out, value)
        else:
            kept[m - 1] = value


def sub_root_back(tiles, own, other, kept, out):
    value = times(total(tiles).astype(BF16), block(own, other, 0))
    kept[...] = value
    to_all(out, value)


def sub_leaf_back(pairs, w, tiles, kept, own, other, out):
    z = total(tiles).astype(BF16)
    for m in LEAVES:
        p = pairs.sub[m, 1, 0]
        value = kept[m - 1] - w[p, 1].astype(F32) * times_t(z, block(own, other, SUB_NODES + p))
        for i in range(out.shape[0]):
            out[i, m - 1] = value.astype(BF16)


def sub_finish(tiles, root, own, other, out):
    t = total(tiles).astype(BF16)
    parts = [root[...]] + [times(t[m - 1], block(own, other, m)) for m in LEAVES]
    fill = out.shape[2] - sum(part.shape[0] for part in parts)
    if fill:
        parts.append(jnp.zeros((fill, parts[0].shape[1]), F32))
    flipped = jnp.concatenate(parts, 0).T
    out[...] = flipped.reshape(out.shape).astype(BF16)


def local(anc_lower, anc_upper, sub_lower, sub_upper, anc_rhs, sub_rhs, layer_subtree, sub_pattern):
    layers = lax.axis_size("gz")
    levels = layers.bit_length() - 1
    anc_count = layers - 1
    nrow, nz = lax.axis_size("row"), lax.axis_size("z")
    own, wide = sub_lower.shape[1:]
    size = wide * nrow
    pair_rows = own * CORES
    out_rows = wide // (nz * CORES)
    cols = sub_rhs.shape[2] // CORES
    g, r, z, core = (lax.axis_index(name) for name in ("gz", "row", "z", "core"))
    pairs = Pairs(levels, anc_count)
    part = functools.partial
    scr8 = pltpu.VMEM((ROWS8, size), F32)

    held = (r == z * nrow // nz).astype(jnp.int32)
    base = jnp.clip(z * pair_rows - r * wide, 0, wide - pair_rows)
    where = jnp.stack([core, z, held, base, g, core * cols + g * nrow + r]).astype(jnp.int32)

    def gathered(blocks):
        return lax.all_gather(blocks, ("row", "core"), axis=0, tiled=False)

    def exchange(array, axes):
        return lax.all_to_all(array, axes, 0, 0, tiled=True)

    def two_cores(array):
        return array, swapped(array)

    def tied(send, *others):
        return lax.optimization_barrier((send, *others))

    low = (sub_lower, swapped(sub_lower))
    rhs_there = swapped(sub_rhs)
    anc_low = gathered(anc_lower)
    anc_up = gathered(anc_upper)

    def diagonal(depth):
        return list(range(*level_span(depth)))

    def pair_blocks(depth, u):
        return [pairs.anc[a, u] for a in range(*level_span(depth))]

    def loaded(blocks, stack):
        near = shape(BF16, len(blocks), own, size)
        sems = pltpu.SemaphoreType.DMA((len(blocks) * nrow * CORES,))
        return run(part(load_blocks, blocks), (near, near), (where,), (), (sems,), (stack,))

    def others(depth, down, values, acc, stack):
        blocks = [index for u in range(depth - 1) for index in pair_blocks(depth, u)]
        near = pltpu.VMEM((len(blocks), own, size), BF16)
        sems = pltpu.SemaphoreType.DMA((len(blocks) * nrow * CORES,))
        body = part(other_pairs, blocks, depth, down)
        return run(body, acc_shape, (where,), (values, acc), (near, near, sems), (stack,))

    def level_shape(depth):
        return shape(BF16, nz, max(2, 2**depth), size)

    acc_shape = shape(F32, ROWS8, pair_rows)
    row_shape = shape(F32, ROWS8, size)

    rhs, tiles = run(
        sub_leaf_solve,
        (shape(BF16, SUB_NODES, cols, pair_rows), shape(BF16, nz, 2, cols, wide)),
        (where,),
        (rhs_there, low[1]),
        (
            pltpu.VMEM((len(LEAVES), own, wide), BF16),
            pltpu.VMEM(sub_rhs.shape, BF16),
            pltpu.SemaphoreType.DMA((2,)),
        ),
        (sub_lower, sub_rhs),
    )
    tiles, anc_rhs = tied(tiles, anc_rhs)
    anc_there = swapped(anc_rhs)
    choose, given8 = run(
        part(anc_prepare, layers, nrow),
        (shape(F32, levels, ROWS8, layers * nrow), acc_shape),
        (where, layer_subtree),
        (anc_rhs, anc_there),
    )
    tiles = exchange(tiles, "z")
    tiles, given8, choose = tied(tiles, given8, choose)
    y_leaf, tiles = run(
        part(sub_leaf_update, pairs),
        (shape(BF16, 2, cols, wide), shape(BF16, nrow, cols, pair_rows)),
        (sub_pattern,),
        (tiles, *low),
    )
    tiles = exchange(tiles, "row")
    so_far = run(
        part(sub_leaf_anc, pairs, levels),
        shape(F32, levels, cols, pair_rows),
        (sub_pattern,),
        (y_leaf, *low),
    )
    tiles, so_far = tied(tiles, so_far)
    tiles = run(sub_root_solve, shape(BF16, nz, cols, wide), (), (tiles, rhs, *low))
    tiles = exchange(tiles, "z")
    c_scratch = pltpu.VMEM((layers * nrow, ROWS8, pair_rows), F32)
    y_root, tiles = run(
        part(sub_root_anc, pairs, levels),
        (shape(BF16, cols, wide), shape(BF16, layers * nrow, ROWS8, pair_rows)),
        (sub_pattern,),
        (tiles, so_far, *low),
        (c_scratch,),
    )
    tiles = exchange(tiles, ("gz", "row"))
    near = loaded(diagonal(levels - 1), anc_low)
    tiles, *near = tied(tiles, *near)

    acc, tiles = run(
        part(anc_first, levels - 1),
        (acc_shape, level_shape(levels - 1)),
        (),
        (tiles, choose, given8, *near),
        (scr8, c_scratch),
    )
    tiles = exchange(tiles, "z")
    y_parts = []
    for depth in range(levels - 1, 0, -1):
        blocks = pair_blocks(depth, depth - 1) + diagonal(depth - 1)
        near = loaded(blocks, anc_low)
        tiles, *near = tied(tiles, *near)
        y8, acc, tiles = run(
            part(anc_forward, depth),
            (row_shape, acc_shape, level_shape(depth - 1)),
            (),
            (tiles, acc, *near),
            (scr8,),
        )
        y_parts.append(y8)
        tiles = exchange(tiles, "z")
        if depth > 1:
            acc = others(depth, True, y8, acc, anc_low)
            tiles, acc = tied(tiles, acc)
    near = loaded(diagonal(0), anc_up)
    tiles, *near = tied(tiles, *near)
    y8, tiles = run(
        anc_turn, (row_shape, level_shape(0)), (where,), (tiles, *near), (scr8,)
    )
    y_parts.append(y8)
    tiles = exchange(tiles, "z")
    start8 = run(anc_start, acc_shape, (where,), y_parts)
    tiles, start8 = tied(tiles, start8)
    z8 = None
    for depth in range(1, levels):
        acc = start8
        blocks = pair_blocks(depth, depth - 1) + diagonal(depth)
        near = loaded(blocks, anc_up)
        tiles, *near = tied(tiles, *near)
        if depth > 1:
            acc = others(depth, False, z8, acc, anc_up)
            tiles, acc = tied(tiles, acc)
        z_now, tiles = run(
            part(anc_backward, depth),
            (row_shape, level_shape(depth)),
            (),
            (tiles, acc, *near),
            (scr8,),
        )
        if depth == levels - 1:
            tiles, sub_upper = tied(tiles, sub_upper)
        tiles = exchange(tiles, "z")
        if z8 is None:
            z8 = z_now
        else:
            z8 = run(added, row_shape, (), (z8, z_now))
            tiles, z8 = tied(tiles, z8)
    up = two_cores(sub_upper)
    tiles = run(
        part(anc_spread, levels - 1, nrow),
        shape(BF16, layers * nrow, ROWS8, wide),
        (),
        (tiles, z8),
        (scr8,),
    )
    z_all = exchange(tiles, ("gz", "row"))
    y_own = run(sub_pieces, shape(F32, SUB_NODES, cols, pair_rows), (where,), (y_root, y_leaf))
    z_all, y_own, up_there = tied(z_all, y_own, up[1])
    up = (up[0], up_there)

    kept, tiles = run(
        part(sub_turn, pairs, layers, levels),
        (shape(F32, 2, cols, pair_rows), shape(BF16, nrow, cols, pair_rows)),
        (where, layer_subtree, sub_pattern),
        (z_all, y_own, *up),
        (pltpu.VMEM(z_all.shape, F32),),
    )
    tiles = exchange(tiles, "row")

    def out_slice(which):
        start = (z * CORES + which) * out_rows
        return lax.dynamic_slice_in_dim(z_all, start, out_rows, 2)[:, :anc_count].transpose(1, 2, 0)

    def joined(here, there):
        flipped = core == 1
        return jnp.concatenate([jnp.where(flipped, there, here), jnp.where(flipped, here, there)], -1)

    anc_out = joined(out_slice(core), swapped(out_slice(1 - core))).astype(F32)

    root, tiles = run(
        sub_root_back,
        (shape(F32, cols, wide), shape(BF16, nz, cols, wide)),
        (),
        (tiles, *up),
    )
    tiles = exchange(tiles, "z")
    tiles = run(
        part(sub_leaf_back, pairs),
        shape(BF16, nrow, 2, cols, pair_rows),
        (sub_pattern,),
        (tiles, kept, *up),
    )
    tiles = exchange(tiles, "row")
    packed = -(-SUB_NODES * cols // 128) * 128
    tiles = run(
        sub_finish,
        shape(BF16, nz * CORES, out_rows, packed),
        (),
        (tiles, root, *up),
    )
    tiles = exchange(tiles, ("z", "core"))
    sums = jnp.sum(tiles.astype(F32).reshape(nz, CORES, out_rows, packed), 0)
    sums = sums[:, :, : SUB_NODES * cols].reshape(CORES, out_rows, SUB_NODES, cols)
    sub_out = sums.transpose(2, 1, 0, 3).reshape(SUB_NODES, out_rows, CORES * cols)
    return anc_out, sub_out


def solution(mesh):
    sizes = dict(mesh.shape)
    devices = mesh.devices.reshape(sizes["gz"], sizes["row"], sizes["col"] // CORES, CORES)
    split = Mesh(devices, ("gz", "row", "z", "core"))
    col = ("z", "core")
    in_specs = (
        P(None, col, "row"),
        P(None, col, "row"),
        P("gz", col, "row"),
        P("gz", col, "row"),
        P(None, col, None),
        P("gz", col, None),
        P(),
        P("gz", None),
    )
    out_specs = (P(None, ("row", "z", "core"), None), P("gz", ("row", "z", "core"), None))

    return jax.shard_map(local, mesh=split, in_specs=in_specs, out_specs=out_specs, check_vma=False)
```

```python
import functools

import jax
import jax.numpy as jnp
from jax import lax
from jax.experimental import pallas as pl
from jax.experimental.pallas import tpu as pltpu
from jax.sharding import Mesh, PartitionSpec as P


SUB_NODES = 3
LEAVES = (1, 2)
CORES = 2
ROWS8 = 8
F32 = jnp.float32
BF16 = jnp.bfloat16
VMEM_BYTES = 12 * 2**20


def level_span(depth):
    return 2**depth - 1, 2 ** (depth + 1) - 1


def depth_of(node):
    return (node + 1).bit_length() - 1


def above(node, level):
    return ((node + 1) >> (depth_of(node) - level)) - 1


def swapped(array):
    return lax.ppermute(array, "core", [(0, 1), (1, 0)])


def shape(dtype, *dims):
    return jax.ShapeDtypeStruct(dims, dtype)


def run(body, outs, smem, vmem, scratch=(), far=()):
    in_specs = [pl.BlockSpec(memory_space=pltpu.SMEM)] * len(smem)
    in_specs += [pl.BlockSpec(memory_space=pltpu.VMEM)] * len(vmem)
    in_specs += [pl.BlockSpec(memory_space=pltpu.HBM)] * len(far)
    far = [pltpu.with_memory_space_constraint(array, pltpu.HBM) for array in far]
    single = not isinstance(outs, (list, tuple))
    spec = pl.BlockSpec(memory_space=pltpu.VMEM)
    return pl.pallas_call(
        body,
        out_shape=outs,
        in_specs=in_specs,
        out_specs=spec if single else [spec] * len(outs),
        scratch_shapes=list(scratch),
        compiler_params=pltpu.CompilerParams(vmem_limit_bytes=VMEM_BYTES),
    )(*smem, *vmem, *far)


def total(tiles_ref):
    value = tiles_ref[0].astype(F32)
    for i in range(1, tiles_ref.shape[0]):
        value = value + tiles_ref[i].astype(F32)
    return value


def to_all(out_ref, value):
    value = value.astype(out_ref.dtype)
    for i in range(out_ref.shape[0]):
        out_ref[i] = value


def block(own_ref, other_ref, index):
    return jnp.concatenate([own_ref[index], other_ref[index]], 0)


def times(v, matrix):
    return lax.dot_general(v, matrix, (((1,), (0,)), ((), ())), preferred_element_type=F32)


def times_t(v, matrix):
    return lax.dot_general(v, matrix, (((1,), (1,)), ((), ())), preferred_element_type=F32)


def in_row(v, row):
    rows = lax.broadcasted_iota(jnp.int32, v.shape, 0)
    return jnp.where(rows == row, v, 0.0)


def own_first(v, core):
    return jnp.where(core == 1, pltpu.roll(v, v.shape[1] // 2, 1), v)


class Pairs:
    def __init__(self, levels, anc_count):
        self.sub = {}
        for m in range(SUB_NODES):
            for kind, count in ((0, levels), (1, depth_of(m))):
                for u in range(count):
                    self.sub[m, kind, u] = len(self.sub)
        self.anc = {}
        for a in range(anc_count):
            for u in range(depth_of(a)):
                self.anc[a, u] = anc_count + len(self.anc)


def sub_leaf_solve(where, there, other, own, here, rhs, out, near, near_rhs, sems):
    first, count = LEAVES[0], len(LEAVES)
    copies = [
        pltpu.make_async_copy(own.at[pl.ds(first, count)], near, sems.at[0]),
        pltpu.make_async_copy(here, near_rhs, sems.at[1]),
    ]
    for copy in copies:
        copy.start()
    for copy in copies:
        copy.wait()
    core = where[0]
    cols = rhs.shape[1]
    for m in range(SUB_NODES):
        flipped = jnp.concatenate([near_rhs[m], there[m]], 0).astype(F32).T
        rhs[m] = jnp.where(core == 0, flipped[:cols], flipped[cols:]).astype(BF16)
    for m in LEAVES:
        both = jnp.concatenate([near[m - first], other[m]], 0)
        part = times(rhs[m], both).astype(BF16)
        for i in range(out.shape[0]):
            out[i, m - 1] = part


def sub_low(y, w, pairs, own, other, m, kind, u):
    p = pairs.sub[m, kind, u]
    return w[p, 0].astype(F32) * times_t(y, block(own, other, SUB_NODES + p))


def sub_leaf_update(pairs, w, tiles, own, other, y_out, out):
    y = total(tiles).astype(BF16)
    y_out[...] = y
    value = sum(sub_low(y[m - 1], w, pairs, own, other, m, 1, 0) for m in LEAVES)
    to_all(out, value)


def sub_leaf_anc(pairs, levels, w, y, own, other, out):
    for e in range(levels):
        out[e] = sum(sub_low(y[m - 1], w, pairs, own, other, m, 0, e) for m in LEAVES)


def sub_root_solve(tiles, rhs, own, other, out):
    given = (rhs[0].astype(F32) - total(tiles)).astype(BF16)
    to_all(out, times(given, block(own, other, 0)))


def sub_root_anc(pairs, levels, w, tiles, so_far, own, other, y_out, out, scratch):
    y = total(tiles).astype(BF16)
    y_out[...] = y
    scratch[...] = jnp.zeros_like(scratch)
    for e in range(levels):
        scratch[:, e, :] = so_far[e] + sub_low(y, w, pairs, own, other, 0, 0, e)
    out[...] = scratch[...].astype(BF16)


def fetch(groups, core, near, near_x, sems):
    copies = []
    base = 0
    for blocks, gathered in groups:
        wide = gathered.shape[3]
        at = 0
        while at < len(blocks):
            count = 1
            while at + count < len(blocks) and blocks[at + count] == blocks[at] + count:
                count += 1
            for r in range(gathered.shape[0] // CORES):
                for which, target in ((core, near), (1 - core, near_x)):
                    copies.append(
                        pltpu.make_async_copy(
                            gathered.at[r * CORES + which, pl.ds(blocks[at], count)],
                            target.at[pl.ds(base + at, count), :, pl.ds(r * wide, wide)],
                            sems.at[len(copies)],
                        )
                    )
            at += count
        base += len(blocks)
    for copy in copies:
        copy.start()
    return copies


def load_blocks(lists, where, *refs):
    *stacks, near, near_x, sems = refs
    for copy in fetch(list(zip(lists, stacks)), where[0], near, near_x, sems):
        copy.wait()


def make_root(where, low, upper, root, root_x, near, near_x, near_up, sems, up_sem):
    copy = pltpu.make_async_copy(upper, near_up, up_sem.at[0])
    copy.start()
    for other in fetch([([0], low)], where[0], near, near_x, sems):
        other.wait()
    copy.wait()
    left = block(near, near_x, 0)
    own, wide = upper.shape[1:]
    span = left.shape[1] // own
    for r in range(upper.shape[0] // span):
        right = near_up[r * span : (r + 1) * span].reshape(span * own, wide)
        value = times(left, right).astype(BF16)
        root[0, :, r * wide : (r + 1) * wide] = value[:own]
        root_x[0, :, r * wide : (r + 1) * wide] = value[own:]


def solve_level(depth, v8, offset, near, near_x, out, scratch):
    first, stop = level_span(depth)
    value = jnp.zeros_like(scratch)
    for i, a in enumerate(range(first, stop)):
        value = value + in_row(times(v8, block(near, near_x, offset + i)), a)
    scratch[...] = value
    to_all(out, scratch[first : first + out.shape[1], :])


def ancestor(subtree, g, layers, levels, e):
    return lax.shift_right_logical(subtree[g] + layers, levels - e) - 1


def anc_prepare(layers, nrow, where, subtree, here, there, choose, out):
    levels = choose.shape[0]
    rows = lax.broadcasted_iota(jnp.int32, choose.shape[1:], 0)
    source = lax.broadcasted_iota(jnp.int32, choose.shape[1:], 1)
    for e in range(levels):
        value = jnp.zeros(choose.shape[1:], F32)
        for g in range(layers):
            ours = (source >= g * nrow) & (source < (g + 1) * nrow)
            hit = ours & (rows == ancestor(subtree, g, layers, levels, e))
            value = jnp.where(hit, 1.0, value)
        choose[e] = value
    lanes = lax.broadcasted_iota(jnp.int32, (ROWS8, here.shape[2]), 1)
    pick = jnp.where(lanes == where[5], 1.0, 0.0).astype(BF16)
    value = jnp.zeros_like(out)
    for a in range(here.shape[0]):
        value = value + in_row(times_t(pick, block(here, there, a)), a)
    out[...] = value


def anc_first(depth, tiles, choose, given, near, near_x, acc_out, out, scratch, arrived):
    arrived[...] = tiles[...].astype(F32)
    acc = given[...]
    for e in range(choose.shape[0]):
        acc = acc - lax.dot_general(
            choose[e],
            arrived[:, e, :],
            (((1,), (0,)), ((), ())),
            precision=lax.Precision.HIGHEST,
            preferred_element_type=F32,
        )
    acc_out[...] = acc
    solve_level(depth, acc.astype(BF16), 0, near, near_x, out, scratch)


def pair_sum(depth, u, values, offset, blocks, down):
    first, stop = level_span(depth)
    result = 0.0
    for i, d in enumerate(range(first, stop)):
        source, target = (d, above(d, u)) if down else (above(d, u), d)
        v = jnp.broadcast_to(values[source : source + 1, :], values.shape)
        v = in_row(v, target).astype(BF16)
        result = result + times_t(v, block(*blocks, offset + i))
    return result


def level_rows(depth, tiles, out):
    first, stop = level_span(depth)
    out[...] = jnp.zeros_like(out)
    out[first:stop, :] = total(tiles)[: stop - first].astype(BF16).astype(F32)


def anc_forward(depth, tiles, acc_in, near, near_x, y_out, acc_out, out, scratch):
    level_rows(depth, tiles, y_out)
    acc = acc_in[...] - pair_sum(depth, depth - 1, y_out, 0, (near, near_x), True)
    acc_out[...] = acc
    solve_level(depth - 1, acc.astype(BF16), 2**depth, near, near_x, out, scratch)


def other_pairs(blocks, depth, down, where, values, acc_in, gathered, acc_out, near, near_x, sems):
    copies = fetch([(blocks, gathered)], where[0], near, near_x, sems)
    acc = acc_in[...]
    for copy in copies:
        copy.wait()
    for u in range(depth - 1):
        acc = acc - pair_sum(depth, u, values, u * 2**depth, (near, near_x), down)
    acc_out[...] = acc


def z_rows(where, values, rows):
    core, z = where[0], where[1]
    return own_first(values[:, pl.ds(pl.multiple_of(z * rows, rows), rows)], core)


def anc_turn(tiles, acc_in, near, near_x, root, root_x, y_out, out, scratch):
    level_rows(1, tiles, y_out)
    acc = acc_in[...] - pair_sum(1, 0, y_out, 0, (near, near_x), True)
    solve_level(0, acc.astype(BF16), 0, root, root_x, out, scratch)


def anc_start(where, *refs):
    out = refs[-1]
    out[...] = sum(z_rows(where, values, out.shape[1]) for values in refs[:-1])


def added(*refs):
    refs[-1][...] = sum(values[...] for values in refs[:-1])


def anc_backward(depth, tiles, acc_in, near, near_x, z_out, out, scratch):
    level_rows(depth - 1, tiles, z_out)
    acc = acc_in[...] - pair_sum(depth, depth - 1, z_out, 2**depth, (near, near_x), False)
    solve_level(depth, acc.astype(BF16), 0, near, near_x, out, scratch)


def sub_pieces(where, y_root, y_leaf, out):
    core, held, base = where[0], where[2], where[3]
    rows = out.shape[2]
    span = pl.ds(pl.multiple_of(base, rows), rows)
    scale = held.astype(F32)
    for m in range(SUB_NODES):
        y = y_root[:, span] if m == 0 else y_leaf[m - 1, :, span]
        out[m] = scale * own_first(y.astype(F32), core)


def anc_spread(depth, nrow, tiles, z_in, out, scratch):
    first, stop = level_span(depth)
    scratch[...] = z_in[...]
    scratch[first:stop, :] = total(tiles)
    wide = out.shape[2]
    for i in range(out.shape[0]):
        r = i % nrow
        out[i] = scratch[:, r * wide : (r + 1) * wide].astype(BF16)


def sub_turn(pairs, layers, levels, where, subtree, w, tiles, y_own, own, other, kept, out, scratch):
    scratch[...] = tiles[...].astype(F32)
    picked = []
    for e in range(levels):
        id_here = ancestor(subtree, where[4], layers, levels, e)
        value = 0.0
        for a in range(*level_span(e)):
            value = value + jnp.where(id_here == a, 1.0, 0.0) * scratch[:, a, :]
        picked.append(value.astype(BF16))
    for m in range(SUB_NODES):
        value = y_own[m]
        for e in range(levels):
            p = pairs.sub[m, 0, e]
            value = value - w[p, 1].astype(F32) * times_t(picked[e], block(own, other, SUB_NODES + p))
        if m == 0:
            to_all(out, value)
        else:
            kept[m - 1] = value


def sub_root_back(tiles, own, other, kept, out):
    value = times(total(tiles).astype(BF16), block(own, other, 0))
    kept[...] = value
    to_all(out, value)


def sub_leaf_back(pairs, w, tiles, kept, own, other, out):
    z = total(tiles).astype(BF16)
    for m in LEAVES:
        p = pairs.sub[m, 1, 0]
        value = kept[m - 1] - w[p, 1].astype(F32) * times_t(z, block(own, other, SUB_NODES + p))
        for i in range(out.shape[0]):
            out[i, m - 1] = value.astype(BF16)


def sub_finish(tiles, root, own, other, out):
    t = total(tiles).astype(BF16)
    parts = [root[...]] + [times(t[m - 1], block(own, other, m)) for m in LEAVES]
    fill = out.shape[2] - sum(part.shape[0] for part in parts)
    if fill:
        parts.append(jnp.zeros((fill, parts[0].shape[1]), F32))
    flipped = jnp.concatenate(parts, 0).T
    out[...] = flipped.reshape(out.shape).astype(BF16)


def local(anc_lower, anc_upper, sub_lower, sub_upper, anc_rhs, sub_rhs, layer_subtree, sub_pattern):
    layers = lax.axis_size("gz")
    levels = layers.bit_length() - 1
    anc_count = layers - 1
    nrow, nz = lax.axis_size("row"), lax.axis_size("z")
    own, wide = sub_lower.shape[1:]
    size = wide * nrow
    pair_rows = own * CORES
    out_rows = wide // (nz * CORES)
    cols = sub_rhs.shape[2] // CORES
    g, r, z, core = (lax.axis_index(name) for name in ("gz", "row", "z", "core"))
    pairs = Pairs(levels, anc_count)
    part = functools.partial
    scr8 = pltpu.VMEM((ROWS8, size), F32)

    held = (r == z * nrow // nz).astype(jnp.int32)
    base = jnp.clip(z * pair_rows - r * wide, 0, wide - pair_rows)
    where = jnp.stack([core, z, held, base, g, core * cols + g * nrow + r]).astype(jnp.int32)

    def gathered(blocks, axes):
        return lax.all_gather(blocks, axes, axis=0, tiled=False)

    def exchange(array, axes):
        return lax.all_to_all(array, axes, 0, 0, tiled=True)

    def two_cores(array):
        return array, swapped(array)

    def tied(send, *others):
        return lax.optimization_barrier((send, *others))

    low = (sub_lower, swapped(sub_lower))
    rhs_there = swapped(sub_rhs)
    anc_low = gathered(anc_lower, ("row", "core"))

    def diagonal(depth):
        return list(range(*level_span(depth)))

    up_split = pairs.anc[level_span(levels - 1)[0], 0]

    def from_up(blocks):
        first = [index - 1 for index in blocks if index < up_split]
        return (first, up_a), ([index - up_split for index in blocks if index >= up_split], up_b)

    def pair_blocks(depth, u):
        return [pairs.anc[a, u] for a in range(*level_span(depth))]

    def loaded(groups):
        groups = [group for group in groups if group[0]]
        lists = [blocks for blocks, stack in groups]
        count = sum(len(blocks) for blocks in lists)
        near = shape(BF16, count, own, size)
        sems = pltpu.SemaphoreType.DMA((count * nrow * CORES,))
        stacks = [stack for blocks, stack in groups]
        return run(part(load_blocks, lists), (near, near), (where,), (), (sems,), stacks)

    def others(depth, down, values, acc, group):
        blocks, stack = group
        near = pltpu.VMEM((len(blocks), own, size), BF16)
        sems = pltpu.SemaphoreType.DMA((len(blocks) * nrow * CORES,))
        body = part(other_pairs, blocks, depth, down)
        return run(body, acc_shape, (where,), (values, acc), (near, near, sems), (stack,))

    def older_pairs(depth):
        return [index for u in range(depth - 1) for index in pair_blocks(depth, u)]

    def level_shape(depth):
        return shape(BF16, nz, max(2, 2**depth), size)

    acc_shape = shape(F32, ROWS8, pair_rows)
    row_shape = shape(F32, ROWS8, size)

    rhs, tiles = run(
        sub_leaf_solve,
        (shape(BF16, SUB_NODES, cols, pair_rows), shape(BF16, nz, 2, cols, wide)),
        (where,),
        (rhs_there, low[1]),
        (
            pltpu.VMEM((len(LEAVES), own, wide), BF16),
            pltpu.VMEM(sub_rhs.shape, BF16),
            pltpu.SemaphoreType.DMA((2,)),
        ),
        (sub_lower, sub_rhs),
    )
    tiles, anc_rhs = tied(tiles, anc_rhs)
    anc_there = swapped(anc_rhs)
    choose, given8 = run(
        part(anc_prepare, layers, nrow),
        (shape(F32, levels, ROWS8, layers * nrow), acc_shape),
        (where, layer_subtree),
        (anc_rhs, anc_there),
    )
    given8, anc_upper = tied(given8, anc_upper)
    root_up = gathered(anc_upper[0], ("row", "z", "core"))
    up_a = gathered(anc_upper[1:up_split], ("row", "core"))
    up_b = gathered(anc_upper[up_split:], ("row", "core"))
    tiles = exchange(tiles, "z")
    tiles, given8, choose = tied(tiles, given8, choose)
    y_leaf, tiles = run(
        part(sub_leaf_update, pairs),
        (shape(BF16, 2, cols, wide), shape(BF16, nrow, cols, pair_rows)),
        (sub_pattern,),
        (tiles, *low),
    )
    tiles = exchange(tiles, "row")
    so_far = run(
        part(sub_leaf_anc, pairs, levels),
        shape(F32, levels, cols, pair_rows),
        (sub_pattern,),
        (y_leaf, *low),
    )
    tiles, so_far = tied(tiles, so_far)
    tiles = run(sub_root_solve, shape(BF16, nz, cols, wide), (), (tiles, rhs, *low))
    tiles = exchange(tiles, "z")
    c_scratch = pltpu.VMEM((layers * nrow, ROWS8, pair_rows), F32)
    y_root, tiles = run(
        part(sub_root_anc, pairs, levels),
        (shape(BF16, cols, wide), shape(BF16, layers * nrow, ROWS8, pair_rows)),
        (sub_pattern,),
        (tiles, so_far, *low),
        (c_scratch,),
    )
    tiles = exchange(tiles, ("gz", "row"))
    near = loaded([(diagonal(levels - 1), anc_low)])
    tiles, *near = tied(tiles, *near)

    acc, tiles = run(
        part(anc_first, levels - 1),
        (acc_shape, level_shape(levels - 1)),
        (),
        (tiles, choose, given8, *near),
        (scr8, c_scratch),
    )
    tiles = exchange(tiles, "z")
    near_root = pltpu.VMEM((1, own, size), BF16)
    root = run(
        make_root,
        (shape(BF16, 1, own, size), shape(BF16, 1, own, size)),
        (where,),
        (),
        (
            near_root,
            near_root,
            pltpu.VMEM(root_up.shape, BF16),
            pltpu.SemaphoreType.DMA((nrow * CORES,)),
            pltpu.SemaphoreType.DMA((1,)),
        ),
        (anc_low, root_up),
    )
    tiles, *root = tied(tiles, *root)
    y_parts = []
    for depth in range(levels - 1, 1, -1):
        blocks = pair_blocks(depth, depth - 1) + diagonal(depth - 1)
        near = loaded([(blocks, anc_low)])
        tiles, *near = tied(tiles, *near)
        y8, acc, tiles = run(
            part(anc_forward, depth),
            (row_shape, acc_shape, level_shape(depth - 1)),
            (),
            (tiles, acc, *near),
            (scr8,),
        )
        y_parts.append(y8)
        tiles = exchange(tiles, "z")
        acc = others(depth, True, y8, acc, (older_pairs(depth), anc_low))
        tiles, acc = tied(tiles, acc)
    near = loaded([(pair_blocks(1, 0), anc_low)])
    tiles, *near = tied(tiles, *near)
    y8, tiles = run(
        anc_turn,
        (row_shape, level_shape(0)),
        (),
        (tiles, acc, *near, *root),
        (scr8,),
    )
    y_parts.append(y8)
    tiles = exchange(tiles, "z")
    start8 = run(anc_start, acc_shape, (where,), y_parts)
    tiles, start8 = tied(tiles, start8)
    z8 = None
    for depth in range(1, levels):
        acc = start8
        blocks = diagonal(depth) + pair_blocks(depth, depth - 1)
        near = loaded(from_up(blocks))
        tiles, *near = tied(tiles, *near)
        if depth > 1:
            group = [index - up_split for index in older_pairs(depth)], up_b
            acc = others(depth, False, z8, acc, group)
            tiles, acc = tied(tiles, acc)
        z_now, tiles = run(
            part(anc_backward, depth),
            (row_shape, level_shape(depth)),
            (),
            (tiles, acc, *near),
            (scr8,),
        )
        if depth == levels - 1:
            tiles, sub_upper = tied(tiles, sub_upper)
        tiles = exchange(tiles, "z")
        if z8 is None:
            z8 = z_now
        else:
            z8 = run(added, row_shape, (), (z8, z_now))
            tiles, z8 = tied(tiles, z8)
    up = two_cores(sub_upper)
    tiles = run(
        part(anc_spread, levels - 1, nrow),
        shape(BF16, layers * nrow, ROWS8, wide),
        (),
        (tiles, z8),
        (scr8,),
    )
    z_all = exchange(tiles, ("gz", "row"))
    y_own = run(sub_pieces, shape(F32, SUB_NODES, cols, pair_rows), (where,), (y_root, y_leaf))
    z_all, y_own, up_there = tied(z_all, y_own, up[1])
    up = (up[0], up_there)

    kept, tiles = run(
        part(sub_turn, pairs, layers, levels),
        (shape(F32, 2, cols, pair_rows), shape(BF16, nrow, cols, pair_rows)),
        (where, layer_subtree, sub_pattern),
        (z_all, y_own, *up),
        (pltpu.VMEM(z_all.shape, F32),),
    )
    tiles = exchange(tiles, "row")

    def out_slice(which):
        start = (z * CORES + which) * out_rows
        return lax.dynamic_slice_in_dim(z_all, start, out_rows, 2)[:, :anc_count].transpose(1, 2, 0)

    def joined(here, there):
        flipped = core == 1
        return jnp.concatenate([jnp.where(flipped, there, here), jnp.where(flipped, here, there)], -1)

    anc_out = joined(out_slice(core), swapped(out_slice(1 - core))).astype(F32)

    root, tiles = run(
        sub_root_back,
        (shape(F32, cols, wide), shape(BF16, nz, cols, wide)),
        (),
        (tiles, *up),
    )
    tiles = exchange(tiles, "z")
    tiles = run(
        part(sub_leaf_back, pairs),
        shape(BF16, nrow, 2, cols, pair_rows),
        (sub_pattern,),
        (tiles, kept, *up),
    )
    tiles = exchange(tiles, "row")
    packed = -(-SUB_NODES * cols // 128) * 128
    tiles = run(
        sub_finish,
        shape(BF16, nz * CORES, out_rows, packed),
        (),
        (tiles, root, *up),
    )
    tiles = exchange(tiles, ("z", "core"))
    sums = jnp.sum(tiles.astype(F32).reshape(nz, CORES, out_rows, packed), 0)
    sums = sums[:, :, : SUB_NODES * cols].reshape(CORES, out_rows, SUB_NODES, cols)
    sub_out = sums.transpose(2, 1, 0, 3).reshape(SUB_NODES, out_rows, CORES * cols)
    return anc_out, sub_out


def solution(mesh):
    sizes = dict(mesh.shape)
    devices = mesh.devices.reshape(sizes["gz"], sizes["row"], sizes["col"] // CORES, CORES)
    split = Mesh(devices, ("gz", "row", "z", "core"))
    col = ("z", "core")
    in_specs = (
        P(None, col, "row"),
        P(None, col, "row"),
        P("gz", col, "row"),
        P("gz", col, "row"),
        P(None, col, None),
        P("gz", col, None),
        P(),
        P("gz", None),
    )
    out_specs = (P(None, ("row", "z", "core"), None), P("gz", ("row", "z", "core"), None))

    return jax.shard_map(local, mesh=split, in_specs=in_specs, out_specs=out_specs, check_vma=False)
```

```python
import functools

import jax
import jax.numpy as jnp
from jax import lax
from jax.experimental import pallas as pl
from jax.experimental.pallas import tpu as pltpu
from jax.sharding import Mesh, PartitionSpec as P


SUB_NODES = 3
LEAVES = (1, 2)
CORES = 2
ROWS8 = 8
F32 = jnp.float32
BF16 = jnp.bfloat16
VMEM_BYTES = 12 * 2**20


def level_span(depth):
    return 2**depth - 1, 2 ** (depth + 1) - 1


def depth_of(node):
    return (node + 1).bit_length() - 1


def above(node, level):
    return ((node + 1) >> (depth_of(node) - level)) - 1


def swapped(array):
    return lax.ppermute(array, "core", [(0, 1), (1, 0)])


def shape(dtype, *dims):
    return jax.ShapeDtypeStruct(dims, dtype)


def run(body, outs, smem, vmem, scratch=(), far=()):
    in_specs = [pl.BlockSpec(memory_space=pltpu.SMEM)] * len(smem)
    in_specs += [pl.BlockSpec(memory_space=pltpu.VMEM)] * len(vmem)
    in_specs += [pl.BlockSpec(memory_space=pltpu.HBM)] * len(far)
    far = [pltpu.with_memory_space_constraint(array, pltpu.HBM) for array in far]
    single = not isinstance(outs, (list, tuple))
    spec = pl.BlockSpec(memory_space=pltpu.VMEM)
    return pl.pallas_call(
        body,
        out_shape=outs,
        in_specs=in_specs,
        out_specs=spec if single else [spec] * len(outs),
        scratch_shapes=list(scratch),
        compiler_params=pltpu.CompilerParams(vmem_limit_bytes=VMEM_BYTES),
    )(*smem, *vmem, *far)


def total(tiles_ref):
    value = tiles_ref[0].astype(F32)
    for i in range(1, tiles_ref.shape[0]):
        value = value + tiles_ref[i].astype(F32)
    return value


def to_all(out_ref, value):
    value = value.astype(out_ref.dtype)
    for i in range(out_ref.shape[0]):
        out_ref[i] = value


def block(own_ref, other_ref, index):
    return jnp.concatenate([own_ref[index], other_ref[index]], 0)


def times(v, matrix):
    return lax.dot_general(v, matrix, (((1,), (0,)), ((), ())), preferred_element_type=F32)


def times_t(v, matrix):
    return lax.dot_general(v, matrix, (((1,), (1,)), ((), ())), preferred_element_type=F32)


def in_row(v, row):
    rows = lax.broadcasted_iota(jnp.int32, v.shape, 0)
    return jnp.where(rows == row, v, 0.0)


def own_first(v, core):
    return jnp.where(core == 1, pltpu.roll(v, v.shape[1] // 2, 1), v)


def position():
    return lax.axis_index("core"), lax.axis_index("z")


class Pairs:
    def __init__(self, levels, anc_count):
        self.sub = {}
        for m in range(SUB_NODES):
            for kind, count in ((0, levels), (1, depth_of(m))):
                for u in range(count):
                    self.sub[m, kind, u] = len(self.sub)
        self.anc = {}
        for a in range(anc_count):
            for u in range(depth_of(a)):
                self.anc[a, u] = anc_count + len(self.anc)


def sub_leaf_solve(there, other, own, here, rhs, out, near, near_rhs, sems):
    first, count = LEAVES[0], len(LEAVES)
    copies = [
        pltpu.make_async_copy(own.at[pl.ds(first, count)], near, sems.at[0]),
        pltpu.make_async_copy(here, near_rhs, sems.at[1]),
    ]
    for copy in copies:
        copy.start()
    for copy in copies:
        copy.wait()
    core = lax.axis_index("core")
    cols = rhs.shape[1]
    for m in range(SUB_NODES):
        flipped = jnp.concatenate([near_rhs[m], there[m]], 0).astype(F32).T
        rhs[m] = jnp.where(core == 0, flipped[:cols], flipped[cols:]).astype(BF16)
    for m in LEAVES:
        both = jnp.concatenate([near[m - first], other[m]], 0)
        part = times(rhs[m], both).astype(BF16)
        for i in range(out.shape[0]):
            out[i, m - 1] = part


def sub_low(y, w, pairs, own, other, m, kind, u):
    p = pairs.sub[m, kind, u]
    return w[p : p + 1, :] * times_t(y, block(own, other, SUB_NODES + p))


def sub_leaf_update(pairs, w, tiles, local_low, other, y_out, out):
    y = total(tiles).astype(BF16)
    y_out[...] = y
    value = 0.0
    for i, m in enumerate(LEAVES):
        p = pairs.sub[m, 1, 0]
        both = jnp.concatenate([local_low[i], other[SUB_NODES + p]], 0)
        value = value + w[p : p + 1, :] * times_t(y[i], both)
    to_all(out, value)


def sub_leaf_anc(pairs, levels, w, y, own, other, out):
    for e in range(levels):
        out[e] = sum(sub_low(y[m - 1], w, pairs, own, other, m, 0, e) for m in LEAVES)


def sub_root_solve(tiles, rhs, own, other, out):
    given = (rhs[0].astype(F32) - total(tiles)).astype(BF16)
    to_all(out, times(given, block(own, other, 0)))


def sub_root_anc(pairs, levels, w, tiles, so_far, own, other, y_out, out, scratch):
    y = total(tiles).astype(BF16)
    y_out[...] = y
    scratch[...] = jnp.zeros_like(scratch)
    for e in range(levels):
        scratch[:, e, :] = so_far[e] + sub_low(y, w, pairs, own, other, 0, 0, e)
    out[...] = scratch[...].astype(BF16)


def fetch(blocks, core, gathered, near, near_x, sems):
    wide = gathered.shape[3]
    copies = []
    at = 0
    while at < len(blocks):
        count = 1
        while at + count < len(blocks) and blocks[at + count] == blocks[at] + count:
            count += 1
        for r in range(gathered.shape[0] // CORES):
            for which, target in ((core, near), (1 - core, near_x)):
                copies.append(
                    pltpu.make_async_copy(
                        gathered.at[r * CORES + which, pl.ds(blocks[at], count)],
                        target.at[pl.ds(at, count), :, pl.ds(r * wide, wide)],
                        sems.at[len(copies)],
                    )
                )
        at += count
    for copy in copies:
        copy.start()
    return copies


def load_blocks(blocks, where, gathered, near, near_x, sems):
    for copy in fetch(blocks, where[0], gathered, near, near_x, sems):
        copy.wait()


def solve_level(depth, v8, offset, near, near_x, out, scratch):
    first, stop = level_span(depth)
    value = jnp.zeros_like(scratch)
    for i, a in enumerate(range(first, stop)):
        value = value + in_row(times(v8, block(near, near_x, offset + i)), a)
    scratch[...] = value
    to_all(out, scratch[first : first + out.shape[1], :])


def ancestor(subtree, g, layers, levels, e):
    return lax.shift_right_logical(subtree[g] + layers, levels - e) - 1


def anc_prepare(pairs, layers, nrow, where, subtree, pattern, here, there, blocks, *outs):
    choose, out, low_w, up_w, pick, local_low, sems = outs
    copies = [
        pltpu.make_async_copy(
            blocks.at[SUB_NODES + pairs.sub[m, 1, 0]], local_low.at[i], sems.at[i]
        )
        for i, m in enumerate(LEAVES)
    ]
    for copy in copies:
        copy.start()
    levels = choose.shape[0]
    for target, column in ((low_w, 0), (up_w, 1)):
        for p in range(pattern.shape[0]):
            weight = pattern[p, column].astype(F32)
            target[p : p + 1, :] = jnp.full((1, target.shape[1]), weight, F32)
    nodes = lax.broadcasted_iota(jnp.int32, pick.shape[1:], 0)
    for e in range(levels):
        ours = nodes == ancestor(subtree, where[4], layers, levels, e)
        pick[e] = jnp.where(ours, 1.0, 0.0)
    rows = lax.broadcasted_iota(jnp.int32, choose.shape[1:], 0)
    source = lax.broadcasted_iota(jnp.int32, choose.shape[1:], 1)
    for e in range(levels):
        value = jnp.zeros(choose.shape[1:], F32)
        for g in range(layers):
            ours = (source >= g * nrow) & (source < (g + 1) * nrow)
            hit = ours & (rows == ancestor(subtree, g, layers, levels, e))
            value = jnp.where(hit, 1.0, value)
        choose[e] = value
    lanes = lax.broadcasted_iota(jnp.int32, (ROWS8, here.shape[2]), 1)
    pick = jnp.where(lanes == where[5], 1.0, 0.0).astype(BF16)
    value = jnp.zeros_like(out)
    for a in range(here.shape[0]):
        value = value + in_row(times_t(pick, block(here, there, a)), a)
    out[...] = value
    for copy in copies:
        copy.wait()


def anc_first(depth, tiles, choose, given, near, near_x, acc_out, out, scratch, arrived):
    arrived[...] = tiles[...].astype(F32)
    acc = given[...]
    for e in range(choose.shape[0]):
        acc = acc - lax.dot_general(
            choose[e],
            arrived[:, e, :],
            (((1,), (0,)), ((), ())),
            precision=lax.Precision.HIGHEST,
            preferred_element_type=F32,
        )
    acc_out[...] = acc
    solve_level(depth, acc.astype(BF16), 0, near, near_x, out, scratch)


def pair_sum(depth, u, values, offset, blocks, down):
    first, stop = level_span(depth)
    result = 0.0
    for i, d in enumerate(range(first, stop)):
        source, target = (d, above(d, u)) if down else (above(d, u), d)
        v = jnp.broadcast_to(values[source : source + 1, :], values.shape)
        v = in_row(v, target).astype(BF16)
        result = result + times_t(v, block(*blocks, offset + i))
    return result


def level_rows(depth, tiles, out):
    first, stop = level_span(depth)
    out[...] = jnp.zeros_like(out)
    out[first:stop, :] = total(tiles)[: stop - first].astype(BF16).astype(F32)


def anc_forward(depth, tiles, acc_in, near, near_x, y_out, acc_out, out, scratch):
    level_rows(depth, tiles, y_out)
    acc = acc_in[...] - pair_sum(depth, depth - 1, y_out, 0, (near, near_x), True)
    acc_out[...] = acc
    solve_level(depth - 1, acc.astype(BF16), 2**depth, near, near_x, out, scratch)


def other_pairs(blocks, depth, down, where, values, acc_in, gathered, acc_out, near, near_x, sems):
    copies = fetch(blocks, where[0], gathered, near, near_x, sems)
    acc = acc_in[...]
    for copy in copies:
        copy.wait()
    for u in range(depth - 1):
        acc = acc - pair_sum(depth, u, values, u * 2**depth, (near, near_x), down)
    acc_out[...] = acc


def z_rows(values, rows):
    core, z = position()
    return own_first(values[:, pl.ds(pl.multiple_of(z * rows, rows), rows)], core)


def anc_turn(tiles, near, near_x, y_out, out, scratch):
    level_rows(0, tiles, y_out)
    t = z_rows(y_out, near.shape[1] * CORES)
    solve_level(0, t.astype(BF16), 0, near, near_x, out, scratch)


def anc_start(*refs):
    out = refs[-1]
    out[...] = sum(z_rows(values, out.shape[1]) for values in refs[:-1])


def added(*refs):
    refs[-1][...] = sum(values[...] for values in refs[:-1])


def anc_backward(depth, tiles, acc_in, near, near_x, z_out, out, scratch):
    level_rows(depth - 1, tiles, z_out)
    acc = acc_in[...] - pair_sum(depth, depth - 1, z_out, 0, (near, near_x), False)
    solve_level(depth, acc.astype(BF16), 2**depth, near, near_x, out, scratch)


def sub_pieces(where, y_root, y_leaf, out):
    core, held, base = where[0], where[2], where[3]
    rows = out.shape[2]
    span = pl.ds(pl.multiple_of(base, rows), rows)
    scale = held.astype(F32)
    for m in range(SUB_NODES):
        y = y_root[:, span] if m == 0 else y_leaf[m - 1, :, span]
        out[m] = scale * own_first(y.astype(F32), core)


def anc_spread(depth, nrow, tiles, z_in, out, scratch):
    first, stop = level_span(depth)
    scratch[...] = z_in[...]
    scratch[first:stop, :] = total(tiles)
    wide = out.shape[2]
    for i in range(out.shape[0]):
        r = i % nrow
        out[i] = scratch[:, r * wide : (r + 1) * wide].astype(BF16)


def sub_turn(pairs, levels, w, pick, tiles, y_own, own, other, kept, out, scratch):
    scratch[...] = tiles[...].astype(F32)
    picked = []
    for e in range(levels):
        value = 0.0
        for a in range(*level_span(e)):
            value = value + pick[e, a : a + 1, :] * scratch[:, a, :]
        picked.append(value.astype(BF16))
    for m in range(SUB_NODES):
        value = y_own[m]
        for e in range(levels):
            p = pairs.sub[m, 0, e]
            value = value - w[p : p + 1, :] * times_t(picked[e], block(own, other, SUB_NODES + p))
        if m == 0:
            to_all(out, value)
        else:
            kept[m - 1] = value


def sub_root_back(tiles, own, other, kept, out):
    value = times(total(tiles).astype(BF16), block(own, other, 0))
    kept[...] = value
    to_all(out, value)


def sub_leaf_back(pairs, w, tiles, kept, own, other, out):
    z = total(tiles).astype(BF16)
    for m in LEAVES:
        p = pairs.sub[m, 1, 0]
        value = kept[m - 1] - w[p : p + 1, :] * times_t(z, block(own, other, SUB_NODES + p))
        for i in range(out.shape[0]):
            out[i, m - 1] = value.astype(BF16)


def sub_finish(tiles, root, own, other, out):
    t = total(tiles).astype(BF16)
    parts = [root[...]] + [times(t[m - 1], block(own, other, m)) for m in LEAVES]
    fill = out.shape[2] - sum(part.shape[0] for part in parts)
    if fill:
        parts.append(jnp.zeros((fill, parts[0].shape[1]), F32))
    flipped = jnp.concatenate(parts, 0).T
    out[...] = flipped.reshape(out.shape).astype(BF16)


def local(anc_lower, anc_upper, sub_lower, sub_upper, anc_rhs, sub_rhs, layer_subtree, sub_pattern):
    layers = lax.axis_size("gz")
    levels = layers.bit_length() - 1
    anc_count = layers - 1
    nrow, nz = lax.axis_size("row"), lax.axis_size("z")
    own, wide = sub_lower.shape[1:]
    size = wide * nrow
    pair_rows = own * CORES
    out_rows = wide // (nz * CORES)
    cols = sub_rhs.shape[2] // CORES
    g, r, z, core = (lax.axis_index(name) for name in ("gz", "row", "z", "core"))
    pairs = Pairs(levels, anc_count)
    part = functools.partial
    scr8 = pltpu.VMEM((ROWS8, size), F32)

    held = (r == z * nrow // nz).astype(jnp.int32)
    base = jnp.clip(z * pair_rows - r * wide, 0, wide - pair_rows)
    where = jnp.stack([core, z, held, base, g, core * cols + g * nrow + r]).astype(jnp.int32)

    def gathered(blocks):
        return lax.all_gather(blocks, ("row", "core"), axis=0, tiled=False)

    def exchange(array, axes):
        return lax.all_to_all(array, axes, 0, 0, tiled=True)

    def two_cores(array):
        return array, swapped(array)

    def tied(send, *others):
        return lax.optimization_barrier((send, *others))

    low = (sub_lower, swapped(sub_lower))
    rhs_there = swapped(sub_rhs)
    anc_low = gathered(anc_lower)

    def diagonal(depth):
        return list(range(*level_span(depth)))

    def pair_blocks(depth, u):
        return [pairs.anc[a, u] for a in range(*level_span(depth))]

    def loaded(blocks, stack):
        near = shape(BF16, len(blocks), own, size)
        sems = pltpu.SemaphoreType.DMA((len(blocks) * nrow * CORES,))
        return run(part(load_blocks, blocks), (near, near), (where,), (), (sems,), (stack,))

    def others(depth, down, values, acc, stack):
        blocks = [index for u in range(depth - 1) for index in pair_blocks(depth, u)]
        near = pltpu.VMEM((len(blocks), own, size), BF16)
        sems = pltpu.SemaphoreType.DMA((len(blocks) * nrow * CORES,))
        body = part(other_pairs, blocks, depth, down)
        return run(body, acc_shape, (where,), (values, acc), (near, near, sems), (stack,))

    def level_shape(depth):
        return shape(BF16, nz, max(2, 2**depth), size)

    acc_shape = shape(F32, ROWS8, pair_rows)
    row_shape = shape(F32, ROWS8, size)

    rhs, tiles = run(
        sub_leaf_solve,
        (shape(BF16, SUB_NODES, cols, pair_rows), shape(BF16, nz, 2, cols, wide)),
        (),
        (rhs_there, low[1]),
        (
            pltpu.VMEM((len(LEAVES), own, wide), BF16),
            pltpu.VMEM(sub_rhs.shape, BF16),
            pltpu.SemaphoreType.DMA((2,)),
        ),
        (sub_lower, sub_rhs),
    )
    tiles, anc_rhs = tied(tiles, anc_rhs)
    anc_there = swapped(anc_rhs)
    weights = shape(F32, sub_pattern.shape[0], pair_rows)
    choose, given8, low_w, up_w, pick, local_low = run(
        part(anc_prepare, pairs, layers, nrow),
        (
            shape(F32, levels, ROWS8, layers * nrow),
            acc_shape,
            weights,
            weights,
            shape(F32, levels, ROWS8, wide),
            shape(BF16, len(LEAVES), own, wide),
        ),
        (where, layer_subtree, sub_pattern),
        (anc_rhs, anc_there),
        (pltpu.SemaphoreType.DMA((len(LEAVES),)),),
        (sub_lower,),
    )
    given8, anc_upper = tied(given8, anc_upper)
    anc_up = gathered(anc_upper)
    tiles = exchange(tiles, "z")
    tiles, given8, choose, low_w, local_low = tied(tiles, given8, choose, low_w, local_low)
    y_leaf, tiles = run(
        part(sub_leaf_update, pairs),
        (shape(BF16, 2, cols, wide), shape(BF16, nrow, cols, pair_rows)),
        (),
        (low_w, tiles, local_low, low[1]),
    )
    tiles = exchange(tiles, "row")
    so_far = run(
        part(sub_leaf_anc, pairs, levels),
        shape(F32, levels, cols, pair_rows),
        (),
        (low_w, y_leaf, *low),
    )
    tiles, so_far = tied(tiles, so_far)
    tiles = run(sub_root_solve, shape(BF16, nz, cols, wide), (), (tiles, rhs, *low))
    tiles = exchange(tiles, "z")
    c_scratch = pltpu.VMEM((layers * nrow, ROWS8, pair_rows), F32)
    y_root, tiles = run(
        part(sub_root_anc, pairs, levels),
        (shape(BF16, cols, wide), shape(BF16, layers * nrow, ROWS8, pair_rows)),
        (),
        (low_w, tiles, so_far, *low),
        (c_scratch,),
    )
    tiles = exchange(tiles, ("gz", "row"))
    near = loaded(diagonal(levels - 1), anc_low)
    tiles, *near = tied(tiles, *near)

    acc, tiles = run(
        part(anc_first, levels - 1),
        (acc_shape, level_shape(levels - 1)),
        (),
        (tiles, choose, given8, *near),
        (scr8, c_scratch),
    )
    tiles = exchange(tiles, "z")
    y_parts = []
    for depth in range(levels - 1, 0, -1):
        blocks = pair_blocks(depth, depth - 1) + diagonal(depth - 1)
        near = loaded(blocks, anc_low)
        tiles, *near = tied(tiles, *near)
        y8, acc, tiles = run(
            part(anc_forward, depth),
            (row_shape, acc_shape, level_shape(depth - 1)),
            (),
            (tiles, acc, *near),
            (scr8,),
        )
        y_parts.append(y8)
        tiles = exchange(tiles, "z")
        if depth > 1:
            acc = others(depth, True, y8, acc, anc_low)
            tiles, acc = tied(tiles, acc)
    near = loaded(diagonal(0), anc_up)
    tiles, *near = tied(tiles, *near)
    y8, tiles = run(
        anc_turn, (row_shape, level_shape(0)), (), (tiles, *near), (scr8,)
    )
    y_parts.append(y8)
    tiles = exchange(tiles, "z")
    start8 = run(anc_start, acc_shape, (), y_parts)
    tiles, start8 = tied(tiles, start8)
    z8 = None
    for depth in range(1, levels):
        acc = start8
        blocks = pair_blocks(depth, depth - 1) + diagonal(depth)
        near = loaded(blocks, anc_up)
        tiles, *near = tied(tiles, *near)
        if depth > 1:
            acc = others(depth, False, z8, acc, anc_up)
            tiles, acc = tied(tiles, acc)
        z_now, tiles = run(
            part(anc_backward, depth),
            (row_shape, level_shape(depth)),
            (),
            (tiles, acc, *near),
            (scr8,),
        )
        if depth == levels - 1:
            tiles, sub_upper = tied(tiles, sub_upper)
        tiles = exchange(tiles, "z")
        if z8 is None:
            z8 = z_now
        else:
            z8 = run(added, row_shape, (), (z8, z_now))
            tiles, z8 = tied(tiles, z8)
    up = two_cores(sub_upper)
    tiles = run(
        part(anc_spread, levels - 1, nrow),
        shape(BF16, layers * nrow, ROWS8, wide),
        (),
        (tiles, z8),
        (scr8,),
    )
    z_all = exchange(tiles, ("gz", "row"))
    y_own = run(sub_pieces, shape(F32, SUB_NODES, cols, pair_rows), (where,), (y_root, y_leaf))
    z_all, y_own, up_there, up_w, pick = tied(z_all, y_own, up[1], up_w, pick)
    up = (up[0], up_there)

    kept, tiles = run(
        part(sub_turn, pairs, levels),
        (shape(F32, 2, cols, pair_rows), shape(BF16, nrow, cols, pair_rows)),
        (),
        (up_w, pick, z_all, y_own, *up),
        (pltpu.VMEM(z_all.shape, F32),),
    )
    tiles = exchange(tiles, "row")

    def out_slice(which):
        start = (z * CORES + which) * out_rows
        return lax.dynamic_slice_in_dim(z_all, start, out_rows, 2)[:, :anc_count].transpose(1, 2, 0)

    def joined(here, there):
        flipped = core == 1
        return jnp.concatenate([jnp.where(flipped, there, here), jnp.where(flipped, here, there)], -1)

    anc_out = joined(out_slice(core), swapped(out_slice(1 - core))).astype(F32)

    root, tiles = run(
        sub_root_back,
        (shape(F32, cols, wide), shape(BF16, nz, cols, wide)),
        (),
        (tiles, *up),
    )
    tiles = exchange(tiles, "z")
    tiles = run(
        part(sub_leaf_back, pairs),
        shape(BF16, nrow, 2, cols, pair_rows),
        (),
        (up_w, tiles, kept, *up),
    )
    tiles = exchange(tiles, "row")
    packed = -(-SUB_NODES * cols // 128) * 128
    tiles = run(
        sub_finish,
        shape(BF16, nz * CORES, out_rows, packed),
        (),
        (tiles, root, *up),
    )
    tiles = exchange(tiles, ("z", "core"))
    sums = jnp.sum(tiles.astype(F32).reshape(nz, CORES, out_rows, packed), 0)
    sums = sums[:, :, : SUB_NODES * cols].reshape(CORES, out_rows, SUB_NODES, cols)
    sub_out = sums.transpose(2, 1, 0, 3).reshape(SUB_NODES, out_rows, CORES * cols)
    return anc_out, sub_out


def solution(mesh):
    sizes = dict(mesh.shape)
    devices = mesh.devices.reshape(sizes["gz"], sizes["row"], sizes["col"] // CORES, CORES)
    split = Mesh(devices, ("gz", "row", "z", "core"))
    col = ("z", "core")
    in_specs = (
        P(None, col, "row"),
        P(None, col, "row"),
        P("gz", col, "row"),
        P("gz", col, "row"),
        P(None, col, None),
        P("gz", col, None),
        P(),
        P("gz", None),
    )
    out_specs = (P(None, ("row", "z", "core"), None), P("gz", ("row", "z", "core"), None))

    return jax.shard_map(local, mesh=split, in_specs=in_specs, out_specs=out_specs, check_vma=False)
```

```python
import functools

import jax
import jax.numpy as jnp
from jax import lax
from jax.experimental import pallas as pl
from jax.experimental.pallas import tpu as pltpu
from jax.sharding import Mesh, PartitionSpec as P


SUB_NODES = 3
LEAVES = (1, 2)
CORES = 2
ROWS8 = 8
F32 = jnp.float32
BF16 = jnp.bfloat16
VMEM_BYTES = 12 * 2**20


def level_span(depth):
    return 2**depth - 1, 2 ** (depth + 1) - 1


def depth_of(node):
    return (node + 1).bit_length() - 1


def above(node, level):
    return ((node + 1) >> (depth_of(node) - level)) - 1


def swapped(array):
    return lax.ppermute(array, "core", [(0, 1), (1, 0)])


def shape(dtype, *dims):
    return jax.ShapeDtypeStruct(dims, dtype)


def run(body, outs, smem, vmem, scratch=(), far=()):
    in_specs = [pl.BlockSpec(memory_space=pltpu.SMEM)] * len(smem)
    in_specs += [pl.BlockSpec(memory_space=pltpu.VMEM)] * len(vmem)
    in_specs += [pl.BlockSpec(memory_space=pltpu.HBM)] * len(far)
    far = [pltpu.with_memory_space_constraint(array, pltpu.HBM) for array in far]
    single = not isinstance(outs, (list, tuple))
    spec = pl.BlockSpec(memory_space=pltpu.VMEM)
    return pl.pallas_call(
        body,
        out_shape=outs,
        in_specs=in_specs,
        out_specs=spec if single else [spec] * len(outs),
        scratch_shapes=list(scratch),
        compiler_params=pltpu.CompilerParams(vmem_limit_bytes=VMEM_BYTES),
    )(*smem, *vmem, *far)


def total(tiles_ref):
    value = tiles_ref[0].astype(F32)
    for i in range(1, tiles_ref.shape[0]):
        value = value + tiles_ref[i].astype(F32)
    return value


def to_all(out_ref, value):
    value = value.astype(out_ref.dtype)
    for i in range(out_ref.shape[0]):
        out_ref[i] = value


def block(own_ref, other_ref, index):
    return jnp.concatenate([own_ref[index], other_ref[index]], 0)


def times(v, matrix):
    return lax.dot_general(v, matrix, (((1,), (0,)), ((), ())), preferred_element_type=F32)


def times_t(v, matrix):
    return lax.dot_general(v, matrix, (((1,), (1,)), ((), ())), preferred_element_type=F32)


def in_row(v, row):
    rows = lax.broadcasted_iota(jnp.int32, v.shape, 0)
    return jnp.where(rows == row, v, 0.0)


def own_first(v, core):
    return jnp.where(core == 1, pltpu.roll(v, v.shape[1] // 2, 1), v)


def position():
    return lax.axis_index("core"), lax.axis_index("z")


class Pairs:
    def __init__(self, levels, anc_count):
        self.sub = {}
        for m in range(SUB_NODES):
            for kind, count in ((0, levels), (1, depth_of(m))):
                for u in range(count):
                    self.sub[m, kind, u] = len(self.sub)
        self.anc = {}
        for a in range(anc_count):
            for u in range(depth_of(a)):
                self.anc[a, u] = anc_count + len(self.anc)


def sub_leaf_solve(there, other, own, here, rhs, out, near, near_rhs, sems):
    first, count = LEAVES[0], len(LEAVES)
    copies = [
        pltpu.make_async_copy(own.at[pl.ds(first, count)], near, sems.at[0]),
        pltpu.make_async_copy(here, near_rhs, sems.at[1]),
    ]
    for copy in copies:
        copy.start()
    for copy in copies:
        copy.wait()
    core = lax.axis_index("core")
    cols = rhs.shape[1]
    for m in range(SUB_NODES):
        flipped = jnp.concatenate([near_rhs[m], there[m]], 0).astype(F32).T
        rhs[m] = jnp.where(core == 0, flipped[:cols], flipped[cols:]).astype(BF16)
    for m in LEAVES:
        both = jnp.concatenate([near[m - first], other[m]], 0)
        part = times(rhs[m], both).astype(BF16)
        for i in range(out.shape[0]):
            out[i, m - 1] = part


def sub_low(y, w, pairs, own, other, m, kind, u):
    p = pairs.sub[m, kind, u]
    return w[p : p + 1, :] * times_t(y, block(own, other, SUB_NODES + p))


def sub_leaf_update(pairs, w, tiles, local_low, other, y_out, out):
    y = total(tiles).astype(BF16)
    y_out[...] = y
    value = 0.0
    for i, m in enumerate(LEAVES):
        p = pairs.sub[m, 1, 0]
        both = jnp.concatenate([local_low[i], other[SUB_NODES + p]], 0)
        value = value + w[p : p + 1, :] * times_t(y[i], both)
    to_all(out, value)


def sub_root_solve(tiles, rhs, own, other, out):
    given = (rhs[0].astype(F32) - total(tiles)).astype(BF16)
    to_all(out, times(given, block(own, other, 0)))


def sub_root_anc(pairs, levels, w, tiles, y_leaf, own, other, y_out, out, scratch):
    y = total(tiles).astype(BF16)
    y_out[...] = y
    scratch[...] = jnp.zeros_like(scratch)
    for e in range(levels):
        value = sub_low(y, w, pairs, own, other, 0, 0, e)
        for m in LEAVES:
            value = value + sub_low(y_leaf[m - 1], w, pairs, own, other, m, 0, e)
        scratch[:, e, :] = value
    out[...] = scratch[...].astype(BF16)


def fetch(blocks, core, gathered, near, near_x, sems):
    wide = gathered.shape[3]
    copies = []
    at = 0
    while at < len(blocks):
        count = 1
        while at + count < len(blocks) and blocks[at + count] == blocks[at] + count:
            count += 1
        for r in range(gathered.shape[0] // CORES):
            for which, target in ((core, near), (1 - core, near_x)):
                copies.append(
                    pltpu.make_async_copy(
                        gathered.at[r * CORES + which, pl.ds(blocks[at], count)],
                        target.at[pl.ds(at, count), :, pl.ds(r * wide, wide)],
                        sems.at[len(copies)],
                    )
                )
        at += count
    for copy in copies:
        copy.start()
    return copies


def load_blocks(blocks, where, gathered, near, near_x, sems):
    for copy in fetch(blocks, where[0], gathered, near, near_x, sems):
        copy.wait()


def solve_level(depth, v8, offset, near, near_x, out, scratch):
    first, stop = level_span(depth)
    value = jnp.zeros_like(scratch)
    for i, a in enumerate(range(first, stop)):
        value = value + in_row(times(v8, block(near, near_x, offset + i)), a)
    scratch[...] = value
    to_all(out, scratch[first : first + out.shape[1], :])


def ancestor(subtree, g, layers, levels, e):
    return lax.shift_right_logical(subtree[g] + layers, levels - e) - 1


def anc_prepare(pairs, layers, nrow, where, subtree, pattern, here, there, blocks, *outs):
    choose, out, low_w, up_w, pick, local_low, sems = outs
    copies = [
        pltpu.make_async_copy(
            blocks.at[SUB_NODES + pairs.sub[m, 1, 0]], local_low.at[i], sems.at[i]
        )
        for i, m in enumerate(LEAVES)
    ]
    for copy in copies:
        copy.start()
    levels = choose.shape[0]
    for target, column in ((low_w, 0), (up_w, 1)):
        for p in range(pattern.shape[0]):
            weight = pattern[p, column].astype(F32)
            target[p : p + 1, :] = jnp.full((1, target.shape[1]), weight, F32)
    nodes = lax.broadcasted_iota(jnp.int32, pick.shape[1:], 0)
    for e in range(levels):
        ours = nodes == ancestor(subtree, where[4], layers, levels, e)
        pick[e] = jnp.where(ours, 1.0, 0.0)
    rows = lax.broadcasted_iota(jnp.int32, choose.shape[1:], 0)
    source = lax.broadcasted_iota(jnp.int32, choose.shape[1:], 1)
    for e in range(levels):
        value = jnp.zeros(choose.shape[1:], F32)
        for g in range(layers):
            ours = (source >= g * nrow) & (source < (g + 1) * nrow)
            hit = ours & (rows == ancestor(subtree, g, layers, levels, e))
            value = jnp.where(hit, 1.0, value)
        choose[e] = value
    lanes = lax.broadcasted_iota(jnp.int32, (ROWS8, here.shape[2]), 1)
    pick = jnp.where(lanes == where[5], 1.0, 0.0).astype(BF16)
    value = jnp.zeros_like(out)
    for a in range(here.shape[0]):
        value = value + in_row(times_t(pick, block(here, there, a)), a)
    out[...] = value
    for copy in copies:
        copy.wait()


def anc_first(depth, tiles, choose, given, near, near_x, acc_out, out, scratch, arrived):
    arrived[...] = tiles[...].astype(F32)
    acc = given[...]
    for e in range(choose.shape[0]):
        acc = acc - lax.dot_general(
            choose[e],
            arrived[:, e, :],
            (((1,), (0,)), ((), ())),
            precision=lax.Precision.HIGHEST,
            preferred_element_type=F32,
        )
    acc_out[...] = acc
    solve_level(depth, acc.astype(BF16), 0, near, near_x, out, scratch)


def pair_sum(depth, u, values, offset, blocks, down):
    first, stop = level_span(depth)
    result = 0.0
    for i, d in enumerate(range(first, stop)):
        source, target = (d, above(d, u)) if down else (above(d, u), d)
        v = jnp.broadcast_to(values[source : source + 1, :], values.shape)
        v = in_row(v, target).astype(BF16)
        result = result + times_t(v, block(*blocks, offset + i))
    return result


def level_rows(depth, tiles, out):
    first, stop = level_span(depth)
    out[...] = jnp.zeros_like(out)
    out[first:stop, :] = total(tiles)[: stop - first].astype(BF16).astype(F32)


def anc_forward(depth, tiles, acc_in, near, near_x, y_out, acc_out, out, scratch):
    level_rows(depth, tiles, y_out)
    acc = acc_in[...] - pair_sum(depth, depth - 1, y_out, 0, (near, near_x), True)
    acc_out[...] = acc
    solve_level(depth - 1, acc.astype(BF16), 2**depth, near, near_x, out, scratch)


def other_pairs(blocks, depth, down, where, values, acc_in, gathered, acc_out, near, near_x, sems):
    copies = fetch(blocks, where[0], gathered, near, near_x, sems)
    acc = acc_in[...]
    for copy in copies:
        copy.wait()
    for u in range(depth - 1):
        acc = acc - pair_sum(depth, u, values, u * 2**depth, (near, near_x), down)
    acc_out[...] = acc


def z_rows(values, rows):
    core, z = position()
    return own_first(values[:, pl.ds(pl.multiple_of(z * rows, rows), rows)], core)


def anc_turn(tiles, near, near_x, y_out, out, scratch):
    level_rows(0, tiles, y_out)
    t = z_rows(y_out, near.shape[1] * CORES)
    solve_level(0, t.astype(BF16), 0, near, near_x, out, scratch)


def anc_start(*refs):
    out = refs[-1]
    out[...] = sum(z_rows(values, out.shape[1]) for values in refs[:-1])


def added(*refs):
    refs[-1][...] = sum(values[...] for values in refs[:-1])


def anc_backward(depth, tiles, acc_in, near, near_x, z_out, out, scratch):
    level_rows(depth - 1, tiles, z_out)
    acc = acc_in[...] - pair_sum(depth, depth - 1, z_out, 0, (near, near_x), False)
    solve_level(depth, acc.astype(BF16), 2**depth, near, near_x, out, scratch)


def sub_pieces(where, y_root, y_leaf, out):
    core, held, base = where[0], where[2], where[3]
    rows = out.shape[2]
    span = pl.ds(pl.multiple_of(base, rows), rows)
    scale = held.astype(F32)
    for m in range(SUB_NODES):
        y = y_root[:, span] if m == 0 else y_leaf[m - 1, :, span]
        out[m] = scale * own_first(y.astype(F32), core)


def anc_spread(depth, nrow, tiles, z_in, out, scratch):
    first, stop = level_span(depth)
    scratch[...] = z_in[...]
    scratch[first:stop, :] = total(tiles)
    wide = out.shape[2]
    for i in range(out.shape[0]):
        r = i % nrow
        out[i] = scratch[:, r * wide : (r + 1) * wide].astype(BF16)


def sub_turn(pairs, levels, w, pick, tiles, y_own, own, other, kept, out, scratch):
    scratch[...] = tiles[...].astype(F32)
    picked = []
    for e in range(levels):
        value = 0.0
        for a in range(*level_span(e)):
            value = value + pick[e, a : a + 1, :] * scratch[:, a, :]
        picked.append(value.astype(BF16))
    for m in range(SUB_NODES):
        value = y_own[m]
        for e in range(levels):
            p = pairs.sub[m, 0, e]
            value = value - w[p : p + 1, :] * times_t(picked[e], block(own, other, SUB_NODES + p))
        if m == 0:
            to_all(out, value)
        else:
            kept[m - 1] = value


def anc_pieces(tiles, here, there, scratch):
    core, z = position()
    scratch[...] = tiles[...].astype(F32)
    rows = here.shape[1]
    line = lax.broadcasted_iota(jnp.int32, (rows, tiles.shape[2]), 0)
    lane = lax.broadcasted_iota(jnp.int32, (rows, tiles.shape[2]), 1)
    for out, which in ((here, core), (there, 1 - core)):
        pick = jnp.where(lane == (z * CORES + which) * rows + line, 1.0, 0.0).astype(BF16)
        for a in range(here.shape[0]):
            out[a] = times_t(pick, scratch[:, a, :].astype(BF16)).astype(BF16)


def sub_root_back(tiles, own, other, kept, out):
    value = times(total(tiles).astype(BF16), block(own, other, 0))
    kept[...] = value
    to_all(out, value)


def sub_leaf_back(pairs, w, tiles, kept, own, other, out):
    z = total(tiles).astype(BF16)
    for m in LEAVES:
        p = pairs.sub[m, 1, 0]
        value = kept[m - 1] - w[p : p + 1, :] * times_t(z, block(own, other, SUB_NODES + p))
        for i in range(out.shape[0]):
            out[i, m - 1] = value.astype(BF16)


def sub_finish(tiles, root, own, other, out):
    t = total(tiles).astype(BF16)
    parts = [root[...]] + [times(t[m - 1], block(own, other, m)) for m in LEAVES]
    fill = out.shape[2] - sum(part.shape[0] for part in parts)
    if fill:
        parts.append(jnp.zeros((fill, parts[0].shape[1]), F32))
    flipped = jnp.concatenate(parts, 0).T
    out[...] = flipped.reshape(out.shape).astype(BF16)


def local(anc_lower, anc_upper, sub_lower, sub_upper, anc_rhs, sub_rhs, layer_subtree, sub_pattern):
    layers = lax.axis_size("gz")
    levels = layers.bit_length() - 1
    anc_count = layers - 1
    nrow, nz = lax.axis_size("row"), lax.axis_size("z")
    own, wide = sub_lower.shape[1:]
    size = wide * nrow
    pair_rows = own * CORES
    out_rows = wide // (nz * CORES)
    cols = sub_rhs.shape[2] // CORES
    g, r, z, core = (lax.axis_index(name) for name in ("gz", "row", "z", "core"))
    pairs = Pairs(levels, anc_count)
    part = functools.partial
    scr8 = pltpu.VMEM((ROWS8, size), F32)

    held = (r == z * nrow // nz).astype(jnp.int32)
    base = jnp.clip(z * pair_rows - r * wide, 0, wide - pair_rows)
    where = jnp.stack([core, z, held, base, g, core * cols + g * nrow + r]).astype(jnp.int32)

    def gathered(blocks):
        return lax.all_gather(blocks, ("row", "core"), axis=0, tiled=False)

    def exchange(array, axes):
        return lax.all_to_all(array, axes, 0, 0, tiled=True)

    def two_cores(array):
        return array, swapped(array)

    def tied(send, *others):
        return lax.optimization_barrier((send, *others))

    low = (sub_lower, swapped(sub_lower))
    rhs_there = swapped(sub_rhs)
    anc_low = gathered(anc_lower)

    def diagonal(depth):
        return list(range(*level_span(depth)))

    def pair_blocks(depth, u):
        return [pairs.anc[a, u] for a in range(*level_span(depth))]

    def loaded(blocks, stack):
        near = shape(BF16, len(blocks), own, size)
        sems = pltpu.SemaphoreType.DMA((len(blocks) * nrow * CORES,))
        return run(part(load_blocks, blocks), (near, near), (where,), (), (sems,), (stack,))

    def others(depth, down, values, acc, stack):
        blocks = [index for u in range(depth - 1) for index in pair_blocks(depth, u)]
        near = pltpu.VMEM((len(blocks), own, size), BF16)
        sems = pltpu.SemaphoreType.DMA((len(blocks) * nrow * CORES,))
        body = part(other_pairs, blocks, depth, down)
        return run(body, acc_shape, (where,), (values, acc), (near, near, sems), (stack,))

    def level_shape(depth):
        return shape(BF16, nz, max(2, 2**depth), size)

    acc_shape = shape(F32, ROWS8, pair_rows)
    row_shape = shape(F32, ROWS8, size)

    rhs, tiles = run(
        sub_leaf_solve,
        (shape(BF16, SUB_NODES, cols, pair_rows), shape(BF16, nz, 2, cols, wide)),
        (),
        (rhs_there, low[1]),
        (
            pltpu.VMEM((len(LEAVES), own, wide), BF16),
            pltpu.VMEM(sub_rhs.shape, BF16),
            pltpu.SemaphoreType.DMA((2,)),
        ),
        (sub_lower, sub_rhs),
    )
    tiles, anc_rhs = tied(tiles, anc_rhs)
    anc_there = swapped(anc_rhs)
    weights = shape(F32, sub_pattern.shape[0], pair_rows)
    choose, given8, low_w, up_w, pick, local_low = run(
        part(anc_prepare, pairs, layers, nrow),
        (
            shape(F32, levels, ROWS8, layers * nrow),
            acc_shape,
            weights,
            weights,
            shape(F32, levels, ROWS8, wide),
            shape(BF16, len(LEAVES), own, wide),
        ),
        (where, layer_subtree, sub_pattern),
        (anc_rhs, anc_there),
        (pltpu.SemaphoreType.DMA((len(LEAVES),)),),
        (sub_lower,),
    )
    given8, anc_upper = tied(given8, anc_upper)
    anc_up = gathered(anc_upper)
    tiles = exchange(tiles, "z")
    tiles, given8, choose, low_w, local_low = tied(tiles, given8, choose, low_w, local_low)
    y_leaf, tiles = run(
        part(sub_leaf_update, pairs),
        (shape(BF16, 2, cols, wide), shape(BF16, nrow, cols, pair_rows)),
        (),
        (low_w, tiles, local_low, low[1]),
    )
    tiles = exchange(tiles, "row")
    tiles = run(sub_root_solve, shape(BF16, nz, cols, wide), (), (tiles, rhs, *low))
    tiles = exchange(tiles, "z")
    c_scratch = pltpu.VMEM((layers * nrow, ROWS8, pair_rows), F32)
    y_root, tiles = run(
        part(sub_root_anc, pairs, levels),
        (shape(BF16, cols, wide), shape(BF16, layers * nrow, ROWS8, pair_rows)),
        (),
        (low_w, tiles, y_leaf, *low),
        (c_scratch,),
    )
    tiles = exchange(tiles, ("gz", "row"))
    near = loaded(diagonal(levels - 1), anc_low)
    tiles, *near = tied(tiles, *near)

    acc, tiles = run(
        part(anc_first, levels - 1),
        (acc_shape, level_shape(levels - 1)),
        (),
        (tiles, choose, given8, *near),
        (scr8, c_scratch),
    )
    tiles = exchange(tiles, "z")
    y_parts = []
    for depth in range(levels - 1, 0, -1):
        blocks = pair_blocks(depth, depth - 1) + diagonal(depth - 1)
        near = loaded(blocks, anc_low)
        tiles, *near = tied(tiles, *near)
        y8, acc, tiles = run(
            part(anc_forward, depth),
            (row_shape, acc_shape, level_shape(depth - 1)),
            (),
            (tiles, acc, *near),
            (scr8,),
        )
        y_parts.append(y8)
        tiles = exchange(tiles, "z")
        if depth > 1:
            acc = others(depth, True, y8, acc, anc_low)
            tiles, acc = tied(tiles, acc)
    near = loaded(diagonal(0), anc_up)
    tiles, *near = tied(tiles, *near)
    y8, tiles = run(
        anc_turn, (row_shape, level_shape(0)), (), (tiles, *near), (scr8,)
    )
    y_parts.append(y8)
    tiles = exchange(tiles, "z")
    start8 = run(anc_start, acc_shape, (), y_parts)
    tiles, start8 = tied(tiles, start8)
    z8 = None
    for depth in range(1, levels):
        acc = start8
        blocks = pair_blocks(depth, depth - 1) + diagonal(depth)
        near = loaded(blocks, anc_up)
        tiles, *near = tied(tiles, *near)
        if depth > 1:
            acc = others(depth, False, z8, acc, anc_up)
            tiles, acc = tied(tiles, acc)
        z_now, tiles = run(
            part(anc_backward, depth),
            (row_shape, level_shape(depth)),
            (),
            (tiles, acc, *near),
            (scr8,),
        )
        if depth == levels - 1:
            tiles, sub_upper = tied(tiles, sub_upper)
        tiles = exchange(tiles, "z")
        if z8 is None:
            z8 = z_now
        else:
            z8 = run(added, row_shape, (), (z8, z_now))
            tiles, z8 = tied(tiles, z8)
    up = two_cores(sub_upper)
    tiles = run(
        part(anc_spread, levels - 1, nrow),
        shape(BF16, layers * nrow, ROWS8, wide),
        (),
        (tiles, z8),
        (scr8,),
    )
    z_all = exchange(tiles, ("gz", "row"))
    y_own = run(sub_pieces, shape(F32, SUB_NODES, cols, pair_rows), (where,), (y_root, y_leaf))
    z_all, y_own, up_there, up_w, pick = tied(z_all, y_own, up[1], up_w, pick)
    up = (up[0], up_there)

    kept, tiles = run(
        part(sub_turn, pairs, levels),
        (shape(F32, 2, cols, pair_rows), shape(BF16, nrow, cols, pair_rows)),
        (),
        (up_w, pick, z_all, y_own, *up),
        (pltpu.VMEM(z_all.shape, F32),),
    )
    tiles = exchange(tiles, "row")

    def joined(here, there):
        flipped = core == 1
        return jnp.concatenate([jnp.where(flipped, there, here), jnp.where(flipped, here, there)], -1)

    root, tiles = run(
        sub_root_back,
        (shape(F32, cols, wide), shape(BF16, nz, cols, wide)),
        (),
        (tiles, *up),
    )
    tiles = exchange(tiles, "z")
    tiles = run(
        part(sub_leaf_back, pairs),
        shape(BF16, nrow, 2, cols, pair_rows),
        (),
        (up_w, tiles, kept, *up),
    )
    tiles = exchange(tiles, "row")
    packed = -(-SUB_NODES * cols // 128) * 128
    tiles = run(
        sub_finish,
        shape(BF16, nz * CORES, out_rows, packed),
        (),
        (tiles, root, *up),
    )
    tiles = exchange(tiles, ("z", "core"))
    piece = shape(BF16, anc_count, out_rows, cols)
    out_here, out_there = run(
        anc_pieces, (piece, piece), (), (z_all,), (pltpu.VMEM(z_all.shape, F32),)
    )
    out_there = swapped(out_there)
    anc_out = joined(out_here, out_there).astype(F32)
    sums = jnp.sum(tiles.astype(F32).reshape(nz, CORES, out_rows, packed), 0)
    sums = sums[:, :, : SUB_NODES * cols].reshape(CORES, out_rows, SUB_NODES, cols)
    sub_out = sums.transpose(2, 1, 0, 3).reshape(SUB_NODES, out_rows, CORES * cols)
    return anc_out, sub_out


def solution(mesh):
    sizes = dict(mesh.shape)
    devices = mesh.devices.reshape(sizes["gz"], sizes["row"], sizes["col"] // CORES, CORES)
    split = Mesh(devices, ("gz", "row", "z", "core"))
    col = ("z", "core")
    in_specs = (
        P(None, col, "row"),
        P(None, col, "row"),
        P("gz", col, "row"),
        P("gz", col, "row"),
        P(None, col, None),
        P("gz", col, None),
        P(),
        P("gz", None),
    )
    out_specs = (P(None, ("row", "z", "core"), None), P("gz", ("row", "z", "core"), None))

    return jax.shard_map(local, mesh=split, in_specs=in_specs, out_specs=out_specs, check_vma=False)
```

```python
import functools

import jax
import jax.numpy as jnp
from jax import lax
from jax.experimental import pallas as pl
from jax.experimental.pallas import tpu as pltpu
from jax.sharding import Mesh, PartitionSpec as P


SUB_NODES = 3
LEAVES = (1, 2)
CORES = 2
ROWS8 = 8
F32 = jnp.float32
BF16 = jnp.bfloat16
VMEM_BYTES = 12 * 2**20


def level_span(depth):
    return 2**depth - 1, 2 ** (depth + 1) - 1


def depth_of(node):
    return (node + 1).bit_length() - 1


def above(node, level):
    return ((node + 1) >> (depth_of(node) - level)) - 1


def swapped(array):
    return lax.ppermute(array, "core", [(0, 1), (1, 0)])


def shape(dtype, *dims):
    return jax.ShapeDtypeStruct(dims, dtype)


def run(body, outs, smem, vmem, scratch=(), far=()):
    in_specs = [pl.BlockSpec(memory_space=pltpu.SMEM)] * len(smem)
    in_specs += [pl.BlockSpec(memory_space=pltpu.VMEM)] * len(vmem)
    in_specs += [pl.BlockSpec(memory_space=pltpu.HBM)] * len(far)
    far = [pltpu.with_memory_space_constraint(array, pltpu.HBM) for array in far]
    single = not isinstance(outs, (list, tuple))
    spec = pl.BlockSpec(memory_space=pltpu.VMEM)
    return pl.pallas_call(
        body,
        out_shape=outs,
        in_specs=in_specs,
        out_specs=spec if single else [spec] * len(outs),
        scratch_shapes=list(scratch),
        compiler_params=pltpu.CompilerParams(vmem_limit_bytes=VMEM_BYTES),
    )(*smem, *vmem, *far)


def total(tiles_ref):
    value = tiles_ref[0].astype(F32)
    for i in range(1, tiles_ref.shape[0]):
        value = value + tiles_ref[i].astype(F32)
    return value


def to_all(out_ref, value):
    value = value.astype(out_ref.dtype)
    for i in range(out_ref.shape[0]):
        out_ref[i] = value


def block(own_ref, other_ref, index):
    return jnp.concatenate([own_ref[index], other_ref[index]], 0)


def times(v, matrix):
    return lax.dot_general(v, matrix, (((1,), (0,)), ((), ())), preferred_element_type=F32)


def times_t(v, matrix):
    return lax.dot_general(v, matrix, (((1,), (1,)), ((), ())), preferred_element_type=F32)


def in_row(v, row):
    rows = lax.broadcasted_iota(jnp.int32, v.shape, 0)
    return jnp.where(rows == row, v, 0.0)


def own_first(v, core):
    return jnp.where(core == 1, pltpu.roll(v, v.shape[1] // 2, 1), v)


def position():
    return lax.axis_index("core"), lax.axis_index("z")


class Pairs:
    def __init__(self, levels, anc_count):
        self.sub = {}
        for m in range(SUB_NODES):
            for kind, count in ((0, levels), (1, depth_of(m))):
                for u in range(count):
                    self.sub[m, kind, u] = len(self.sub)
        self.anc = {}
        for a in range(anc_count):
            for u in range(depth_of(a)):
                self.anc[a, u] = anc_count + len(self.anc)


def sub_leaf_solve(there, other, own, here, rhs, out, near, near_rhs, sems):
    first, count = LEAVES[0], len(LEAVES)
    copies = [
        pltpu.make_async_copy(own.at[pl.ds(first, count)], near, sems.at[0]),
        pltpu.make_async_copy(here, near_rhs, sems.at[1]),
    ]
    for copy in copies:
        copy.start()
    for copy in copies:
        copy.wait()
    core = lax.axis_index("core")
    cols = rhs.shape[1]
    for m in range(SUB_NODES):
        flipped = jnp.concatenate([near_rhs[m], there[m]], 0).astype(F32).T
        rhs[m] = jnp.where(core == 0, flipped[:cols], flipped[cols:]).astype(BF16)
    for m in LEAVES:
        both = jnp.concatenate([near[m - first], other[m]], 0)
        part = times(rhs[m], both).astype(BF16)
        for i in range(out.shape[0]):
            out[i, m - 1] = part


def sub_low(y, w, pairs, own, other, m, kind, u):
    p = pairs.sub[m, kind, u]
    return w[p : p + 1, :] * times_t(y, block(own, other, SUB_NODES + p))


def sub_leaf_update(pairs, w, tiles, local_low, other, y_out, out):
    y = total(tiles).astype(BF16)
    y_out[...] = y
    value = 0.0
    for i, m in enumerate(LEAVES):
        p = pairs.sub[m, 1, 0]
        both = jnp.concatenate([local_low[i], other[SUB_NODES + p]], 0)
        value = value + w[p : p + 1, :] * times_t(y[i], both)
    to_all(out, value)


def sub_root_solve(tiles, rhs, own, other, out):
    given = (rhs[0].astype(F32) - total(tiles)).astype(BF16)
    to_all(out, times(given, block(own, other, 0)))


def sub_root_anc(pairs, levels, w, tiles, y_leaf, own, other, y_out, out, scratch):
    y = total(tiles).astype(BF16)
    y_out[...] = y
    scratch[...] = jnp.zeros_like(scratch)
    for e in range(levels):
        value = sub_low(y, w, pairs, own, other, 0, 0, e)
        for m in LEAVES:
            value = value + sub_low(y_leaf[m - 1], w, pairs, own, other, m, 0, e)
        scratch[:, e, :] = value
    out[...] = scratch[...].astype(BF16)


def fetch(blocks, core, gathered, near, near_x, sems):
    wide = gathered.shape[3]
    copies = []
    at = 0
    while at < len(blocks):
        count = 1
        while at + count < len(blocks) and blocks[at + count] == blocks[at] + count:
            count += 1
        for r in range(gathered.shape[0] // CORES):
            for which, target in ((core, near), (1 - core, near_x)):
                copies.append(
                    pltpu.make_async_copy(
                        gathered.at[r * CORES + which, pl.ds(blocks[at], count)],
                        target.at[pl.ds(at, count), :, pl.ds(r * wide, wide)],
                        sems.at[len(copies)],
                    )
                )
        at += count
    for copy in copies:
        copy.start()
    return copies


def load_blocks(blocks, where, gathered, near, near_x, sems):
    for copy in fetch(blocks, where[0], gathered, near, near_x, sems):
        copy.wait()


def solve_level(depth, v8, offset, near, near_x, out, scratch):
    first, stop = level_span(depth)
    value = jnp.zeros_like(scratch)
    for i, a in enumerate(range(first, stop)):
        value = value + in_row(times(v8, block(near, near_x, offset + i)), a)
    scratch[...] = value
    to_all(out, scratch[first : first + out.shape[1], :])


def ancestor(subtree, g, layers, levels, e):
    return lax.shift_right_logical(subtree[g] + layers, levels - e) - 1


def anc_prepare(pairs, layers, nrow, where, subtree, pattern, here, there, blocks, *outs):
    choose, out, low_w, up_w, pick, local_low, sems = outs
    copies = [
        pltpu.make_async_copy(
            blocks.at[SUB_NODES + pairs.sub[m, 1, 0]], local_low.at[i], sems.at[i]
        )
        for i, m in enumerate(LEAVES)
    ]
    for copy in copies:
        copy.start()
    levels = choose.shape[0]
    for target, column in ((low_w, 0), (up_w, 1)):
        for p in range(pattern.shape[0]):
            weight = pattern[p, column].astype(F32)
            target[p : p + 1, :] = jnp.full((1, target.shape[1]), weight, F32)
    nodes = lax.broadcasted_iota(jnp.int32, pick.shape[1:], 0)
    for e in range(levels):
        ours = nodes == ancestor(subtree, where[4], layers, levels, e)
        pick[e] = jnp.where(ours, 1.0, 0.0)
    rows = lax.broadcasted_iota(jnp.int32, choose.shape[1:], 0)
    source = lax.broadcasted_iota(jnp.int32, choose.shape[1:], 1)
    for e in range(levels):
        value = jnp.zeros(choose.shape[1:], F32)
        for g in range(layers):
            ours = (source >= g * nrow) & (source < (g + 1) * nrow)
            hit = ours & (rows == ancestor(subtree, g, layers, levels, e))
            value = jnp.where(hit, 1.0, value)
        choose[e] = value
    lanes = lax.broadcasted_iota(jnp.int32, (ROWS8, here.shape[2]), 1)
    pick = jnp.where(lanes == where[5], 1.0, 0.0).astype(BF16)
    value = jnp.zeros_like(out)
    for a in range(here.shape[0]):
        value = value + in_row(times_t(pick, block(here, there, a)), a)
    out[...] = value
    for copy in copies:
        copy.wait()


def anc_first(depth, tiles, choose, given, near, near_x, acc_out, out, scratch, arrived):
    arrived[...] = tiles[...].astype(F32)
    acc = given[...]
    for e in range(choose.shape[0]):
        acc = acc - lax.dot_general(
            choose[e],
            arrived[:, e, :],
            (((1,), (0,)), ((), ())),
            precision=lax.Precision.HIGHEST,
            preferred_element_type=F32,
        )
    acc_out[...] = acc
    solve_level(depth, acc.astype(BF16), 0, near, near_x, out, scratch)


def pair_sum(depth, u, values, offset, blocks, down):
    first, stop = level_span(depth)
    result = 0.0
    for i, d in enumerate(range(first, stop)):
        source, target = (d, above(d, u)) if down else (above(d, u), d)
        v = jnp.broadcast_to(values[source : source + 1, :], values.shape)
        v = in_row(v, target).astype(BF16)
        result = result + times_t(v, block(*blocks, offset + i))
    return result


def level_rows(depth, tiles, out):
    first, stop = level_span(depth)
    out[...] = jnp.zeros_like(out)
    out[first:stop, :] = total(tiles)[: stop - first].astype(BF16).astype(F32)


def anc_forward(depth, tiles, acc_in, near, near_x, y_out, acc_out, out, scratch):
    level_rows(depth, tiles, y_out)
    acc = acc_in[...] - pair_sum(depth, depth - 1, y_out, 0, (near, near_x), True)
    acc_out[...] = acc
    solve_level(depth - 1, acc.astype(BF16), 2**depth, near, near_x, out, scratch)


def other_pairs(blocks, depth, down, where, values, acc_in, gathered, acc_out, near, near_x, sems):
    copies = fetch(blocks, where[0], gathered, near, near_x, sems)
    acc = acc_in[...]
    for copy in copies:
        copy.wait()
    for u in range(depth - 1):
        acc = acc - pair_sum(depth, u, values, u * 2**depth, (near, near_x), down)
    acc_out[...] = acc


def z_rows(values, rows):
    core, z = position()
    return own_first(values[:, pl.ds(pl.multiple_of(z * rows, rows), rows)], core)


def anc_turn(tiles, near, near_x, y_out, out, scratch):
    level_rows(0, tiles, y_out)
    t = z_rows(y_out, near.shape[1] * CORES)
    solve_level(0, t.astype(BF16), 0, near, near_x, out, scratch)


def anc_start(*refs):
    out = refs[-1]
    out[...] = sum(z_rows(values, out.shape[1]) for values in refs[:-1])


def anc_backward(depth, tiles, acc_in, near, near_x, z_out, out, scratch):
    level_rows(depth - 1, tiles, z_out)
    acc = acc_in[...] - pair_sum(depth, depth - 1, z_out, 0, (near, near_x), False)
    solve_level(depth, acc.astype(BF16), 2**depth, near, near_x, out, scratch)


def sub_pieces(where, y_root, y_leaf, out):
    core, held, base = where[0], where[2], where[3]
    rows = out.shape[2]
    span = pl.ds(pl.multiple_of(base, rows), rows)
    scale = held.astype(F32)
    for m in range(SUB_NODES):
        y = y_root[:, span] if m == 0 else y_leaf[m - 1, :, span]
        out[m] = scale * own_first(y.astype(F32), core)


def anc_spread(depth, nrow, tiles, *refs):
    *z_parts, out, scratch = refs
    first, stop = level_span(depth)
    scratch[...] = sum(values[...] for values in z_parts)
    scratch[first:stop, :] = total(tiles)
    wide = out.shape[2]
    for i in range(out.shape[0]):
        r = i % nrow
        out[i] = scratch[:, r * wide : (r + 1) * wide].astype(BF16)


def sub_turn(pairs, levels, w, pick, tiles, y_own, own, other, kept, out, scratch):
    scratch[...] = tiles[...].astype(F32)
    picked = []
    for e in range(levels):
        value = 0.0
        for a in range(*level_span(e)):
            value = value + pick[e, a : a + 1, :] * scratch[:, a, :]
        picked.append(value.astype(BF16))
    for m in range(SUB_NODES):
        value = y_own[m]
        for e in range(levels):
            p = pairs.sub[m, 0, e]
            value = value - w[p : p + 1, :] * times_t(picked[e], block(own, other, SUB_NODES + p))
        if m == 0:
            to_all(out, value)
        else:
            kept[m - 1] = value


def anc_pieces(tiles, here, there, scratch):
    core, z = position()
    scratch[...] = tiles[...].astype(F32)
    rows = here.shape[1]
    line = lax.broadcasted_iota(jnp.int32, (rows, tiles.shape[2]), 0)
    lane = lax.broadcasted_iota(jnp.int32, (rows, tiles.shape[2]), 1)
    for out, which in ((here, core), (there, 1 - core)):
        pick = jnp.where(lane == (z * CORES + which) * rows + line, 1.0, 0.0).astype(BF16)
        for a in range(here.shape[0]):
            out[a] = times_t(pick, scratch[:, a, :].astype(BF16)).astype(BF16)


def sub_root_back(tiles, own, other, kept, out):
    value = times(total(tiles).astype(BF16), block(own, other, 0))
    kept[...] = value
    to_all(out, value)


def sub_leaf_back(pairs, w, tiles, kept, own, other, out):
    z = total(tiles).astype(BF16)
    for m in LEAVES:
        p = pairs.sub[m, 1, 0]
        value = kept[m - 1] - w[p : p + 1, :] * times_t(z, block(own, other, SUB_NODES + p))
        for i in range(out.shape[0]):
            out[i, m - 1] = value.astype(BF16)


def sub_finish(tiles, root, own, other, out):
    t = total(tiles).astype(BF16)
    parts = [root[...]] + [times(t[m - 1], block(own, other, m)) for m in LEAVES]
    fill = out.shape[2] - sum(part.shape[0] for part in parts)
    if fill:
        parts.append(jnp.zeros((fill, parts[0].shape[1]), F32))
    flipped = jnp.concatenate(parts, 0).T
    out[...] = flipped.reshape(out.shape).astype(BF16)


def local(anc_lower, anc_upper, sub_lower, sub_upper, anc_rhs, sub_rhs, layer_subtree, sub_pattern):
    layers = lax.axis_size("gz")
    levels = layers.bit_length() - 1
    anc_count = layers - 1
    nrow, nz = lax.axis_size("row"), lax.axis_size("z")
    own, wide = sub_lower.shape[1:]
    size = wide * nrow
    pair_rows = own * CORES
    out_rows = wide // (nz * CORES)
    cols = sub_rhs.shape[2] // CORES
    g, r, z, core = (lax.axis_index(name) for name in ("gz", "row", "z", "core"))
    pairs = Pairs(levels, anc_count)
    part = functools.partial
    scr8 = pltpu.VMEM((ROWS8, size), F32)

    held = (r == z * nrow // nz).astype(jnp.int32)
    base = jnp.clip(z * pair_rows - r * wide, 0, wide - pair_rows)
    where = jnp.stack([core, z, held, base, g, core * cols + g * nrow + r]).astype(jnp.int32)

    def gathered(blocks):
        return lax.all_gather(blocks, ("row", "core"), axis=0, tiled=False)

    def exchange(array, axes):
        return lax.all_to_all(array, axes, 0, 0, tiled=True)

    def two_cores(array):
        return array, swapped(array)

    def tied(send, *others):
        return lax.optimization_barrier((send, *others))

    low = (sub_lower, swapped(sub_lower))
    rhs_there = swapped(sub_rhs)
    anc_low = gathered(anc_lower)

    def diagonal(depth):
        return list(range(*level_span(depth)))

    def pair_blocks(depth, u):
        return [pairs.anc[a, u] for a in range(*level_span(depth))]

    def loaded(blocks, stack):
        near = shape(BF16, len(blocks), own, size)
        sems = pltpu.SemaphoreType.DMA((len(blocks) * nrow * CORES,))
        return run(part(load_blocks, blocks), (near, near), (where,), (), (sems,), (stack,))

    def others(depth, down, values, acc, stack):
        blocks = [index for u in range(depth - 1) for index in pair_blocks(depth, u)]
        near = pltpu.VMEM((len(blocks), own, size), BF16)
        sems = pltpu.SemaphoreType.DMA((len(blocks) * nrow * CORES,))
        body = part(other_pairs, blocks, depth, down)
        return run(body, acc_shape, (where,), (values, acc), (near, near, sems), (stack,))

    def level_shape(depth):
        return shape(BF16, nz, max(2, 2**depth), size)

    acc_shape = shape(F32, ROWS8, pair_rows)
    row_shape = shape(F32, ROWS8, size)

    rhs, tiles = run(
        sub_leaf_solve,
        (shape(BF16, SUB_NODES, cols, pair_rows), shape(BF16, nz, 2, cols, wide)),
        (),
        (rhs_there, low[1]),
        (
            pltpu.VMEM((len(LEAVES), own, wide), BF16),
            pltpu.VMEM(sub_rhs.shape, BF16),
            pltpu.SemaphoreType.DMA((2,)),
        ),
        (sub_lower, sub_rhs),
    )
    tiles, anc_rhs = tied(tiles, anc_rhs)
    anc_there = swapped(anc_rhs)
    weights = shape(F32, sub_pattern.shape[0], pair_rows)
    choose, given8, low_w, up_w, pick, local_low = run(
        part(anc_prepare, pairs, layers, nrow),
        (
            shape(F32, levels, ROWS8, layers * nrow),
            acc_shape,
            weights,
            weights,
            shape(F32, levels, ROWS8, wide),
            shape(BF16, len(LEAVES), own, wide),
        ),
        (where, layer_subtree, sub_pattern),
        (anc_rhs, anc_there),
        (pltpu.SemaphoreType.DMA((len(LEAVES),)),),
        (sub_lower,),
    )
    given8, anc_upper = tied(given8, anc_upper)
    anc_up = gathered(anc_upper)
    tiles = exchange(tiles, "z")
    tiles, given8, choose, low_w, local_low = tied(tiles, given8, choose, low_w, local_low)
    y_leaf, tiles = run(
        part(sub_leaf_update, pairs),
        (shape(BF16, 2, cols, wide), shape(BF16, nrow, cols, pair_rows)),
        (),
        (low_w, tiles, local_low, low[1]),
    )
    tiles = exchange(tiles, "row")
    tiles = run(sub_root_solve, shape(BF16, nz, cols, wide), (), (tiles, rhs, *low))
    tiles = exchange(tiles, "z")
    c_scratch = pltpu.VMEM((layers * nrow, ROWS8, pair_rows), F32)
    y_root, tiles = run(
        part(sub_root_anc, pairs, levels),
        (shape(BF16, cols, wide), shape(BF16, layers * nrow, ROWS8, pair_rows)),
        (),
        (low_w, tiles, y_leaf, *low),
        (c_scratch,),
    )
    tiles = exchange(tiles, ("gz", "row"))

    def step_blocks(depth):
        return pair_blocks(depth, depth - 1) + diagonal(depth - 1)

    near = loaded(diagonal(levels - 1), anc_low)
    ready = loaded(step_blocks(levels - 1), anc_low)
    tiles, *both = tied(tiles, *near, *ready)
    near, ready = both[:2], both[2:]

    acc, tiles = run(
        part(anc_first, levels - 1),
        (acc_shape, level_shape(levels - 1)),
        (),
        (tiles, choose, given8, *near),
        (scr8, c_scratch),
    )
    tiles = exchange(tiles, "z")
    y_parts = []
    for depth in range(levels - 1, 0, -1):
        near = ready
        if depth < levels - 1:
            near = loaded(step_blocks(depth), anc_low)
            tiles, *near = tied(tiles, *near)
        if depth == 1:
            near_root = loaded(diagonal(0), anc_up)
            tiles, *near_root = tied(tiles, *near_root)
        y8, acc, tiles = run(
            part(anc_forward, depth),
            (row_shape, acc_shape, level_shape(depth - 1)),
            (),
            (tiles, acc, *near),
            (scr8,),
        )
        y_parts.append(y8)
        tiles = exchange(tiles, "z")
        if depth > 1:
            acc = others(depth, True, y8, acc, anc_low)
            tiles, acc = tied(tiles, acc)
    y8, tiles = run(anc_turn, (row_shape, level_shape(0)), (), (tiles, *near_root), (scr8,))
    y_parts.append(y8)
    tiles = exchange(tiles, "z")
    start8 = run(anc_start, acc_shape, (), y_parts)
    tiles, start8 = tied(tiles, start8)
    z8 = None
    z_parts = []
    for depth in range(1, levels):
        acc = start8
        blocks = pair_blocks(depth, depth - 1) + diagonal(depth)
        near = loaded(blocks, anc_up)
        tiles, *near = tied(tiles, *near)
        if depth > 1:
            acc = others(depth, False, z8, acc, anc_up)
            tiles, acc = tied(tiles, acc)
        z_now, tiles = run(
            part(anc_backward, depth),
            (row_shape, level_shape(depth)),
            (),
            (tiles, acc, *near),
            (scr8,),
        )
        tiles = exchange(tiles, "z")
        z_parts.append(z_now)
        z8 = z_now
    tiles = run(
        part(anc_spread, levels - 1, nrow),
        shape(BF16, layers * nrow, ROWS8, wide),
        (),
        (tiles, *z_parts),
        (scr8,),
    )
    tiles, sub_upper = tied(tiles, sub_upper)
    up = two_cores(sub_upper)
    z_all = exchange(tiles, ("gz", "row"))
    y_own = run(sub_pieces, shape(F32, SUB_NODES, cols, pair_rows), (where,), (y_root, y_leaf))
    z_all, y_own, up_there, up_w, pick = tied(z_all, y_own, up[1], up_w, pick)
    up = (up[0], up_there)

    kept, tiles = run(
        part(sub_turn, pairs, levels),
        (shape(F32, 2, cols, pair_rows), shape(BF16, nrow, cols, pair_rows)),
        (),
        (up_w, pick, z_all, y_own, *up),
        (pltpu.VMEM(z_all.shape, F32),),
    )
    tiles = exchange(tiles, "row")

    def joined(here, there):
        flipped = core == 1
        return jnp.concatenate([jnp.where(flipped, there, here), jnp.where(flipped, here, there)], -1)

    root, tiles = run(
        sub_root_back,
        (shape(F32, cols, wide), shape(BF16, nz, cols, wide)),
        (),
        (tiles, *up),
    )
    tiles = exchange(tiles, "z")
    tiles = run(
        part(sub_leaf_back, pairs),
        shape(BF16, nrow, 2, cols, pair_rows),
        (),
        (up_w, tiles, kept, *up),
    )
    tiles = exchange(tiles, "row")
    packed = -(-SUB_NODES * cols // 128) * 128
    tiles = run(
        sub_finish,
        shape(BF16, nz * CORES, out_rows, packed),
        (),
        (tiles, root, *up),
    )
    tiles = exchange(tiles, ("z", "core"))
    piece = shape(BF16, anc_count, out_rows, cols)
    out_here, out_there = run(
        anc_pieces, (piece, piece), (), (z_all,), (pltpu.VMEM(z_all.shape, F32),)
    )
    out_there = swapped(out_there)
    anc_out = joined(out_here, out_there).astype(F32)
    sums = jnp.sum(tiles.astype(F32).reshape(nz, CORES, out_rows, packed), 0)
    sums = sums[:, :, : SUB_NODES * cols].reshape(CORES, out_rows, SUB_NODES, cols)
    sub_out = sums.transpose(2, 1, 0, 3).reshape(SUB_NODES, out_rows, CORES * cols)
    return anc_out, sub_out


def solution(mesh):
    sizes = dict(mesh.shape)
    devices = mesh.devices.reshape(sizes["gz"], sizes["row"], sizes["col"] // CORES, CORES)
    split = Mesh(devices, ("gz", "row", "z", "core"))
    col = ("z", "core")
    in_specs = (
        P(None, col, "row"),
        P(None, col, "row"),
        P("gz", col, "row"),
        P("gz", col, "row"),
        P(None, col, None),
        P("gz", col, None),
        P(),
        P("gz", None),
    )
    out_specs = (P(None, ("row", "z", "core"), None), P("gz", ("row", "z", "core"), None))

    return jax.shard_map(local, mesh=split, in_specs=in_specs, out_specs=out_specs, check_vma=False)
```

```python
import functools

import jax
import jax.numpy as jnp
from jax import lax
from jax.experimental import pallas as pl
from jax.experimental.pallas import tpu as pltpu
from jax.sharding import Mesh, PartitionSpec as P


SUB_NODES = 3
LEAVES = (1, 2)
CORES = 2
ROWS8 = 8
F32 = jnp.float32
BF16 = jnp.bfloat16
VMEM_BYTES = 12 * 2**20


def level_span(depth):
    return 2**depth - 1, 2 ** (depth + 1) - 1


def depth_of(node):
    return (node + 1).bit_length() - 1


def above(node, level):
    return ((node + 1) >> (depth_of(node) - level)) - 1


def swapped(array):
    return lax.ppermute(array, "core", [(0, 1), (1, 0)])


def shape(dtype, *dims):
    return jax.ShapeDtypeStruct(dims, dtype)


def run(body, outs, smem, vmem, scratch=(), far=()):
    in_specs = [pl.BlockSpec(memory_space=pltpu.SMEM)] * len(smem)
    in_specs += [pl.BlockSpec(memory_space=pltpu.VMEM)] * len(vmem)
    in_specs += [pl.BlockSpec(memory_space=pltpu.HBM)] * len(far)
    far = [pltpu.with_memory_space_constraint(array, pltpu.HBM) for array in far]
    single = not isinstance(outs, (list, tuple))
    spec = pl.BlockSpec(memory_space=pltpu.VMEM)
    return pl.pallas_call(
        body,
        out_shape=outs,
        in_specs=in_specs,
        out_specs=spec if single else [spec] * len(outs),
        scratch_shapes=list(scratch),
        compiler_params=pltpu.CompilerParams(vmem_limit_bytes=VMEM_BYTES),
    )(*smem, *vmem, *far)


def total(tiles_ref):
    value = tiles_ref[0].astype(F32)
    for i in range(1, tiles_ref.shape[0]):
        value = value + tiles_ref[i].astype(F32)
    return value


def to_all(out_ref, value):
    value = value.astype(out_ref.dtype)
    for i in range(out_ref.shape[0]):
        out_ref[i] = value


def block(own_ref, other_ref, index):
    return jnp.concatenate([own_ref[index], other_ref[index]], 0)


def times(v, matrix):
    return lax.dot_general(v, matrix, (((1,), (0,)), ((), ())), preferred_element_type=F32)


def times_t(v, matrix):
    return lax.dot_general(v, matrix, (((1,), (1,)), ((), ())), preferred_element_type=F32)


def in_row(v, row):
    rows = lax.broadcasted_iota(jnp.int32, v.shape, 0)
    return jnp.where(rows == row, v, 0.0)


def own_first(v, core):
    return jnp.where(core == 1, pltpu.roll(v, v.shape[1] // 2, 1), v)


def position():
    return lax.axis_index("core"), lax.axis_index("z")


class Pairs:
    def __init__(self, levels, anc_count):
        self.sub = {}
        for m in range(SUB_NODES):
            for kind, count in ((0, levels), (1, depth_of(m))):
                for u in range(count):
                    self.sub[m, kind, u] = len(self.sub)
        self.anc = {}
        for a in range(anc_count):
            for u in range(depth_of(a)):
                self.anc[a, u] = anc_count + len(self.anc)


def sub_leaf_load(own, here, near, near_rhs, sems):
    copies = [
        pltpu.make_async_copy(own.at[pl.ds(LEAVES[0], len(LEAVES))], near, sems.at[0]),
        pltpu.make_async_copy(here, near_rhs, sems.at[1]),
    ]
    for copy in copies:
        copy.start()
    for copy in copies:
        copy.wait()


def sub_leaf_solve(there, other, near, near_rhs, rhs, out):
    core = lax.axis_index("core")
    cols = rhs.shape[1]
    for m in range(SUB_NODES):
        flipped = jnp.concatenate([near_rhs[m], there[m]], 0).astype(F32).T
        rhs[m] = jnp.where(core == 0, flipped[:cols], flipped[cols:]).astype(BF16)
    for m in LEAVES:
        both = jnp.concatenate([near[m - LEAVES[0]], other[m]], 0)
        part = times(rhs[m], both).astype(BF16)
        for i in range(out.shape[0]):
            out[i, m - 1] = part


def sub_low(y, w, pairs, own, other, m, kind, u):
    p = pairs.sub[m, kind, u]
    return w[p : p + 1, :] * times_t(y, block(own, other, SUB_NODES + p))


def sub_leaf_update(pairs, w, tiles, local_low, other, y_out, out):
    y = total(tiles).astype(BF16)
    y_out[...] = y
    value = 0.0
    for i, m in enumerate(LEAVES):
        p = pairs.sub[m, 1, 0]
        both = jnp.concatenate([local_low[i], other[SUB_NODES + p]], 0)
        value = value + w[p : p + 1, :] * times_t(y[i], both)
    to_all(out, value)


def sub_root_solve(tiles, rhs, own, other, out):
    given = (rhs[0].astype(F32) - total(tiles)).astype(BF16)
    to_all(out, times(given, block(own, other, 0)))


def sub_root_anc(pairs, levels, w, tiles, y_leaf, own, other, y_out, out, scratch):
    y = total(tiles).astype(BF16)
    y_out[...] = y
    scratch[...] = jnp.zeros_like(scratch)
    for e in range(levels):
        value = sub_low(y, w, pairs, own, other, 0, 0, e)
        for m in LEAVES:
            value = value + sub_low(y_leaf[m - 1], w, pairs, own, other, m, 0, e)
        scratch[:, e, :] = value
    out[...] = scratch[...].astype(BF16)


def fetch(blocks, core, gathered, near, near_x, sems):
    wide = gathered.shape[3]
    copies = []
    at = 0
    while at < len(blocks):
        count = 1
        while at + count < len(blocks) and blocks[at + count] == blocks[at] + count:
            count += 1
        for r in range(gathered.shape[0] // CORES):
            for which, target in ((core, near), (1 - core, near_x)):
                copies.append(
                    pltpu.make_async_copy(
                        gathered.at[r * CORES + which, pl.ds(blocks[at], count)],
                        target.at[pl.ds(at, count), :, pl.ds(r * wide, wide)],
                        sems.at[len(copies)],
                    )
                )
        at += count
    for copy in copies:
        copy.start()
    return copies


def load_blocks(blocks, where, gathered, near, near_x, sems):
    for copy in fetch(blocks, where[0], gathered, near, near_x, sems):
        copy.wait()


def solve_level(depth, v8, offset, near, near_x, out, scratch):
    first, stop = level_span(depth)
    value = jnp.zeros_like(scratch)
    for i, a in enumerate(range(first, stop)):
        value = value + in_row(times(v8, block(near, near_x, offset + i)), a)
    scratch[...] = value
    to_all(out, scratch[first : first + out.shape[1], :])


def ancestor(subtree, g, layers, levels, e):
    return lax.shift_right_logical(subtree[g] + layers, levels - e) - 1


def anc_prepare(pairs, layers, nrow, where, subtree, pattern, here, there, blocks, *outs):
    choose, out, low_w, up_w, pick, local_low, sems = outs
    copies = [
        pltpu.make_async_copy(
            blocks.at[SUB_NODES + pairs.sub[m, 1, 0]], local_low.at[i], sems.at[i]
        )
        for i, m in enumerate(LEAVES)
    ]
    for copy in copies:
        copy.start()
    levels = choose.shape[0]
    for target, column in ((low_w, 0), (up_w, 1)):
        for p in range(pattern.shape[0]):
            weight = pattern[p, column].astype(F32)
            target[p : p + 1, :] = jnp.full((1, target.shape[1]), weight, F32)
    nodes = lax.broadcasted_iota(jnp.int32, pick.shape[1:], 0)
    for e in range(levels):
        ours = nodes == ancestor(subtree, where[4], layers, levels, e)
        pick[e] = jnp.where(ours, 1.0, 0.0)
    rows = lax.broadcasted_iota(jnp.int32, choose.shape[1:], 0)
    source = lax.broadcasted_iota(jnp.int32, choose.shape[1:], 1)
    for e in range(levels):
        value = jnp.zeros(choose.shape[1:], F32)
        for g in range(layers):
            ours = (source >= g * nrow) & (source < (g + 1) * nrow)
            hit = ours & (rows == ancestor(subtree, g, layers, levels, e))
            value = jnp.where(hit, 1.0, value)
        choose[e] = value
    lanes = lax.broadcasted_iota(jnp.int32, (ROWS8, here.shape[2]), 1)
    pick = jnp.where(lanes == where[5], 1.0, 0.0).astype(BF16)
    value = jnp.zeros_like(out)
    for a in range(here.shape[0]):
        value = value + in_row(times_t(pick, block(here, there, a)), a)
    out[...] = value
    for copy in copies:
        copy.wait()


def anc_first(depth, tiles, choose, given, near, near_x, acc_out, out, scratch, arrived):
    arrived[...] = tiles[...].astype(F32)
    acc = given[...]
    for e in range(choose.shape[0]):
        acc = acc - lax.dot_general(
            choose[e],
            arrived[:, e, :],
            (((1,), (0,)), ((), ())),
            precision=lax.Precision.HIGHEST,
            preferred_element_type=F32,
        )
    acc_out[...] = acc
    solve_level(depth, acc.astype(BF16), 0, near, near_x, out, scratch)


def pair_sum(depth, u, values, offset, blocks, down):
    first, stop = level_span(depth)
    result = 0.0
    for i, d in enumerate(range(first, stop)):
        source, target = (d, above(d, u)) if down else (above(d, u), d)
        v = jnp.broadcast_to(values[source : source + 1, :], values.shape)
        v = in_row(v, target).astype(BF16)
        result = result + times_t(v, block(*blocks, offset + i))
    return result


def level_rows(depth, tiles, out):
    first, stop = level_span(depth)
    out[...] = jnp.zeros_like(out)
    out[first:stop, :] = total(tiles)[: stop - first].astype(BF16).astype(F32)


def anc_forward(depth, tiles, acc_in, near, near_x, y_out, acc_out, out, scratch):
    level_rows(depth, tiles, y_out)
    acc = acc_in[...] - pair_sum(depth, depth - 1, y_out, 0, (near, near_x), True)
    acc_out[...] = acc
    solve_level(depth - 1, acc.astype(BF16), 2**depth, near, near_x, out, scratch)


def other_pairs(blocks, depth, down, where, values, acc_in, gathered, acc_out, near, near_x, sems):
    copies = fetch(blocks, where[0], gathered, near, near_x, sems)
    acc = acc_in[...]
    for copy in copies:
        copy.wait()
    for u in range(depth - 1):
        acc = acc - pair_sum(depth, u, values, u * 2**depth, (near, near_x), down)
    acc_out[...] = acc


def z_rows(values, rows):
    core, z = position()
    return own_first(values[:, pl.ds(pl.multiple_of(z * rows, rows), rows)], core)


def anc_turn(tiles, near, near_x, y_out, out, scratch):
    level_rows(0, tiles, y_out)
    t = z_rows(y_out, near.shape[1] * CORES)
    solve_level(0, t.astype(BF16), 0, near, near_x, out, scratch)


def anc_start(*refs):
    out = refs[-1]
    out[...] = sum(z_rows(values, out.shape[1]) for values in refs[:-1])


def anc_backward(depth, tiles, acc_in, near, near_x, z_out, out, scratch):
    level_rows(depth - 1, tiles, z_out)
    acc = acc_in[...] - pair_sum(depth, depth - 1, z_out, 0, (near, near_x), False)
    solve_level(depth, acc.astype(BF16), 2**depth, near, near_x, out, scratch)


def sub_pieces(where, y_root, y_leaf, out):
    core, held, base = where[0], where[2], where[3]
    rows = out.shape[2]
    span = pl.ds(pl.multiple_of(base, rows), rows)
    scale = held.astype(F32)
    for m in range(SUB_NODES):
        y = y_root[:, span] if m == 0 else y_leaf[m - 1, :, span]
        out[m] = scale * own_first(y.astype(F32), core)


def anc_spread(depth, nrow, tiles, *refs):
    *z_parts, out, scratch = refs
    first, stop = level_span(depth)
    scratch[...] = sum(values[...] for values in z_parts)
    scratch[first:stop, :] = total(tiles)
    wide = out.shape[2]
    for i in range(out.shape[0]):
        r = i % nrow
        out[i] = scratch[:, r * wide : (r + 1) * wide].astype(BF16)


def sub_turn(pairs, levels, w, pick, tiles, y_own, own, other, kept, out, scratch):
    scratch[...] = tiles[...].astype(F32)
    picked = []
    for e in range(levels):
        value = 0.0
        for a in range(*level_span(e)):
            value = value + pick[e, a : a + 1, :] * scratch[:, a, :]
        picked.append(value.astype(BF16))
    for m in range(SUB_NODES):
        value = y_own[m]
        for e in range(levels):
            p = pairs.sub[m, 0, e]
            value = value - w[p : p + 1, :] * times_t(picked[e], block(own, other, SUB_NODES + p))
        if m == 0:
            to_all(out, value)
        else:
            kept[m - 1] = value


def anc_pieces(tiles, here, there, scratch):
    core, z = position()
    scratch[...] = tiles[...].astype(F32)
    rows = here.shape[1]
    line = lax.broadcasted_iota(jnp.int32, (rows, tiles.shape[2]), 0)
    lane = lax.broadcasted_iota(jnp.int32, (rows, tiles.shape[2]), 1)
    for out, which in ((here, core), (there, 1 - core)):
        pick = jnp.where(lane == (z * CORES + which) * rows + line, 1.0, 0.0).astype(BF16)
        for a in range(here.shape[0]):
            out[a] = times_t(pick, scratch[:, a, :].astype(BF16)).astype(BF16)


def sub_root_back(tiles, own, other, kept, out):
    value = times(total(tiles).astype(BF16), block(own, other, 0))
    kept[...] = value
    to_all(out, value)


def sub_leaf_back(pairs, w, tiles, kept, own, other, out):
    z = total(tiles).astype(BF16)
    for m in LEAVES:
        p = pairs.sub[m, 1, 0]
        value = kept[m - 1] - w[p : p + 1, :] * times_t(z, block(own, other, SUB_NODES + p))
        for i in range(out.shape[0]):
            out[i, m - 1] = value.astype(BF16)


def sub_finish(tiles, root, own, other, out):
    t = total(tiles).astype(BF16)
    parts = [root[...]] + [times(t[m - 1], block(own, other, m)) for m in LEAVES]
    fill = out.shape[2] - sum(part.shape[0] for part in parts)
    if fill:
        parts.append(jnp.zeros((fill, parts[0].shape[1]), F32))
    flipped = jnp.concatenate(parts, 0).T
    out[...] = flipped.reshape(out.shape).astype(BF16)


def local(anc_lower, anc_upper, sub_lower, sub_upper, anc_rhs, sub_rhs, layer_subtree, sub_pattern):
    layers = lax.axis_size("gz")
    levels = layers.bit_length() - 1
    anc_count = layers - 1
    nrow, nz = lax.axis_size("row"), lax.axis_size("z")
    own, wide = sub_lower.shape[1:]
    size = wide * nrow
    pair_rows = own * CORES
    out_rows = wide // (nz * CORES)
    cols = sub_rhs.shape[2] // CORES
    g, r, z, core = (lax.axis_index(name) for name in ("gz", "row", "z", "core"))
    pairs = Pairs(levels, anc_count)
    part = functools.partial
    scr8 = pltpu.VMEM((ROWS8, size), F32)

    held = (r == z * nrow // nz).astype(jnp.int32)
    base = jnp.clip(z * pair_rows - r * wide, 0, wide - pair_rows)
    where = jnp.stack([core, z, held, base, g, core * cols + g * nrow + r]).astype(jnp.int32)

    def gathered(blocks):
        return lax.all_gather(blocks, ("row", "core"), axis=0, tiled=False)

    def exchange(array, axes):
        return lax.all_to_all(array, axes, 0, 0, tiled=True)

    def two_cores(array):
        return array, swapped(array)

    def tied(send, *others):
        return lax.optimization_barrier((send, *others))

    low = (sub_lower, swapped(sub_lower))
    rhs_there = swapped(sub_rhs)
    anc_low = gathered(anc_lower)

    def diagonal(depth):
        return list(range(*level_span(depth)))

    def pair_blocks(depth, u):
        return [pairs.anc[a, u] for a in range(*level_span(depth))]

    def loaded(blocks, stack):
        near = shape(BF16, len(blocks), own, size)
        sems = pltpu.SemaphoreType.DMA((len(blocks) * nrow * CORES,))
        return run(part(load_blocks, blocks), (near, near), (where,), (), (sems,), (stack,))

    def others(depth, down, values, acc, stack):
        blocks = [index for u in range(depth - 1) for index in pair_blocks(depth, u)]
        near = pltpu.VMEM((len(blocks), own, size), BF16)
        sems = pltpu.SemaphoreType.DMA((len(blocks) * nrow * CORES,))
        body = part(other_pairs, blocks, depth, down)
        return run(body, acc_shape, (where,), (values, acc), (near, near, sems), (stack,))

    def level_shape(depth):
        return shape(BF16, nz, max(2, 2**depth), size)

    acc_shape = shape(F32, ROWS8, pair_rows)
    row_shape = shape(F32, ROWS8, size)

    first = run(
        sub_leaf_load,
        (shape(BF16, len(LEAVES), own, wide), shape(BF16, *sub_rhs.shape)),
        (),
        (),
        (pltpu.SemaphoreType.DMA((2,)),),
        (sub_lower, sub_rhs),
    )
    rhs, tiles = run(
        sub_leaf_solve,
        (shape(BF16, SUB_NODES, cols, pair_rows), shape(BF16, nz, 2, cols, wide)),
        (),
        (rhs_there, low[1], *first),
    )
    tiles, anc_rhs = tied(tiles, anc_rhs)
    anc_there = swapped(anc_rhs)
    weights = shape(F32, sub_pattern.shape[0], pair_rows)
    choose, given8, low_w, up_w, pick, local_low = run(
        part(anc_prepare, pairs, layers, nrow),
        (
            shape(F32, levels, ROWS8, layers * nrow),
            acc_shape,
            weights,
            weights,
            shape(F32, levels, ROWS8, wide),
            shape(BF16, len(LEAVES), own, wide),
        ),
        (where, layer_subtree, sub_pattern),
        (anc_rhs, anc_there),
        (pltpu.SemaphoreType.DMA((len(LEAVES),)),),
        (sub_lower,),
    )
    given8, anc_upper = tied(given8, anc_upper)
    anc_up = gathered(anc_upper)
    tiles = exchange(tiles, "z")
    tiles, given8, choose, low_w, local_low = tied(tiles, given8, choose, low_w, local_low)
    y_leaf, tiles = run(
        part(sub_leaf_update, pairs),
        (shape(BF16, 2, cols, wide), shape(BF16, nrow, cols, pair_rows)),
        (),
        (low_w, tiles, local_low, low[1]),
    )
    tiles = exchange(tiles, "row")
    tiles = run(sub_root_solve, shape(BF16, nz, cols, wide), (), (tiles, rhs, *low))
    tiles = exchange(tiles, "z")
    c_scratch = pltpu.VMEM((layers * nrow, ROWS8, pair_rows), F32)
    y_root, tiles = run(
        part(sub_root_anc, pairs, levels),
        (shape(BF16, cols, wide), shape(BF16, layers * nrow, ROWS8, pair_rows)),
        (),
        (low_w, tiles, y_leaf, *low),
        (c_scratch,),
    )
    tiles = exchange(tiles, ("gz", "row"))

    def step_blocks(depth):
        return pair_blocks(depth, depth - 1) + diagonal(depth - 1)

    near = loaded(diagonal(levels - 1), anc_low)
    ready = loaded(step_blocks(levels - 1), anc_low)
    tiles, *both = tied(tiles, *near, *ready)
    near, ready = both[:2], both[2:]

    acc, tiles = run(
        part(anc_first, levels - 1),
        (acc_shape, level_shape(levels - 1)),
        (),
        (tiles, choose, given8, *near),
        (scr8, c_scratch),
    )
    tiles = exchange(tiles, "z")
    y_parts = []
    for depth in range(levels - 1, 0, -1):
        near = ready
        if depth < levels - 1:
            near = loaded(step_blocks(depth), anc_low)
            tiles, *near = tied(tiles, *near)
        y8, acc, tiles = run(
            part(anc_forward, depth),
            (row_shape, acc_shape, level_shape(depth - 1)),
            (),
            (tiles, acc, *near),
            (scr8,),
        )
        y_parts.append(y8)
        tiles = exchange(tiles, "z")
        if depth > 1:
            acc = others(depth, True, y8, acc, anc_low)
            tiles, acc = tied(tiles, acc)
    near_root = loaded(diagonal(0), anc_up)
    tiles, *near_root = tied(tiles, *near_root)
    y8, tiles = run(anc_turn, (row_shape, level_shape(0)), (), (tiles, *near_root), (scr8,))
    y_parts.append(y8)
    tiles = exchange(tiles, "z")
    start8 = run(anc_start, acc_shape, (), y_parts)
    tiles, start8 = tied(tiles, start8)
    z8 = None
    z_parts = []
    for depth in range(1, levels):
        acc = start8
        blocks = pair_blocks(depth, depth - 1) + diagonal(depth)
        near = loaded(blocks, anc_up)
        tiles, *near = tied(tiles, *near)
        if depth > 1:
            acc = others(depth, False, z8, acc, anc_up)
            tiles, acc = tied(tiles, acc)
        z_now, tiles = run(
            part(anc_backward, depth),
            (row_shape, level_shape(depth)),
            (),
            (tiles, acc, *near),
            (scr8,),
        )
        tiles = exchange(tiles, "z")
        z_parts.append(z_now)
        z8 = z_now
    tiles = run(
        part(anc_spread, levels - 1, nrow),
        shape(BF16, layers * nrow, ROWS8, wide),
        (),
        (tiles, *z_parts),
        (scr8,),
    )
    tiles, sub_upper = tied(tiles, sub_upper)
    up = two_cores(sub_upper)
    z_all = exchange(tiles, ("gz", "row"))
    y_own = run(sub_pieces, shape(F32, SUB_NODES, cols, pair_rows), (where,), (y_root, y_leaf))
    z_all, y_own, up_there, up_w, pick = tied(z_all, y_own, up[1], up_w, pick)
    up = (up[0], up_there)

    kept, tiles = run(
        part(sub_turn, pairs, levels),
        (shape(F32, 2, cols, pair_rows), shape(BF16, nrow, cols, pair_rows)),
        (),
        (up_w, pick, z_all, y_own, *up),
        (pltpu.VMEM(z_all.shape, F32),),
    )
    tiles = exchange(tiles, "row")

    def joined(here, there):
        flipped = core == 1
        return jnp.concatenate([jnp.where(flipped, there, here), jnp.where(flipped, here, there)], -1)

    root, tiles = run(
        sub_root_back,
        (shape(F32, cols, wide), shape(BF16, nz, cols, wide)),
        (),
        (tiles, *up),
    )
    tiles = exchange(tiles, "z")
    tiles = run(
        part(sub_leaf_back, pairs),
        shape(BF16, nrow, 2, cols, pair_rows),
        (),
        (up_w, tiles, kept, *up),
    )
    tiles = exchange(tiles, "row")
    packed = -(-SUB_NODES * cols // 128) * 128
    tiles = run(
        sub_finish,
        shape(BF16, nz * CORES, out_rows, packed),
        (),
        (tiles, root, *up),
    )
    tiles = exchange(tiles, ("z", "core"))
    piece = shape(BF16, anc_count, out_rows, cols)
    out_here, out_there = run(
        anc_pieces, (piece, piece), (), (z_all,), (pltpu.VMEM(z_all.shape, F32),)
    )
    out_there = swapped(out_there)
    anc_out = joined(out_here, out_there).astype(F32)
    sums = jnp.sum(tiles.astype(F32).reshape(nz, CORES, out_rows, packed), 0)
    sums = sums[:, :, : SUB_NODES * cols].reshape(CORES, out_rows, SUB_NODES, cols)
    sub_out = sums.transpose(2, 1, 0, 3).reshape(SUB_NODES, out_rows, CORES * cols)
    return anc_out, sub_out


def solution(mesh):
    sizes = dict(mesh.shape)
    devices = mesh.devices.reshape(sizes["gz"], sizes["row"], sizes["col"] // CORES, CORES)
    split = Mesh(devices, ("gz", "row", "z", "core"))
    col = ("z", "core")
    in_specs = (
        P(None, col, "row"),
        P(None, col, "row"),
        P("gz", col, "row"),
        P("gz", col, "row"),
        P(None, col, None),
        P("gz", col, None),
        P(),
        P("gz", None),
    )
    out_specs = (P(None, ("row", "z", "core"), None), P("gz", ("row", "z", "core"), None))

    return jax.shard_map(local, mesh=split, in_specs=in_specs, out_specs=out_specs, check_vma=False)
```
